256 devices in a mesh: groups: 2 (over z), tp: 16 (over x, core), dp: 8 (over y).
Axes of the slice: x: 8, y: 8, z: 2, core: 2. Of those that a mesh axis runs over, the one named last changes fastest.
The devices are a block of a 8x8x16 slice.
Arguments:
- hidden: bfloat16 [256, 2560], P(('groups', 'dp'), 'tp'), parts along dimension 0, may hold values from -40 to 40
- in_gain: float32 [2560], replicated, may hold values from 0.1 to 1.9
- z_weight: bfloat16 [2560, 5120], P(None, 'tp'), may hold values from -0.125 to 0.125
- x_weight: bfloat16 [2560, 5120], P(None, 'tp'), may hold values from -0.125 to 0.125
- bc_weight: bfloat16 [2560, 256], P(None, 'tp'), may hold values from -0.125 to 0.125
- dt_weight: bfloat16 [2560, 80], P(None, 'tp'), may hold values from -0.125 to 0.125
- conv_x_weight: bfloat16 [4, 5120], P(None, 'tp'), may hold values from -3 to 3
- conv_x_bias: bfloat16 [5120], P('tp'), may hold values from -3 to 3
- conv_bc_weight: bfloat16 [4, 256], P(None, 'tp'), may hold values from -3 to 3
- conv_bc_bias: bfloat16 [256], P('tp'), may hold values from -3 to 3
- conv_x_state: bfloat16 [256, 3, 5120], P(('groups', 'dp'), None, 'tp'), parts along dimension 0, may hold values from -6 to 6
- conv_bc_state: bfloat16 [256, 3, 256], P(('groups', 'dp'), None, 'tp'), parts along dimension 0, may hold values from -6 to 6
- dt_bias: float32 [80], P('tp'), may hold values from -4 to -1
- log_rate: float32 [80], P('tp'), may hold values from 0 to 2.5
- skip_gain: float32 [80], P('tp'), may hold values from 0.5 to 2
- ssm_state: float32 [256, 80, 64, 128], P(('groups', 'dp'), 'tp'), parts along dimension 0, may hold values from -20 to 20
- norm_gain: float32 [5120], P('tp'), may hold values from 0.1 to 1.9
- out_weight: bfloat16 [5120, 2560], P('tp'), may hold values from -0.125 to 0.125
- pool_slot: int32 [16, 16], P(('groups', 'dp')), parts along dimension 0, may hold values from 0 to 15, as said below
- active: int32 [256], P(('groups', 'dp')), parts along dimension 0, may hold values 0 or 1
Outputs:
- layer_out: bfloat16 [256, 2560], P(('groups', 'dp'), 'tp'), parts along dimension 0
- conv_x_next: bfloat16 [256, 3, 5120], P(('groups', 'dp'), None, 'tp'), parts along dimension 0
- conv_bc_next: bfloat16 [256, 3, 256], P(('groups', 'dp'), None, 'tp'), parts along dimension 0
- ssm_next: float32 [256, 80, 64, 128], P(('groups', 'dp'), 'tp'), parts along dimension 0
The draws below stay inside these ranges and needn't reach their ends.
There are 2 independent parts, one for each index of `groups`. The reference program is written for one: setup_inputs(seed, part) draws one part's arguments, and reference() takes and returns one part's arrays. A program takes and returns all parts, laid end to end along the dimension named above; an argument that names none is the same for every part. Nothing has to cross between parts.
Inputs may be any that keep to these rules, and one draw needn't show every extreme that they name: `pool_slot`: each row is a permutation of 0 to 15.
All inputs are finite; a program needn't handle non-finite values. No bound on the sum of `active` on one device may be relied on, other than what follows from the above.
Results may differ from the reference program's by a relative error of at most 0.0085.
Values may be sent and summed in bfloat16 or wider, within the bound.
A program may use at most 64 MiB of HBM per device.

```python
import math
import jax
import jax.numpy as jnp
from jax import lax

D = 2560
HEADS = 80
HP = 64
NS = 128
KW = 4
SEQ_DEV = 16
INNER = 5120
BATCH = 128
N_DP = 8


def draw_hidden(key, part):
    base_key = jax.random.fold_in(key, 21)
    row_key = jax.random.fold_in(key, 22)
    col_key = jax.random.fold_in(key, 23)
    position = jnp.arange(D, dtype=jnp.float32) / (D - 1)
    jitter = jnp.exp(jax.random.uniform(col_key, (D,), jnp.float32, 0.0, math.log(3.3)))
    row_scale = jnp.exp(jax.random.uniform(row_key, (BATCH,), jnp.float32, math.log(0.3), math.log(3.0)))
    base_draw = jnp.clip(jax.random.normal(base_key, (BATCH, D), jnp.float32), -4.0, 4.0)
    col_scale = 3.0 ** position * jitter / 3.3
    return (base_draw * row_scale[:, None] * col_scale[None, :]).astype(jnp.bfloat16)


def draw_ssm_state(key, part):
    base_key = jax.random.fold_in(key, 11)
    head_key = jax.random.fold_in(key, 12)
    position = jnp.arange(HEADS, dtype=jnp.float32) / (HEADS - 1)
    base_draw = jnp.clip(jax.random.normal(base_key, (BATCH, HEADS, HP, NS), jnp.float32), -5.0, 5.0)
    head_trend = 3.0 ** position
    jitter = jnp.exp(jax.random.uniform(head_key, (HEADS,), jnp.float32, 0.0, math.log(3.0)))
    return 0.3 * base_draw * (head_trend * jitter)[None, :, None, None]


def permute_slots(slot_key):
    return jax.random.permutation(slot_key, SEQ_DEV)


def draw_pool_slot(key, part):
    slot_keys = jax.random.split(jax.random.fold_in(key, 31), N_DP)
    return jax.vmap(permute_slots)(slot_keys).astype(jnp.int32)


def place_ends(result, own_key, low, high):
    index_at = [jax.random.randint(jax.random.fold_in(own_key, axis), (), 0, length) for axis, length in enumerate(result.shape)]
    widest = result.shape.index(max(result.shape))
    beside = index_at[:widest] + [(index_at[widest] + 1) % result.shape[widest]] + index_at[widest + 1:]
    return result.at[tuple(index_at)].set(low).at[tuple(beside)].set(high)


def raised(values, own_key, source, target, blocks, factor):
    owner, partner = [(jnp.arange(values.shape[axis_at]) // (values.shape[axis_at] // blocks)).reshape([-1 if axis == axis_at else 1 for axis in range(values.ndim)]) for axis_at in (source, target)]
    chosen = jax.random.permutation(own_key, blocks)[partner]
    strong = (owner == chosen) | (owner == (partner + blocks // 2) % blocks)
    return jnp.where(strong, factor * values, values)


def level_of(stream_key, extent, cuts, least, largest):
    loudness = 1.0
    for axis_at, shards_of in cuts:
        steps = jax.random.uniform(jax.random.fold_in(jax.random.fold_in(stream_key, 6), axis_at), (shards_of,), jnp.float32, least / len(cuts), largest / len(cuts))
        loudness = loudness * jnp.repeat(jnp.exp(steps), extent[axis_at] // shards_of).reshape((-1,) + (1,) * (len(extent) - 1 - axis_at))
    return loudness


def normal_values(rng, dims, scale, bound, pieces=(), kind=jnp.bfloat16):
    entries = jax.random.normal(rng, dims, jnp.float32) * scale
    if len(pieces) > 0:
        entries = level_of(rng, dims, pieces, -0.22, 0.18) * entries
    return jnp.clip(entries, min=-bound, max=bound).astype(kind)


def gaussian_with(stream_key, shape, width, bound, cuts, heavy, kind=jnp.bfloat16):
    result = width * jax.random.normal(stream_key, shape, jnp.float32)
    if cuts:
        result = result * level_of(stream_key, shape, cuts, -0.22, 0.18)
    return jnp.clip(raised(result, jax.random.fold_in(stream_key, 3), *heavy), -bound, bound).astype(kind)


def setup_inputs(seed: int = 0, part: int = 0) -> dict:
    splits = jax.random.split(jax.random.key(seed), 21)
    part_splits = jax.random.split(jax.random.fold_in(splits[20], part), 21)
    hidden = draw_hidden(jax.random.fold_in(jax.random.fold_in(splits[20], part), 71), part)
    in_gain = jnp.clip(1.0 + 0.18 * jax.random.normal(splits[1], (D,), jnp.float32), 0.1, 1.9)
    z_weight = normal_values(splits[2], (D, INNER), D ** -0.5, 0.125, ((1, 16),))
    x_weight = normal_values(splits[3], (D, INNER), D ** -0.5, 0.125, ((1, 16),))
    bc_weight = normal_values(splits[4], (D, 2 * NS), D ** -0.5, 0.125, ((1, 16),))
    dt_weight = normal_values(splits[5], (D, HEADS), D ** -0.5, 0.125, ((1, 16),))
    conv_x_weight = normal_values(splits[6], (KW, INNER), KW ** -0.5, 3.0, ((1, 16),))
    conv_x_bias = normal_values(splits[7], (INNER,), 0.5, 3.0, ((0, 16),))
    conv_bc_weight = normal_values(splits[8], (KW, 2 * NS), KW ** -0.5, 3.0, ((1, 16),))
    conv_bc_bias = normal_values(splits[9], (2 * NS,), 0.5, 3.0, ((0, 16),))
    conv_x_state = normal_values(part_splits[10], (BATCH, KW - 1, INNER), 1.0, 6.0, ((0, 8), (2, 16)))
    conv_bc_state = normal_values(part_splits[11], (BATCH, KW - 1, 2 * NS), 1.0, 6.0, ((0, 8), (2, 16)))
    dt_bias = jnp.clip(-4.0 + 3.0 * jax.random.uniform(splits[12], (HEADS,), jnp.float32) ** level_of(splits[12], (HEADS,), ((0, 16),), -0.2, 0.2), -4.0, -1.0)
    log_rate = jnp.clip(2.5 * jax.random.uniform(splits[13], (HEADS,), jnp.float32) ** level_of(splits[13], (HEADS,), ((0, 16),), -0.2, 0.2), 0.0, 2.5)
    skip_gain = jnp.clip(0.5 + 1.5 * jax.random.uniform(splits[14], (HEADS,), jnp.float32) ** level_of(splits[14], (HEADS,), ((0, 16),), -0.2, 0.2), 0.5, 2.0)
    ssm_state = draw_ssm_state(jax.random.fold_in(jax.random.fold_in(splits[20], part), 71), part)
    norm_gain = jnp.clip(1.0 + 0.18 * jax.random.normal(splits[16], (INNER,), jnp.float32), 0.1, 1.9)
    out_weight = gaussian_with(splits[17], (INNER, D), INNER ** -0.5, 0.125, ((0, 16),), (0, 1, 16, 2.0))
    pool_slot = draw_pool_slot(jax.random.fold_in(jax.random.fold_in(splits[20], part), 71), part)
    active = place_ends((jax.random.randint(part_splits[19], (BATCH,), 0, 4) < 3).astype(jnp.int32), jax.random.fold_in(part_splits[19], 1), 0, 1)
    return dict(hidden=hidden, in_gain=in_gain, z_weight=z_weight, x_weight=x_weight, bc_weight=bc_weight, dt_weight=dt_weight, conv_x_weight=conv_x_weight, conv_x_bias=conv_x_bias, conv_bc_weight=conv_bc_weight, conv_bc_bias=conv_bc_bias, conv_x_state=conv_x_state, conv_bc_state=conv_bc_state, dt_bias=dt_bias, log_rate=log_rate, skip_gain=skip_gain, ssm_state=ssm_state, norm_gain=norm_gain, out_weight=out_weight, pool_slot=pool_slot, active=active)


def convolve(old_state, current, weight, conv_bias):
    window = jnp.concatenate([old_state.astype(jnp.float32), current.astype(jnp.float32)[:, None, :]], axis=1)
    conv_out = lax.optimization_barrier(jnp.sum(window * weight.astype(jnp.float32)[None], axis=1)) + conv_bias.astype(jnp.float32)
    return (jax.nn.silu(conv_out).astype(jnp.bfloat16), window[:, 1:, :].astype(jnp.bfloat16))

def reference(hidden, in_gain, z_weight, x_weight, bc_weight, dt_weight, conv_x_weight, conv_x_bias, conv_bc_weight, conv_bc_bias, conv_x_state, conv_bc_state, dt_bias, log_rate, skip_gain, ssm_state, norm_gain, out_weight, pool_slot, active):
    pool_row = (pool_slot + (jnp.arange(N_DP, dtype=jnp.int32) * SEQ_DEV)[:, None]).reshape(-1).astype(jnp.int32)
    is_live = active > 0
    hidden_f32 = hidden.astype(jnp.float32)
    inv_rms = lax.rsqrt(lax.optimization_barrier(jnp.mean(hidden_f32 * hidden_f32, axis=1, keepdims=True)) + 1e-05)
    normed = (hidden_f32 * inv_rms * in_gain).astype(jnp.bfloat16)
    z_proj = jnp.dot(normed, z_weight, preferred_element_type=jnp.float32).astype(jnp.bfloat16)
    x_proj = jnp.dot(normed, x_weight, preferred_element_type=jnp.float32).astype(jnp.bfloat16)
    bc_proj = jnp.dot(normed, bc_weight, preferred_element_type=jnp.float32).astype(jnp.bfloat16)
    dt_proj = jnp.dot(normed, dt_weight, preferred_element_type=jnp.float32).astype(jnp.bfloat16)
    x_old = conv_x_state[pool_row]
    bc_old = conv_bc_state[pool_row]
    x_conv, x_kept = convolve(x_old, x_proj, conv_x_weight, conv_x_bias)
    bc_conv, bc_kept = convolve(bc_old, bc_proj, conv_bc_weight, conv_bc_bias)
    conv_x_next = conv_x_state.at[pool_row].set(jnp.where(is_live[:, None, None], x_kept, x_old))
    conv_bc_next = conv_bc_state.at[pool_row].set(jnp.where(is_live[:, None, None], bc_kept, bc_old))
    b_rows = bc_conv[:, :NS].astype(jnp.float32)
    c_rows = bc_conv[:, NS:].astype(jnp.float32)
    dt_step = jax.nn.softplus(dt_proj.astype(jnp.float32) + dt_bias)
    decay_rate = jnp.exp(-dt_step * jnp.exp(log_rate))
    x_heads = x_conv.astype(jnp.float32).reshape(BATCH, HEADS, HP)
    old_state = ssm_state[pool_row]
    fresh_state = decay_rate[:, :, None, None] * old_state + (dt_step[:, :, None] * x_heads)[:, :, :, None] * b_rows[:, None, None, :]
    fresh_state = jnp.where(is_live[:, None, None, None], fresh_state, old_state)
    y_heads = jnp.einsum('bhpn,bn->bhp', fresh_state, c_rows, precision=lax.Precision.HIGHEST) + skip_gain[None, :, None] * x_heads
    gated_y = y_heads.reshape(BATCH, INNER) * jax.nn.silu(z_proj.astype(jnp.float32))
    inv_out = lax.rsqrt(lax.optimization_barrier(jnp.mean(gated_y * gated_y, axis=1)) + 1e-05)
    scaled = (gated_y * norm_gain).astype(jnp.bfloat16)
    branch_sum = jnp.dot(scaled, out_weight, preferred_element_type=jnp.float32)
    layer_out = jnp.where(is_live[:, None], (hidden_f32 + inv_out[:, None] * branch_sum).astype(jnp.bfloat16), hidden)
    ssm_next = ssm_state.at[pool_row].set(fresh_state)
    return (layer_out, conv_x_next, conv_bc_next, ssm_next)
```

```python
import jax
import jax.numpy as jnp
from jax import lax
from jax.experimental import pallas as pl
from jax.experimental.pallas import tpu as pltpu
from jax.sharding import PartitionSpec as P

HP = 64
NS = 128
INNER = 5120
EPS = 1e-05
F32 = jnp.float32
BF16 = jnp.bfloat16
LANES = 128

NT = (((1,), (1,)), ((), ()))


def dot(a, b):
    return jnp.dot(a, b, preferred_element_type=F32)


def dot_nt(a, b):
    return lax.dot_general(a, b, NT, preferred_element_type=F32)


def iota(shape, dim):
    return lax.broadcasted_iota(jnp.int32, shape, dim)


def eye(n):
    return (iota((n, n), 0) == iota((n, n), 1)).astype(F32).astype(BF16)


def silu(x):
    return x * jax.nn.sigmoid(x)


def make_kernel(n_tp, seqs, feats, heads, chans, bc_dev):
    width = n_tp * feats
    tiles = width // LANES
    chips = n_tp // 2
    half = chips // 2
    offsets = []
    for far in range(half, 0, -1):
        for sign in (1, -1) if far < half or chips % 2 else (1,):
            for flip in (1, 0):
                offsets.append((sign * far, flip))
    offsets.append((0, 1))

    def body(
        hid, slot, act, in_gain, z_w, x_w, bc_w, dt_w, cx_w, cx_b, cbc_w, cbc_b, cx_s, cbc_s,
        dt_bias, log_rate, skip_gain, state, norm_gain, out_w,
        out_layer, out_cx, out_cbc, out_state,
        zw, xw, bcw, dtw, cxs, cbcs, st, ow, gain, stb, xn,
        hid_send, hid_recv, bc_send, bc_recv, sq_send, sq_recv, br_send, br_recv,
        in_sem, out_sem, send_sem, recv_sem,
    ):
        me = lax.axis_index("tp")
        chip, core = me // 2, lax.rem(me, 2)

        def partner(step, flip):
            return lax.rem(chip + step + chips, chips) * 2 + lax.rem(core + flip, 2)

        def local(i, src, dst):
            return pltpu.make_async_copy(src, dst, in_sem.at[i])

        barrier = pltpu.get_barrier_semaphore()
        for step, flip in offsets:
            pl.semaphore_signal(
                barrier, inc=1, device_id={"tp": partner(step, flip)}, device_id_type=pl.DeviceIdType.MESH
            )
        loads = [
            local(0, bc_w, bcw),
            local(1, dt_w, dtw),
            local(2, in_gain, gain),
            local(3, cbc_s, cbcs),
            local(4, z_w, zw),
            local(5, x_w, xw),
            local(6, cx_s, cxs),
            local(7, state, st),
            local(8, out_w, ow),
        ]
        for copy in loads:
            copy.start()

        def exchange(phase, src_of, dst_of, to):
            sends = []
            for j, (step, flip) in enumerate(offsets):
                peer = partner(step, flip)
                sends.append(
                    pltpu.make_async_remote_copy(
                        src_ref=src_of(peer), dst_ref=dst_of(me),
                        send_sem=send_sem.at[phase, j], recv_sem=recv_sem.at[phase, j],
                        device_id={"tp": peer}, device_id_type=pl.DeviceIdType.MESH,
                    )
                )
            for copy in sends:
                copy.start()
            return sends

        def arrive(phase, src_of, dst_of):
            for j, (step, flip) in enumerate(offsets):
                source = partner(-step, flip)
                pltpu.make_async_remote_copy(
                    src_ref=src_of(source), dst_ref=dst_of(source),
                    send_sem=send_sem.at[phase, j], recv_sem=recv_sem.at[phase, j],
                    device_id={"tp": source}, device_id_type=pl.DeviceIdType.MESH,
                ).wait_recv()

        slot_row = slot[...]
        act_row = act[...]
        by_slot = iota((seqs, seqs), 0) == jnp.broadcast_to(slot_row, (seqs, seqs))
        to_slot = by_slot.astype(F32).astype(BF16)
        shift = lax.rem(me * feats, LANES)
        place = (iota((feats, 2 * LANES), 1) == iota((feats, 2 * LANES), 0) + shift).astype(F32).astype(BF16)
        mine = dot(to_slot, hid[...]).astype(BF16)
        window = dot(mine, place).astype(BF16)
        hid_send[0] = window[:, :LANES]
        hid_send[1] = window[:, LANES:]
        pl.semaphore_wait(barrier, len(offsets))
        hid_out = exchange(0, lambda peer: hid_send, lambda who: hid_recv.at[who], 0)
        hid_recv[me] = hid_send[...]

        eye16 = eye(seqs)
        to_seq = dot_nt(eye16, to_slot).astype(BF16)
        act_f = act_row.astype(F32)
        live_col = jnp.sum(jnp.where(by_slot, jnp.broadcast_to(act_f, (seqs, seqs)), 0.0), axis=1, keepdims=True) > 0
        act_col = jnp.sum(
            jnp.where(iota((seqs, seqs), 0) == iota((seqs, seqs), 1), jnp.broadcast_to(act_f, (seqs, seqs)), 0.0),
            axis=1, keepdims=True,
        )
        live_row = jnp.sum(to_seq.astype(F32) * act_col, axis=0, keepdims=True) > 0
        eye_ch = eye(chans)
        g0 = norm_gain[...]
        g1 = g0.astype(BF16)
        r1 = g0 - g1.astype(F32)
        g2 = r1.astype(BF16)
        g3 = (r1 - g2.astype(F32)).astype(BF16)
        rows = jnp.concatenate([cx_w[...].astype(F32), cx_b[...].astype(F32), g1.astype(F32), g2.astype(F32), g3.astype(F32)], axis=0)
        cols = dot_nt(eye_ch, rows.astype(BF16))
        gain_col = (cols[:, 5:6] + cols[:, 6:7]) + cols[:, 7:8]
        brows = jnp.concatenate([cbc_w[...].astype(F32), cbc_b[...].astype(F32)], axis=0)
        bcols = dot_nt(eye(bc_dev), brows.astype(BF16))
        loads[3].wait()
        bc_old = [dot_nt(eye(bc_dev), cbcs[k]) for k in range(3)]
        bc_base = (bc_old[0] * bcols[:, 0:1] + bc_old[1] * bcols[:, 1:2]) + bc_old[2] * bcols[:, 2:3]
        loads[6].wait()
        x_old = [dot_nt(eye_ch, cxs[k]) for k in range(3)]
        x_base = (x_old[0] * cols[:, 0:1] + x_old[1] * cols[:, 1:2]) + x_old[2] * cols[:, 2:3]
        loads[7].wait()

        def narrow(b, carry):
            stb[b] = st[b].astype(BF16)
            return carry

        lax.fori_loop(0, seqs, narrow, 0)
        loads[0].wait()
        loads[1].wait()
        loads[2].wait()

        arrive(0, lambda who: hid_send, lambda who: hid_recv.at[who])
        parts = [None] * tiles
        for t in range(n_tp):
            at = (t * feats) // LANES
            for k in range(2):
                piece = hid_recv[t, k].astype(F32)
                parts[at + k] = piece if parts[at + k] is None else parts[at + k] + piece
        squares = parts[0] * parts[0]
        for k in range(1, tiles):
            squares = squares + parts[k] * parts[k]
        inv = lax.rsqrt(jnp.sum(squares, axis=1, keepdims=True) / width + EPS)
        for k in range(tiles):
            xn[:, k * LANES : (k + 1) * LANES] = (parts[k] * inv * gain[k : k + 1, :]).astype(BF16)

        bc_proj = dot_nt(bcw[...], xn[...]).astype(BF16)
        bc_conv = silu(bc_base + bc_proj.astype(F32) * bcols[:, 3:4] + bcols[:, 4:5]).astype(BF16)
        bc_send[...] = jnp.concatenate([bc_conv.astype(F32), jnp.zeros((bc_dev, LANES - seqs), F32)], axis=1).astype(BF16)
        bc_out = exchange(1, lambda peer: bc_send, lambda who: bc_recv.at[who], 0)
        bc_recv[me] = bc_send[...]

        dt_proj = dot_nt(dtw[...], xn[...]).astype(BF16).astype(F32)
        loads[5].wait()
        x_proj = dot_nt(xw[...], xn[...]).astype(BF16)
        loads[4].wait()
        z_proj = dot_nt(zw[...], xn[...]).astype(BF16)
        x_conv = silu(x_base + x_proj.astype(F32) * cols[:, 3:4] + cols[:, 4:5]).astype(BF16).astype(F32)
        z_gate = silu(z_proj.astype(F32))
        steps, decays, skips = [], [], []
        for h in range(heads):
            raw = dt_proj[h : h + 1, :] + dt_bias[h]
            step = jnp.maximum(raw, 0.0) + jnp.log1p(jnp.exp(-jnp.abs(raw)))
            rate = jnp.exp(jnp.full((1, seqs), log_rate[h], F32))
            decay = jnp.exp(-step * rate)
            steps.append(jnp.broadcast_to(jnp.where(live_row, step, 0.0), (HP, seqs)))
            decays.append(jnp.broadcast_to(jnp.where(live_row, decay, 1.0), (HP, seqs)))
            skips.append(jnp.full((HP, seqs), skip_gain[h], F32))
        dtx = jnp.concatenate(steps, axis=0) * x_conv
        decay = jnp.concatenate(decays, axis=0)
        skipped = jnp.concatenate(skips, axis=0) * x_conv
        x_now = dot_nt(eye16, x_proj)
        bc_now = dot_nt(eye16, bc_proj)
        for out, old, now in ((out_cx, cxs, x_now), (out_cbc, cbcs, bc_now)):
            held = [old[k].astype(F32) for k in range(3)]
            for k, new in enumerate((held[1], held[2], now)):
                out[k] = jnp.where(live_col, new, held[k]).astype(BF16)

        arrive(1, lambda who: bc_send, lambda who: bc_recv.at[who])
        groups = NS // bc_dev
        b_t = jnp.concatenate([bc_recv[t] for t in range(groups)], axis=0)[:, :seqs]
        c_t = jnp.concatenate([bc_recv[groups + t] for t in range(groups)], axis=0)[:, :seqs]
        b_f, c_f = b_t.astype(F32), c_t.astype(F32)
        bc_dot = jnp.sum(b_f * c_f, axis=0, keepdims=True)
        lane = iota((NS, seqs), 1)
        c_big = jnp.concatenate([jnp.where(lane == b, c_f, 0.0).astype(BF16) for b in range(seqs)], axis=0)
        s_big = jnp.concatenate([stb[b] for b in range(seqs)], axis=1)
        s_c = dot(s_big, c_big)
        y = (decay * s_c + dtx * bc_dot) + skipped
        gated = y * z_gate
        sq_send[...] = jnp.concatenate([jnp.sum(gated * gated, axis=0, keepdims=True), jnp.zeros((1, LANES - seqs), F32)], axis=1)
        sq_out = exchange(2, lambda peer: sq_send, lambda who: sq_recv.at[who], 0)
        scaled = (gated * gain_col).astype(BF16)
        loads[8].wait()
        rows_seq = dot_nt(to_seq, scaled).astype(BF16)
        branch = dot(rows_seq, ow[...])
        for k in range(tiles):
            br_send[k] = branch[:, k * LANES : (k + 1) * LANES].astype(BF16)

        def first_tile(who):
            return (who * feats) // LANES

        br_out = exchange(
            3, lambda peer: br_send.at[pl.ds(first_tile(peer), 2)], lambda who: br_recv.at[who], 0
        )
        br_recv[me] = br_send[pl.ds(first_tile(me), 2)]
        sq_recv[me] = sq_send[...]

        b_rows = dot_nt(eye16, b_t)
        for b in range(seqs):
            grown = dtx[:, b : b + 1] * b_rows[b : b + 1, :]
            st[b] = decay[:, b : b + 1] * st[b] + grown
        put = pltpu.make_async_copy(st, out_state, out_sem.at[0])
        put.start()

        arrive(2, lambda who: sq_send, lambda who: sq_recv.at[who])
        total_sq = sq_recv[0]
        for t in range(1, n_tp):
            total_sq = total_sq + sq_recv[t]
        sq_row = jnp.broadcast_to(total_sq[:, :seqs], (seqs, seqs))
        sq_col = jnp.sum(jnp.where(to_seq.astype(F32) > 0, sq_row, 0.0), axis=1, keepdims=True)
        inv_out = lax.rsqrt(sq_col / INNER + EPS)
        arrive(3, lambda who: br_send.at[pl.ds(0, 2)], lambda who: br_recv.at[who])
        sums = [br_recv[0, k].astype(F32) for k in range(2)]
        for t in range(1, n_tp):
            sums = [sums[k] + br_recv[t, k].astype(F32) for k in range(2)]
        whole = jnp.concatenate(sums, axis=1)
        branch_sum = pltpu.roll(whole, lax.rem(2 * LANES - shift, 2 * LANES), 1)[:, :feats]
        held = hid[...].astype(F32)
        fresh = (held + inv_out * branch_sum).astype(BF16).astype(F32)
        out_layer[...] = jnp.where(act_col > 0, fresh, held).astype(BF16)
        for copy in hid_out + bc_out + sq_out + br_out:
            copy.wait_send()
        put.wait()

    return body, offsets


def shards(
    hidden, in_gain, z_weight, x_weight, bc_weight, dt_weight, conv_x_weight, conv_x_bias,
    conv_bc_weight, conv_bc_bias, conv_x_state, conv_bc_state, dt_bias, log_rate, skip_gain,
    ssm_state, norm_gain, out_weight, pool_slot, active,
):
    n_tp = lax.axis_size("tp")
    seqs, feats = hidden.shape
    heads = ssm_state.shape[1]
    chans = z_weight.shape[1]
    bc_dev = bc_weight.shape[1]
    width = in_gain.shape[0]
    tiles = width // LANES
    body, offsets = make_kernel(n_tp, seqs, feats, heads, chans, bc_dev)
    vmem = pl.BlockSpec(memory_space=pltpu.VMEM)
    smem = pl.BlockSpec(memory_space=pltpu.SMEM)
    hbm = pl.BlockSpec(memory_space=pl.ANY)
    shape = jax.ShapeDtypeStruct
    out_layer, out_cx, out_cbc, out_state = pl.pallas_call(
        body,
        out_shape=(
            shape((seqs, feats), BF16),
            shape((3, seqs, chans), BF16),
            shape((3, seqs, bc_dev), BF16),
            shape((seqs, chans, NS), F32),
        ),
        in_specs=[
            vmem, vmem, vmem, hbm, hbm, hbm, hbm, hbm, vmem, vmem, vmem, vmem, hbm, hbm,
            smem, smem, smem, hbm, vmem, hbm,
        ],
        out_specs=(vmem, vmem, vmem, hbm),
        scratch_shapes=[
            pltpu.VMEM((chans, width), BF16),
            pltpu.VMEM((chans, width), BF16),
            pltpu.VMEM((bc_dev, width), BF16),
            pltpu.VMEM((heads, width), BF16),
            pltpu.VMEM((3, seqs, chans), BF16),
            pltpu.VMEM((3, seqs, bc_dev), BF16),
            pltpu.VMEM((seqs, chans, NS), F32),
            pltpu.VMEM((chans, width), BF16),
            pltpu.VMEM((tiles, LANES), F32),
            pltpu.VMEM((seqs, chans, NS), BF16),
            pltpu.VMEM((seqs, width), BF16),
            pltpu.VMEM((2, seqs, LANES), BF16),
            pltpu.VMEM((n_tp, 2, seqs, LANES), BF16),
            pltpu.VMEM((bc_dev, LANES), BF16),
            pltpu.VMEM((n_tp, bc_dev, LANES), BF16),
            pltpu.VMEM((1, LANES), F32),
            pltpu.VMEM((n_tp, 1, LANES), F32),
            pltpu.VMEM((tiles, seqs, LANES), BF16),
            pltpu.VMEM((n_tp, 2, seqs, LANES), BF16),
            pltpu.SemaphoreType.DMA((9,)),
            pltpu.SemaphoreType.DMA((1,)),
            pltpu.SemaphoreType.DMA((4, len(offsets))),
            pltpu.SemaphoreType.DMA((4, len(offsets))),
        ],
        compiler_params=pltpu.CompilerParams(
            collective_id=0, has_side_effects=True, vmem_limit_bytes=60 * 1024 * 1024
        ),
        name="step",
    )(
        hidden, pool_slot, active.reshape(1, seqs), in_gain.reshape(tiles, LANES),
        z_weight.T, x_weight.T, bc_weight.T, dt_weight.T,
        conv_x_weight, conv_x_bias.reshape(1, chans), conv_bc_weight, conv_bc_bias.reshape(1, bc_dev),
        conv_x_state.transpose(1, 0, 2), conv_bc_state.transpose(1, 0, 2),
        dt_bias, log_rate, skip_gain, ssm_state.reshape(seqs, chans, NS),
        norm_gain.reshape(1, chans), out_weight,
    )
    return (
        out_layer,
        out_cx.transpose(1, 0, 2),
        out_cbc.transpose(1, 0, 2),
        out_state.reshape(ssm_state.shape),
    )


def solution(mesh):
    rows = ("groups", "dp")
    placed = (
        P(rows, "tp"), P(), P(None, "tp"), P(None, "tp"), P(None, "tp"), P(None, "tp"), P(None, "tp"),
        P("tp"), P(None, "tp"), P("tp"), P(rows, None, "tp"), P(rows, None, "tp"), P("tp"), P("tp"),
        P("tp"), P(rows, "tp", None, None), P("tp"), P("tp", None), P(rows, None), P(rows),
    )
    return jax.shard_map(
        shards,
        mesh=mesh,
        in_specs=placed,
        out_specs=(P(rows, "tp"), P(rows, None, "tp"), P(rows, None, "tp"), P(rows, "tp", None, None)),
        check_vma=False,
    )
```

```python
import jax
import jax.numpy as jnp
from jax import lax
from jax.experimental import pallas as pl
from jax.experimental.pallas import tpu as pltpu
from jax.sharding import PartitionSpec as P

HP = 64
NS = 128
INNER = 5120
EPS = 1e-05
F32 = jnp.float32
BF16 = jnp.bfloat16
LANES = 128

NT = (((1,), (1,)), ((), ()))


def dot(a, b):
    return jnp.dot(a, b, preferred_element_type=F32)


def dot_nt(a, b):
    return lax.dot_general(a, b, NT, preferred_element_type=F32)


def iota(shape, dim):
    return lax.broadcasted_iota(jnp.int32, shape, dim)


def eye(n):
    return (iota((n, n), 0) == iota((n, n), 1)).astype(F32).astype(BF16)


def silu(x):
    return x * jax.nn.sigmoid(x)


def put_out(*refs):
    sems = refs[-1]
    copies = [pltpu.make_async_copy(refs[k], refs[4 + k], sems.at[k]) for k in (3, 0, 1, 2)]
    for copy in copies:
        copy.start()
    for copy in copies:
        copy.wait()


def make_kernel(n_tp, seqs, feats, heads, chans, bc_dev):
    width = n_tp * feats
    tiles = width // LANES
    chips = n_tp // 2
    half = chips // 2
    offsets = []
    for far in range(half, 0, -1):
        for sign in (1, -1) if far < half or chips % 2 else (1,):
            for flip in (1, 0):
                offsets.append((sign * far, flip))
    offsets.append((0, 1))

    def body(
        hid, slot, act, in_gain, z_w, x_w, bc_w, dt_w, cx_w, cx_b, cbc_w, cbc_b, cx_s, cbc_s,
        dt_bias, log_rate, skip_gain, state, norm_gain, out_w,
        out_layer, out_cx, out_cbc, out_state,
        zw, xw, bcw, dtw, cxs, cbcs, st, ow, gain, stb, xn,
        hid_send, hid_recv, bc_send, bc_recv, sq_send, sq_recv, br_send, br_recv,
        in_sem, send_sem, recv_sem,
    ):
        me = lax.axis_index("tp")
        chip, core = me // 2, lax.rem(me, 2)

        def partner(step, flip):
            return lax.rem(chip + step + chips, chips) * 2 + lax.rem(core + flip, 2)

        def local(i, src, dst):
            return pltpu.make_async_copy(src, dst, in_sem.at[i])

        barrier = pltpu.get_barrier_semaphore()
        for step, flip in offsets:
            pl.semaphore_signal(
                barrier, inc=1, device_id={"tp": partner(step, flip)}, device_id_type=pl.DeviceIdType.MESH
            )
        loads = [
            local(0, bc_w, bcw),
            local(1, dt_w, dtw),
            local(2, in_gain, gain),
            local(3, cbc_s, cbcs),
            local(4, z_w, zw),
            local(5, x_w, xw),
            local(6, cx_s, cxs),
            local(7, state, st),
            local(8, out_w, ow),
        ]
        for copy in loads:
            copy.start()

        def exchange(phase, src_of, dst_of, to):
            sends = []
            for j, (step, flip) in enumerate(offsets):
                peer = partner(step, flip)
                sends.append(
                    pltpu.make_async_remote_copy(
                        src_ref=src_of(peer), dst_ref=dst_of(me),
                        send_sem=send_sem.at[phase, j], recv_sem=recv_sem.at[phase, j],
                        device_id={"tp": peer}, device_id_type=pl.DeviceIdType.MESH,
                    )
                )
            for copy in sends:
                copy.start()
            return sends

        def arrive(phase, src_of, dst_of):
            for j, (step, flip) in enumerate(offsets):
                source = partner(-step, flip)
                pltpu.make_async_remote_copy(
                    src_ref=src_of(source), dst_ref=dst_of(source),
                    send_sem=send_sem.at[phase, j], recv_sem=recv_sem.at[phase, j],
                    device_id={"tp": source}, device_id_type=pl.DeviceIdType.MESH,
                ).wait_recv()

        slot_row = slot[...]
        act_row = act[...]
        by_slot = iota((seqs, seqs), 0) == jnp.broadcast_to(slot_row, (seqs, seqs))
        to_slot = by_slot.astype(F32).astype(BF16)
        shift = lax.rem(me * feats, LANES)
        place = (iota((feats, 2 * LANES), 1) == iota((feats, 2 * LANES), 0) + shift).astype(F32).astype(BF16)
        mine = dot(to_slot, hid[...]).astype(BF16)
        window = dot(mine, place).astype(BF16)
        hid_send[0] = window[:, :LANES]
        hid_send[1] = window[:, LANES:]
        pl.semaphore_wait(barrier, len(offsets))
        hid_out = exchange(0, lambda peer: hid_send, lambda who: hid_recv.at[who], 0)
        hid_recv[me] = hid_send[...]

        eye16 = eye(seqs)
        to_seq = dot_nt(eye16, to_slot).astype(BF16)
        act_f = act_row.astype(F32)
        live_col = jnp.sum(jnp.where(by_slot, jnp.broadcast_to(act_f, (seqs, seqs)), 0.0), axis=1, keepdims=True) > 0
        act_col = jnp.sum(
            jnp.where(iota((seqs, seqs), 0) == iota((seqs, seqs), 1), jnp.broadcast_to(act_f, (seqs, seqs)), 0.0),
            axis=1, keepdims=True,
        )
        live_row = jnp.sum(to_seq.astype(F32) * act_col, axis=0, keepdims=True) > 0
        eye_ch = eye(chans)
        g0 = norm_gain[...].reshape(1, chans)
        g1 = g0.astype(BF16)
        r1 = g0 - g1.astype(F32)
        g2 = r1.astype(BF16)
        g3 = (r1 - g2.astype(F32)).astype(BF16)
        rows = jnp.concatenate([cx_w[...].astype(F32), cx_b[...].astype(F32).reshape(1, chans), g1.astype(F32), g2.astype(F32), g3.astype(F32)], axis=0)
        cols = dot_nt(eye_ch, rows.astype(BF16))
        gain_col = (cols[:, 5:6] + cols[:, 6:7]) + cols[:, 7:8]
        brows = jnp.concatenate([cbc_w[...].astype(F32), cbc_b[...].astype(F32)], axis=0)
        bcols = dot_nt(eye(bc_dev), brows.astype(BF16))
        loads[3].wait()
        bc_old = [dot_nt(eye(bc_dev), cbcs[k]) for k in range(3)]
        bc_base = (bc_old[0] * bcols[:, 0:1] + bc_old[1] * bcols[:, 1:2]) + bc_old[2] * bcols[:, 2:3]
        loads[6].wait()
        x_old = [dot_nt(eye_ch, cxs[k]) for k in range(3)]
        x_base = (x_old[0] * cols[:, 0:1] + x_old[1] * cols[:, 1:2]) + x_old[2] * cols[:, 2:3]
        loads[7].wait()

        def narrow(b, carry):
            stb[b] = st[b].astype(BF16)
            return carry

        lax.fori_loop(0, seqs, narrow, 0)
        loads[0].wait()
        loads[1].wait()
        loads[2].wait()

        arrive(0, lambda who: hid_send, lambda who: hid_recv.at[who])
        parts = [None] * tiles
        for t in range(n_tp):
            at = (t * feats) // LANES
            for k in range(2):
                piece = hid_recv[t, k].astype(F32)
                parts[at + k] = piece if parts[at + k] is None else parts[at + k] + piece
        squares = parts[0] * parts[0]
        for k in range(1, tiles):
            squares = squares + parts[k] * parts[k]
        inv = lax.rsqrt(jnp.sum(squares, axis=1, keepdims=True) / width + EPS)
        for k in range(tiles):
            xn[:, k * LANES : (k + 1) * LANES] = (parts[k] * inv * gain[k : k + 1, :]).astype(BF16)

        bc_proj = dot_nt(bcw[...], xn[...]).astype(BF16)
        bc_conv = silu(bc_base + bc_proj.astype(F32) * bcols[:, 3:4] + bcols[:, 4:5]).astype(BF16)
        bc_send[...] = jnp.concatenate([bc_conv.astype(F32), jnp.zeros((bc_dev, LANES - seqs), F32)], axis=1).astype(BF16)
        bc_out = exchange(1, lambda peer: bc_send, lambda who: bc_recv.at[who], 0)
        bc_recv[me] = bc_send[...]

        dt_proj = dot_nt(dtw[...], xn[...]).astype(BF16).astype(F32)
        loads[5].wait()
        x_proj = dot_nt(xw[...], xn[...]).astype(BF16)
        loads[4].wait()
        z_proj = dot_nt(zw[...], xn[...]).astype(BF16)
        x_conv = silu(x_base + x_proj.astype(F32) * cols[:, 3:4] + cols[:, 4:5]).astype(BF16).astype(F32)
        z_gate = silu(z_proj.astype(F32))
        steps, decays, skips = [], [], []
        for h in range(heads):
            raw = dt_proj[h : h + 1, :] + dt_bias[h]
            step = jnp.maximum(raw, 0.0) + jnp.log1p(jnp.exp(-jnp.abs(raw)))
            rate = jnp.exp(jnp.full((1, seqs), log_rate[h], F32))
            decay = jnp.exp(-step * rate)
            steps.append(jnp.broadcast_to(jnp.where(live_row, step, 0.0), (HP, seqs)))
            decays.append(jnp.broadcast_to(jnp.where(live_row, decay, 1.0), (HP, seqs)))
            skips.append(jnp.full((HP, seqs), skip_gain[h], F32))
        dtx = jnp.concatenate(steps, axis=0) * x_conv
        decay = jnp.concatenate(decays, axis=0)
        skipped = jnp.concatenate(skips, axis=0) * x_conv
        x_now = dot_nt(eye16, x_proj)
        bc_now = dot_nt(eye16, bc_proj)
        for out, old, now in ((out_cx, cxs, x_now), (out_cbc, cbcs, bc_now)):
            held = [old[k].astype(F32) for k in range(3)]
            for k, new in enumerate((held[1], held[2], now)):
                out[k] = jnp.where(live_col, new, held[k]).astype(BF16)

        arrive(1, lambda who: bc_send, lambda who: bc_recv.at[who])
        groups = NS // bc_dev
        b_t = jnp.concatenate([bc_recv[t] for t in range(groups)], axis=0)[:, :seqs]
        c_t = jnp.concatenate([bc_recv[groups + t] for t in range(groups)], axis=0)[:, :seqs]
        b_f, c_f = b_t.astype(F32), c_t.astype(F32)
        bc_dot = jnp.sum(b_f * c_f, axis=0, keepdims=True)
        lane = iota((NS, seqs), 1)
        c_big = jnp.concatenate([jnp.where(lane == b, c_f, 0.0).astype(BF16) for b in range(seqs)], axis=0)
        s_big = jnp.concatenate([stb[b] for b in range(seqs)], axis=1)
        s_c = dot(s_big, c_big)
        y = (decay * s_c + dtx * bc_dot) + skipped
        gated = y * z_gate
        sq_send[...] = jnp.concatenate([jnp.sum(gated * gated, axis=0, keepdims=True), jnp.zeros((1, LANES - seqs), F32)], axis=1)
        sq_out = exchange(2, lambda peer: sq_send, lambda who: sq_recv.at[who], 0)
        scaled = (gated * gain_col).astype(BF16)
        loads[8].wait()
        rows_seq = dot_nt(to_seq, scaled).astype(BF16)
        branch = dot(rows_seq, ow[...])
        for k in range(tiles):
            br_send[k] = branch[:, k * LANES : (k + 1) * LANES].astype(BF16)

        def first_tile(who):
            return (who * feats) // LANES

        br_out = exchange(
            3, lambda peer: br_send.at[pl.ds(first_tile(peer), 2)], lambda who: br_recv.at[who], 0
        )
        br_recv[me] = br_send[pl.ds(first_tile(me), 2)]
        sq_recv[me] = sq_send[...]

        b_rows = dot_nt(eye16, b_t)
        for b in range(seqs):
            grown = dtx[:, b : b + 1] * b_rows[b : b + 1, :]
            out_state[b] = decay[:, b : b + 1] * st[b] + grown

        arrive(2, lambda who: sq_send, lambda who: sq_recv.at[who])
        total_sq = sq_recv[0]
        for t in range(1, n_tp):
            total_sq = total_sq + sq_recv[t]
        sq_row = jnp.broadcast_to(total_sq[:, :seqs], (seqs, seqs))
        sq_col = jnp.sum(jnp.where(to_seq.astype(F32) > 0, sq_row, 0.0), axis=1, keepdims=True)
        inv_out = lax.rsqrt(sq_col / INNER + EPS)
        arrive(3, lambda who: br_send.at[pl.ds(0, 2)], lambda who: br_recv.at[who])
        sums = [br_recv[0, k].astype(F32) for k in range(2)]
        for t in range(1, n_tp):
            sums = [sums[k] + br_recv[t, k].astype(F32) for k in range(2)]
        whole = jnp.concatenate(sums, axis=1)
        branch_sum = pltpu.roll(whole, lax.rem(2 * LANES - shift, 2 * LANES), 1)[:, :feats]
        held = hid[...].astype(F32)
        fresh = (held + inv_out * branch_sum).astype(BF16).astype(F32)
        out_layer[...] = jnp.where(act_col > 0, fresh, held).astype(BF16)
        for copy in hid_out + bc_out + sq_out + br_out:
            copy.wait_send()

    return body, offsets


def shards(
    hidden, in_gain, z_weight, x_weight, bc_weight, dt_weight, conv_x_weight, conv_x_bias,
    conv_bc_weight, conv_bc_bias, conv_x_state, conv_bc_state, dt_bias, log_rate, skip_gain,
    ssm_state, norm_gain, out_weight, pool_slot, active,
):
    n_tp = lax.axis_size("tp")
    seqs, feats = hidden.shape
    heads = ssm_state.shape[1]
    chans = z_weight.shape[1]
    bc_dev = bc_weight.shape[1]
    width = in_gain.shape[0]
    tiles = width // LANES
    body, offsets = make_kernel(n_tp, seqs, feats, heads, chans, bc_dev)
    vmem = pl.BlockSpec(memory_space=pltpu.VMEM)
    smem = pl.BlockSpec(memory_space=pltpu.SMEM)
    hbm = pl.BlockSpec(memory_space=pl.ANY)
    shape = jax.ShapeDtypeStruct
    results = (
        ((seqs, feats), BF16),
        ((3, seqs, chans), BF16),
        ((3, seqs, bc_dev), BF16),
        ((seqs, chans, NS), F32),
    )
    made = pl.pallas_call(
        body,
        out_shape=tuple(pltpu.VMEM(dims, kind) for dims, kind in results),
        in_specs=[
            vmem, vmem, vmem, hbm, hbm, hbm, hbm, hbm, vmem, vmem, vmem, vmem, hbm, hbm,
            smem, smem, smem, hbm, vmem, hbm,
        ],
        out_specs=(vmem,) * 4,
        scratch_shapes=[
            pltpu.VMEM((chans, width), BF16),
            pltpu.VMEM((chans, width), BF16),
            pltpu.VMEM((bc_dev, width), BF16),
            pltpu.VMEM((heads, width), BF16),
            pltpu.VMEM((3, seqs, chans), BF16),
            pltpu.VMEM((3, seqs, bc_dev), BF16),
            pltpu.VMEM((seqs, chans, NS), F32),
            pltpu.VMEM((chans, width), BF16),
            pltpu.VMEM((tiles, LANES), F32),
            pltpu.VMEM((seqs, chans, NS), BF16),
            pltpu.VMEM((seqs, width), BF16),
            pltpu.VMEM((2, seqs, LANES), BF16),
            pltpu.VMEM((n_tp, 2, seqs, LANES), BF16),
            pltpu.VMEM((bc_dev, LANES), BF16),
            pltpu.VMEM((n_tp, bc_dev, LANES), BF16),
            pltpu.VMEM((1, LANES), F32),
            pltpu.VMEM((n_tp, 1, LANES), F32),
            pltpu.VMEM((tiles, seqs, LANES), BF16),
            pltpu.VMEM((n_tp, 2, seqs, LANES), BF16),
            pltpu.SemaphoreType.DMA((9,)),
            pltpu.SemaphoreType.DMA((4, len(offsets))),
            pltpu.SemaphoreType.DMA((4, len(offsets))),
        ],
        compiler_params=pltpu.CompilerParams(
            collective_id=0, has_side_effects=True, vmem_limit_bytes=60 * 1024 * 1024
        ),
        name="step",
    )(
        hidden, pool_slot, active.reshape(1, seqs), in_gain.reshape(tiles, LANES),
        z_weight.T, x_weight.T, bc_weight.T, dt_weight.T,
        conv_x_weight, conv_x_bias, conv_bc_weight, conv_bc_bias.reshape(1, bc_dev),
        conv_x_state.transpose(1, 0, 2), conv_bc_state.transpose(1, 0, 2),
        dt_bias, log_rate, skip_gain, ssm_state.reshape(seqs, chans, NS),
        norm_gain, out_weight,
    )
    out_layer, out_cx, out_cbc, out_state = pl.pallas_call(
        put_out,
        out_shape=tuple(shape(dims, kind) for dims, kind in results),
        in_specs=[vmem] * 4,
        out_specs=(hbm,) * 4,
        scratch_shapes=[pltpu.SemaphoreType.DMA((4,))],
        name="put",
    )(*(pltpu.with_memory_space_constraint(x, pltpu.VMEM) for x in made))
    return (
        out_layer,
        out_cx.transpose(1, 0, 2),
        out_cbc.transpose(1, 0, 2),
        out_state.reshape(ssm_state.shape),
    )


def solution(mesh):
    rows = ("groups", "dp")
    placed = (
        P(rows, "tp"), P(), P(None, "tp"), P(None, "tp"), P(None, "tp"), P(None, "tp"), P(None, "tp"),
        P("tp"), P(None, "tp"), P("tp"), P(rows, None, "tp"), P(rows, None, "tp"), P("tp"), P("tp"),
        P("tp"), P(rows, "tp", None, None), P("tp"), P("tp", None), P(rows, None), P(rows),
    )
    return jax.shard_map(
        shards,
        mesh=mesh,
        in_specs=placed,
        out_specs=(P(rows, "tp"), P(rows, None, "tp"), P(rows, None, "tp"), P(rows, "tp", None, None)),
        check_vma=False,
    )
```

```python
import jax
import jax.numpy as jnp
from jax import lax
from jax.experimental import pallas as pl
from jax.experimental.pallas import tpu as pltpu
from jax.sharding import PartitionSpec as P

HP = 64
NS = 128
INNER = 5120
EPS = 1e-05
F32 = jnp.float32
BF16 = jnp.bfloat16
LANES = 128
SUBS = 8

NT = (((1,), (1,)), ((), ()))
MESH = pl.DeviceIdType.MESH


def dot(a, b):
    return jnp.dot(a, b, preferred_element_type=F32)


def dot_nt(a, b):
    return lax.dot_general(a, b, NT, preferred_element_type=F32)


def iota(shape, dim):
    return lax.broadcasted_iota(jnp.int32, shape, dim)


def one_hot(mask):
    return mask.astype(F32).astype(BF16)


def eye(n):
    return one_hot(iota((n, n), 0) == iota((n, n), 1))


def silu(x):
    return x * jax.nn.sigmoid(x)


def exact_dot(x, picks):
    first = x.astype(BF16)
    rest = x - first.astype(F32)
    second = rest.astype(BF16)
    third = (rest - second.astype(F32)).astype(BF16)
    return (dot(first, picks) + dot(second, picks)) + dot(third, picks)


def put_out(*refs):
    sems = refs[-1]
    copies = [pltpu.make_async_copy(refs[k], refs[4 + k], sems.at[k]) for k in (3, 0, 1, 2)]
    for copy in copies:
        copy.start()
    for copy in copies:
        copy.wait()


def make_kernel(n_tp, seqs, feats, heads, chans, bc_dev):
    width = n_tp * feats
    tiles = width // LANES
    chips = n_tp // 2
    half = chips // 2
    steps_far = [half]
    for far in range(half - 1, 0, -1):
        steps_far += [far, chips - far]
    partners = [(step, flip) for step in steps_far for flip in (1, 0)] + [(0, 1)]
    others = len(partners)

    def body(
        hid, slot, act, in_gain, z_w, x_w, bc_w, dt_w, cx_w, cx_b, cbc_w, cbc_b, cx_s, cbc_s,
        dt_bias, log_rate, skip_gain, state, norm_gain, out_w,
        out_layer, out_cx, out_cbc, out_state,
        zw, xw, bcw, dtw, cxs, cbcs, st, ow, gain, slot_v, slot_m, act_v, cxw, cxb, cbcw, cbcb, ngain,
        dtb_m, rate_m, skip_m,
        stb, xn, hid_recv, bc_send, bc_recv, sq_send, sq_recv, br_send, br_recv,
        in_sem, send_sem, recv_sem, relay_sem,
    ):
        me = lax.axis_index("tp")
        chip, core = me // 2, lax.rem(me, 2)
        barrier = pltpu.get_barrier_semaphore()

        def device(step, which):
            return {"tp": lax.rem(chip + step, chips) * 2 + which}

        loads = {}

        def load(name, src, dst):
            loads[name] = pltpu.make_async_copy(src, dst, in_sem.at[len(loads)])
            loads[name].start()

        load("hid", hid, hid_recv.at[core])

        @pl.when(core == 0)
        def _():
            pl.semaphore_signal(barrier, inc=1, device_id=device(0, 1), device_id_type=MESH)

        @pl.when(core == 1)
        def _():
            for step in steps_far:
                pl.semaphore_signal(barrier, inc=1, device_id=device(step, 1), device_id_type=MESH)

        load("slot", slot, slot_v)
        load("slot_m", slot, slot_m)
        load("act", act, act_v)
        load("bc_w", bc_w, bcw)
        load("in_gain", in_gain, gain)
        load("cbc_s", cbc_s, cbcs)
        load("cbc_w", cbc_w, cbcw)
        load("cbc_b", cbc_b, cbcb)
        load("dt_w", dt_w, dtw)
        load("cx_s", cx_s, cxs)
        load("cx_w", cx_w, cxw)
        load("cx_b", cx_b, cxb)
        load("norm_gain", norm_gain, ngain)
        load("dt_bias", dt_bias, dtb_m)
        load("log_rate", log_rate, rate_m)
        load("skip_gain", skip_gain, skip_m)
        load("state", state, st)
        load("x_w", x_w, xw)
        load("z_w", z_w, zw)
        load("out_w", out_w, ow)

        def first_send(step, which, dst_slot):
            return pltpu.make_async_remote_copy(
                src_ref=hid_recv.at[core], dst_ref=hid_recv.at[dst_slot],
                send_sem=send_sem.at[0], recv_sem=recv_sem.at[0],
                device_id=device(step, which), device_id_type=MESH,
            )

        def relay():
            return pltpu.make_async_remote_copy(
                src_ref=hid_recv.at[pl.ds(1, n_tp - 1)], dst_ref=hid_recv.at[pl.ds(1, n_tp - 1)],
                send_sem=relay_sem.at[0], recv_sem=recv_sem.at[0],
                device_id=device(0, 0), device_id_type=MESH,
            )

        @pl.when(core == 0)
        def _():
            loads["hid"].wait()
            pl.semaphore_wait(barrier, 1)
            for step in steps_far:
                first_send(step, 1, 2 * (chips - step)).start()
            first_send(0, 1, 0).start()

        @pl.when(core == 1)
        def _():
            loads["hid"].wait()
            pl.semaphore_wait(barrier, chips)
            pl.semaphore_signal(barrier, inc=1, device_id=device(0, 0), device_id_type=MESH)
            for step in steps_far:
                first_send(step, 1, 2 * (chips - step) + 1).start()

        for name in ("slot", "slot_m", "act", "in_gain", "cbc_s", "cbc_w", "cbc_b"):
            loads[name].wait()
        slot_row = slot_v[...]
        by_slot = iota((seqs, seqs), 0) == jnp.broadcast_to(slot_row, (seqs, seqs))
        to_slot = one_hot(by_slot)
        eye16 = eye(seqs)
        diagonal = iota((seqs, seqs), 0) == iota((seqs, seqs), 1)
        to_seq = dot_nt(eye16, to_slot).astype(BF16)
        act_f = jnp.broadcast_to(act_v[...].astype(F32), (seqs, seqs))
        live_row = act_v[...] > 0
        act_col = jnp.sum(jnp.where(diagonal, act_f, 0.0), axis=1, keepdims=True) > 0
        live_slot = jnp.sum(jnp.where(by_slot, act_f, 0.0), axis=1, keepdims=True) > 0
        bc_rows = jnp.concatenate([cbcw[...].astype(F32), cbcb[...].astype(F32)], axis=0)
        row_at, col_at = iota((bc_dev, bc_dev), 0), iota((bc_dev, bc_dev), 1)
        mirror = one_hot(col_at == row_at // SUBS * SUBS + lax.rem(SUBS - lax.rem(row_at, SUBS), SUBS))
        bc_cols = dot_nt(mirror, bc_rows.astype(BF16))
        bc_old = [dot_nt(mirror, dot(to_seq, cbcs[k]).astype(BF16)) for k in range(3)]
        bc_base = (bc_old[0] * bc_cols[:, 0:1] + bc_old[1] * bc_cols[:, 1:2]) + bc_old[2] * bc_cols[:, 2:3]
        for name in ("cx_s", "cx_w", "cx_b", "norm_gain", "dt_bias", "log_rate", "skip_gain"):
            loads[name].wait()
        eye_ch = eye(chans)
        g0 = ngain[...].reshape(1, chans)
        g1 = g0.astype(BF16).astype(F32)
        g2 = (g0 - g1).astype(BF16).astype(F32)
        g3 = (g0 - g1) - g2
        rows = jnp.concatenate([cxw[...].astype(F32), cxb[...].astype(F32).reshape(1, chans), g1, g2, g3], axis=0)
        cols = dot_nt(eye_ch, rows.astype(BF16))
        gain_col = (cols[:, 5:6] + cols[:, 6:7]) + cols[:, 7:8]
        x_old = [dot_nt(eye_ch, dot(to_seq, cxs[k]).astype(BF16)) for k in range(3)]
        x_base = (x_old[0] * cols[:, 0:1] + x_old[1] * cols[:, 1:2]) + x_old[2] * cols[:, 2:3]
        loads["state"].wait()

        def narrow(i, carry):
            stb[i] = st[slot_m[0, i]].astype(BF16)
            return carry

        lax.fori_loop(0, seqs, narrow, 0)
        for name in ("bc_w", "dt_w"):
            loads[name].wait()
        bcw[...] = dot(mirror, bcw[...]).astype(BF16)

        pltpu.make_async_remote_copy(
            src_ref=hid_recv.at[pl.ds(1, n_tp - 1)], dst_ref=hid_recv.at[pl.ds(1, n_tp - 1)],
            send_sem=send_sem.at[0], recv_sem=recv_sem.at[0],
            device_id=device(0, 1 - core), device_id_type=MESH,
        ).wait_recv()

        @pl.when(core == 1)
        def _():
            relay().start()

        blocks = [
            hid_recv[2 * lax.rem(t // 2 - chip + chips, chips) + t % 2].astype(F32) for t in range(n_tp)
        ]
        whole = jnp.concatenate(blocks, axis=1)
        squares = whole[:, :LANES] * whole[:, :LANES]
        for k in range(1, tiles):
            part = whole[:, k * LANES : (k + 1) * LANES]
            squares = squares + part * part
        inv = lax.rsqrt(jnp.sum(squares, axis=1, keepdims=True) / width + EPS)
        for k in range(tiles):
            at = slice(k * LANES, (k + 1) * LANES)
            xn[:, at] = (whole[:, at] * inv * gain[k : k + 1, :]).astype(BF16)

        bc_proj = dot_nt(bcw[...], xn[...]).astype(BF16)
        bc_conv = silu(bc_base + bc_proj.astype(F32) * bc_cols[:, 3:4] + bc_cols[:, 4:5]).astype(BF16).astype(F32)
        spread = jnp.concatenate([bc_conv, jnp.zeros((bc_dev, LANES - seqs), F32)], axis=1)
        spread = pltpu.roll(spread, 0, 1, stride=seqs, stride_axis=0)
        bc_send[...] = jnp.sum(spread.reshape(bc_dev // SUBS, SUBS, LANES), axis=1)

        def exchange(phase, src_of, dst_ref):
            for step, flip in partners:
                peer = lax.rem(chip + step, chips) * 2 + (lax.rem(core + 1, 2) if flip else core)
                pltpu.make_async_remote_copy(
                    src_ref=src_of(peer), dst_ref=dst_ref.at[me],
                    send_sem=send_sem.at[phase], recv_sem=recv_sem.at[phase],
                    device_id={"tp": peer}, device_id_type=MESH,
                ).start()

        def all_of(phase, dst_ref):
            return pltpu.make_async_remote_copy(
                src_ref=dst_ref.at[pl.ds(0, others)], dst_ref=dst_ref.at[pl.ds(0, others)],
                send_sem=send_sem.at[phase], recv_sem=recv_sem.at[phase],
                device_id=device(0, 1 - core), device_id_type=MESH,
            )

        exchange(1, lambda peer: bc_send, bc_recv)
        bc_recv[me] = bc_send[...]

        dt_proj = dot_nt(dtw[...], xn[...]).astype(BF16).astype(F32)
        loads["x_w"].wait()
        x_proj = dot_nt(xw[...], xn[...]).astype(BF16)
        loads["z_w"].wait()
        z_proj = dot_nt(zw[...], xn[...]).astype(BF16)
        x_conv = silu(x_base + x_proj.astype(F32) * cols[:, 3:4] + cols[:, 4:5]).astype(BF16)
        x_f = x_conv.astype(F32)
        z_gate = silu(z_proj.astype(F32))
        steps, decays = [], []
        for h in range(heads):
            raw = dt_proj[h : h + 1, :] + dtb_m[h]
            step = jnp.maximum(raw, 0.0) + jnp.log1p(jnp.exp(-jnp.abs(raw)))
            rate = jnp.exp(jnp.full((1, seqs), rate_m[h], F32))
            steps.append(jnp.where(live_row, step, 0.0))
            decays.append(jnp.where(live_row, jnp.exp(-step * rate), 1.0))

        def per_channel(values):
            return jnp.concatenate([jnp.broadcast_to(v, (HP, seqs)) for v in values], axis=0)

        dtx = per_channel(steps) * x_f
        decay = per_channel(decays)
        skipped = jnp.concatenate([jnp.full((HP, seqs), skip_m[h], F32) for h in range(heads)], axis=0) * x_f

        all_of(1, bc_recv).wait_recv()

        def unpacked(at):
            found = []
            for row in range(NS // SUBS):
                line = at // SUBS + row
                packed = bc_recv[line // (bc_dev // SUBS), pl.ds(line % (bc_dev // SUBS), 1), :]
                found.append(
                    pltpu.roll(jnp.broadcast_to(packed, (SUBS, LANES)), 0, 1, stride=seqs, stride_axis=0)
                )
            return jnp.concatenate(found, axis=0)[:, :seqs]

        c_f, b_f = unpacked(NS), unpacked(0)
        lane = iota((NS, seqs), 1)
        c_big = jnp.concatenate([jnp.where(lane == b, c_f, 0.0).astype(BF16) for b in range(seqs)], axis=0)
        s_big = jnp.concatenate([stb[b] for b in range(seqs)], axis=1)
        s_c = dot(s_big, c_big)
        bc_dot = jnp.sum(b_f * c_f, axis=0, keepdims=True)
        y = (decay * s_c + dtx * bc_dot) + skipped
        gated = y * z_gate
        scaled = (gated * gain_col).astype(BF16)
        sq_send[...] = jnp.concatenate(
            [jnp.sum(gated * gated, axis=0, keepdims=True), jnp.zeros((1, LANES - seqs), F32)], axis=1
        )
        exchange(2, lambda peer: sq_send, sq_recv)
        loads["out_w"].wait()
        branch = dot(dot_nt(eye16, scaled).astype(BF16), ow[...])
        for k in range(tiles):
            br_send[k] = branch[:, k * LANES : (k + 1) * LANES].astype(BF16)

        def first_tile(who):
            return (who * feats) // LANES

        exchange(3, lambda peer: br_send.at[pl.ds(first_tile(peer), 2)], br_recv)
        br_recv[me] = br_send[pl.ds(first_tile(me), 2)]
        sq_recv[me] = sq_send[...]

        x_now = dot_nt(to_slot, x_proj)
        bc_now = dot(dot_nt(to_slot, bc_proj).astype(BF16), mirror)
        for out, old, now in ((out_cx, cxs, x_now), (out_cbc, cbcs, bc_now)):
            held = [old[k].astype(F32) for k in range(3)]
            for k, new in enumerate((held[1], held[2], now)):
                out[k] = jnp.where(live_slot, new, held[k]).astype(BF16)
        of_heads = jnp.concatenate(steps + decays + [jnp.zeros((-2 * heads % SUBS, seqs), F32)], axis=0)
        of_heads = exact_dot(of_heads, to_seq)
        steps_slot = [of_heads[h : h + 1, :] for h in range(heads)]
        decays_slot = [of_heads[heads + h : heads + h + 1, :] for h in range(heads)]
        dtx_slot = per_channel(steps_slot) * dot(x_conv, to_seq)
        decay_slot = per_channel(decays_slot)
        b_rows = dot_nt(to_slot, b_f.astype(BF16))
        for b in range(seqs):
            grown = dtx_slot[:, b : b + 1] * b_rows[b : b + 1, :]
            out_state[b] = decay_slot[:, b : b + 1] * st[b] + grown

        all_of(2, sq_recv).wait_recv()
        total_sq = sq_recv[0]
        for t in range(1, n_tp):
            total_sq = total_sq + sq_recv[t]
        sq_all = jnp.broadcast_to(total_sq[:, :seqs], (seqs, seqs))
        sq_col = jnp.sum(jnp.where(diagonal, sq_all, 0.0), axis=1, keepdims=True)
        inv_out = lax.rsqrt(sq_col / INNER + EPS)
        all_of(3, br_recv).wait_recv()
        sums = [br_recv[0, k].astype(F32) for k in range(2)]
        for t in range(1, n_tp):
            sums = [sums[k] + br_recv[t, k].astype(F32) for k in range(2)]
        shift = lax.rem(me * feats, LANES)
        branch_sum = pltpu.roll(jnp.concatenate(sums, axis=1), lax.rem(2 * LANES - shift, 2 * LANES), 1)[:, :feats]
        kept = hid_recv[core].astype(F32)
        fresh = (kept + inv_out * branch_sum).astype(BF16).astype(F32)
        out_layer[...] = jnp.where(act_col, fresh, kept).astype(BF16)

        for phase, ref in ((1, bc_recv), (2, sq_recv), (3, br_recv)):
            all_of(phase, ref).wait_send()

        def hid_sent(count):
            return pltpu.make_async_remote_copy(
                src_ref=hid_recv.at[pl.ds(0, count)], dst_ref=hid_recv.at[pl.ds(0, count)],
                send_sem=send_sem.at[0], recv_sem=recv_sem.at[0],
                device_id=device(0, 1 - core), device_id_type=MESH,
            )

        @pl.when(core == 0)
        def _():
            hid_sent(chips).wait_send()

        @pl.when(core == 1)
        def _():
            hid_sent(chips - 1).wait_send()
            relay().wait_send()

    return body


def shards(
    hidden, in_gain, z_weight, x_weight, bc_weight, dt_weight, conv_x_weight, conv_x_bias,
    conv_bc_weight, conv_bc_bias, conv_x_state, conv_bc_state, dt_bias, log_rate, skip_gain,
    ssm_state, norm_gain, out_weight, pool_slot, active,
):
    n_tp = lax.axis_size("tp")
    seqs, feats = hidden.shape
    heads = ssm_state.shape[1]
    chans = z_weight.shape[1]
    bc_dev = bc_weight.shape[1]
    width = in_gain.shape[0]
    tiles = width // LANES
    vmem = pl.BlockSpec(memory_space=pltpu.VMEM)
    hbm = pl.BlockSpec(memory_space=pl.ANY)
    shape = jax.ShapeDtypeStruct
    results = (
        ((seqs, feats), BF16),
        ((3, seqs, chans), BF16),
        ((3, seqs, bc_dev), BF16),
        ((seqs, chans, NS), F32),
    )
    made = pl.pallas_call(
        make_kernel(n_tp, seqs, feats, heads, chans, bc_dev),
        out_shape=tuple(pltpu.VMEM(dims, kind) for dims, kind in results),
        in_specs=[hbm] * 20,
        out_specs=(vmem,) * 4,
        scratch_shapes=[
            pltpu.VMEM((chans, width), BF16),
            pltpu.VMEM((chans, width), BF16),
            pltpu.VMEM((bc_dev, width), BF16),
            pltpu.VMEM((heads, width), BF16),
            pltpu.VMEM((3, seqs, chans), BF16),
            pltpu.VMEM((3, seqs, bc_dev), BF16),
            pltpu.VMEM((seqs, chans, NS), F32),
            pltpu.VMEM((chans, width), BF16),
            pltpu.VMEM((tiles, LANES), F32),
            pltpu.VMEM((1, seqs), jnp.int32),
            pltpu.SMEM((1, seqs), jnp.int32),
            pltpu.VMEM((1, seqs), jnp.int32),
            pltpu.VMEM((4, chans), BF16),
            pltpu.VMEM((chans,), BF16),
            pltpu.VMEM((4, bc_dev), BF16),
            pltpu.VMEM((1, bc_dev), BF16),
            pltpu.VMEM((chans,), F32),
            pltpu.SMEM((heads,), F32),
            pltpu.SMEM((heads,), F32),
            pltpu.SMEM((heads,), F32),
            pltpu.VMEM((seqs, chans, NS), BF16),
            pltpu.VMEM((seqs, width), BF16),
            pltpu.VMEM((n_tp, seqs, feats), BF16),
            pltpu.VMEM((bc_dev // SUBS, LANES), F32),
            pltpu.VMEM((n_tp, bc_dev // SUBS, LANES), F32),
            pltpu.VMEM((1, LANES), F32),
            pltpu.VMEM((n_tp, 1, LANES), F32),
            pltpu.VMEM((tiles, seqs, LANES), BF16),
            pltpu.VMEM((n_tp, 2, seqs, LANES), BF16),
            pltpu.SemaphoreType.DMA((21,)),
            pltpu.SemaphoreType.DMA((4,)),
            pltpu.SemaphoreType.DMA((4,)),
            pltpu.SemaphoreType.DMA((1,)),
        ],
        compiler_params=pltpu.CompilerParams(
            collective_id=0, has_side_effects=True, vmem_limit_bytes=60 * 1024 * 1024
        ),
        name="step",
    )(
        hidden, pool_slot, active.reshape(1, seqs), in_gain.reshape(tiles, LANES),
        z_weight.T, x_weight.T, bc_weight.T, dt_weight.T,
        conv_x_weight, conv_x_bias, conv_bc_weight, conv_bc_bias.reshape(1, bc_dev),
        conv_x_state.transpose(1, 0, 2), conv_bc_state.transpose(1, 0, 2),
        dt_bias, log_rate, skip_gain, ssm_state.reshape(seqs, chans, NS),
        norm_gain, out_weight,
    )
    out_layer, out_cx, out_cbc, out_state = pl.pallas_call(
        put_out,
        out_shape=tuple(shape(dims, kind) for dims, kind in results),
        in_specs=[vmem] * 4,
        out_specs=(hbm,) * 4,
        scratch_shapes=[pltpu.SemaphoreType.DMA((4,))],
        name="put",
    )(*(pltpu.with_memory_space_constraint(x, pltpu.VMEM) for x in made))
    return (
        out_layer,
        out_cx.transpose(1, 0, 2),
        out_cbc.transpose(1, 0, 2),
        out_state.reshape(ssm_state.shape),
    )


def solution(mesh):
    rows = ("groups", "dp")
    placed = (
        P(rows, "tp"), P(), P(None, "tp"), P(None, "tp"), P(None, "tp"), P(None, "tp"), P(None, "tp"),
        P("tp"), P(None, "tp"), P("tp"), P(rows, None, "tp"), P(rows, None, "tp"), P("tp"), P("tp"),
        P("tp"), P(rows, "tp", None, None), P("tp"), P("tp", None), P(rows, None), P(rows),
    )
    return jax.shard_map(
        shards,
        mesh=mesh,
        in_specs=placed,
        out_specs=(P(rows, "tp"), P(rows, None, "tp"), P(rows, None, "tp"), P(rows, "tp", None, None)),
        check_vma=False,
    )
```

```python
import jax
import jax.numpy as jnp
from jax import lax
from jax.experimental import pallas as pl
from jax.experimental.pallas import tpu as pltpu
from jax.sharding import PartitionSpec as P

HP = 64
NS = 128
INNER = 5120
EPS = 1e-05
F32 = jnp.float32
BF16 = jnp.bfloat16
LANES = 128
SUBS = 8

NT = (((1,), (1,)), ((), ()))
MESH = pl.DeviceIdType.MESH


def dot(a, b):
    return jnp.dot(a, b, preferred_element_type=F32)


def dot_nt(a, b):
    return lax.dot_general(a, b, NT, preferred_element_type=F32)


def iota(shape, dim):
    return lax.broadcasted_iota(jnp.int32, shape, dim)


def one_hot(mask):
    return mask.astype(F32).astype(BF16)


def eye(n):
    return one_hot(iota((n, n), 0) == iota((n, n), 1))


def silu(x):
    return x * jax.nn.sigmoid(x)


def exact_dot(x, picks):
    first = x.astype(BF16)
    rest = x - first.astype(F32)
    second = rest.astype(BF16)
    third = (rest - second.astype(F32)).astype(BF16)
    return (dot(first, picks) + dot(second, picks)) + dot(third, picks)


def put_out(*refs):
    sems = refs[-1]
    copies = [pltpu.make_async_copy(refs[k], refs[4 + k], sems.at[k]) for k in (3, 0, 1, 2)]
    for copy in copies:
        copy.start()
    for copy in copies:
        copy.wait()


def make_kernel(n_tp, seqs, feats, heads, chans, bc_dev):
    width = n_tp * feats
    tiles = width // LANES
    chips = n_tp // 2
    half = chips // 2
    steps_far = [half]
    for far in range(half - 1, 0, -1):
        steps_far += [far, chips - far]
    others = n_tp - 1

    def body(
        hid, slot, act, in_gain, z_w, x_w, bc_w, dt_w, cx_w, cx_b, cbc_w, cbc_b, cx_s, cbc_s,
        dt_bias, log_rate, skip_gain, state, norm_gain, out_w,
        out_layer, out_cx, out_cbc, out_state,
        zw, xw, bcw, dtw, cxs, cbcs, st, ow, gain, slot_v, slot_m, act_v, cxw, cxb, cbcw, cbcb, ngain,
        dtb_m, rate_m, skip_m,
        stb, xn, hid_recv, side, bc_send, bc_recv, br_send, br_recv,
        in_sem, send_sem, recv_sem, relay_sem, side_sem,
    ):
        me = lax.axis_index("tp")
        chip, core = me // 2, lax.rem(me, 2)
        barrier = pltpu.get_barrier_semaphore()

        def device(step, which):
            return {"tp": lax.rem(chip + step, chips) * 2 + which}

        loads = {}

        def load(name, src, dst):
            loads[name] = pltpu.make_async_copy(src, dst, in_sem.at[len(loads)])
            loads[name].start()

        load("hid", hid, hid_recv.at[core])

        @pl.when(core == 0)
        def _():
            pl.semaphore_signal(barrier, inc=1, device_id=device(0, 1), device_id_type=MESH)

        @pl.when(core == 1)
        def _():
            for step in steps_far:
                pl.semaphore_signal(barrier, inc=1, device_id=device(step, 1), device_id_type=MESH)

        load("slot", slot, slot_v)
        load("slot_m", slot, slot_m)
        load("act", act, act_v)
        load("bc_w", bc_w, bcw.at[core])
        load("in_gain", in_gain, gain)
        load("cbc_s", cbc_s, cbcs)
        load("cbc_w", cbc_w, cbcw)
        load("cbc_b", cbc_b, cbcb)
        load("dt_w", dt_w, dtw)
        load("cx_s", cx_s, cxs)
        load("cx_w", cx_w, cxw)
        load("cx_b", cx_b, cxb)
        load("norm_gain", norm_gain, ngain)
        load("dt_bias", dt_bias, dtb_m)
        load("log_rate", log_rate, rate_m)
        load("skip_gain", skip_gain, skip_m)
        load("state", state, st)
        load("x_w", x_w, xw)
        load("z_w", z_w, zw)
        load("out_w", out_w, ow)

        def first_send(step, which, dst_slot):
            return pltpu.make_async_remote_copy(
                src_ref=hid_recv.at[core], dst_ref=hid_recv.at[dst_slot],
                send_sem=send_sem.at[0], recv_sem=recv_sem.at[0],
                device_id=device(step, which), device_id_type=MESH,
            )

        def relay():
            return pltpu.make_async_remote_copy(
                src_ref=hid_recv.at[pl.ds(1, n_tp - 1)], dst_ref=hid_recv.at[pl.ds(1, n_tp - 1)],
                send_sem=relay_sem.at[0], recv_sem=recv_sem.at[0],
                device_id=device(0, 0), device_id_type=MESH,
            )

        @pl.when(core == 0)
        def _():
            loads["hid"].wait()
            pl.semaphore_wait(barrier, 1)
            for step in steps_far:
                first_send(step, 1, 2 * (chips - step)).start()
            first_send(0, 1, 0).start()

        @pl.when(core == 1)
        def _():
            loads["hid"].wait()
            pl.semaphore_wait(barrier, chips)
            pl.semaphore_signal(barrier, inc=1, device_id=device(0, 0), device_id_type=MESH)
            for step in steps_far:
                first_send(step, 1, 2 * (chips - step) + 1).start()

        for name in ("slot", "slot_m", "act", "in_gain", "cbc_s", "cbc_w", "cbc_b"):
            loads[name].wait()
        slot_row = slot_v[...]
        by_slot = iota((seqs, seqs), 0) == jnp.broadcast_to(slot_row, (seqs, seqs))
        to_slot = one_hot(by_slot)
        eye16 = eye(seqs)
        diagonal = iota((seqs, seqs), 0) == iota((seqs, seqs), 1)
        to_seq = dot_nt(eye16, to_slot).astype(BF16)
        act_f = jnp.broadcast_to(act_v[...].astype(F32), (seqs, seqs))
        live_row = act_v[...] > 0
        act_col = jnp.sum(jnp.where(diagonal, act_f, 0.0), axis=1, keepdims=True) > 0
        live_slot = jnp.sum(jnp.where(by_slot, act_f, 0.0), axis=1, keepdims=True) > 0
        bc_rows = jnp.concatenate([cbcw[...].astype(F32), cbcb[...].astype(F32)], axis=0)
        row_at, col_at = iota((bc_dev, bc_dev), 0), iota((bc_dev, bc_dev), 1)
        mirror = one_hot(col_at == row_at // SUBS * SUBS + lax.rem(SUBS - lax.rem(row_at, SUBS), SUBS))
        bc_cols = dot_nt(mirror, bc_rows.astype(BF16))
        bc_old = [dot_nt(mirror, dot(to_seq, cbcs[k]).astype(BF16)) for k in range(3)]
        bc_base = (bc_old[0] * bc_cols[:, 0:1] + bc_old[1] * bc_cols[:, 1:2]) + bc_old[2] * bc_cols[:, 2:3]
        pad = jnp.zeros((bc_dev, LANES - seqs), F32)
        side[core, 0] = jnp.concatenate([bc_base + bc_cols[:, 4:5], pad], axis=1)
        side[core, 1] = jnp.broadcast_to(bc_cols[:, 3:4], (bc_dev, LANES))
        loads["bc_w"].wait()
        bcw[core] = dot(mirror, bcw[core]).astype(BF16)

        def lend(j, ref):
            return pltpu.make_async_remote_copy(
                src_ref=ref.at[0], dst_ref=ref.at[0], send_sem=side_sem.at[0, j], recv_sem=side_sem.at[1, j],
                device_id=device(0, 1), device_id_type=MESH,
            )

        @pl.when(core == 0)
        def _():
            lend(0, side).start()
            lend(1, bcw).start()

        for name in ("cx_s", "cx_w", "cx_b", "norm_gain", "dt_bias", "log_rate", "skip_gain"):
            loads[name].wait()
        eye_ch = eye(chans)
        g0 = ngain[...].reshape(1, chans)
        g1 = g0.astype(BF16).astype(F32)
        g2 = (g0 - g1).astype(BF16).astype(F32)
        g3 = (g0 - g1) - g2
        rows = jnp.concatenate([cxw[...].astype(F32), cxb[...].astype(F32).reshape(1, chans), g1, g2, g3], axis=0)
        cols = dot_nt(eye_ch, rows.astype(BF16))
        gain_col = (cols[:, 5:6] + cols[:, 6:7]) + cols[:, 7:8]
        x_old = [dot_nt(eye_ch, dot(to_seq, cxs[k]).astype(BF16)) for k in range(3)]
        x_base = (x_old[0] * cols[:, 0:1] + x_old[1] * cols[:, 1:2]) + x_old[2] * cols[:, 2:3]
        loads["state"].wait()

        def narrow(i, carry):
            stb[i] = st[slot_m[0, i]].astype(BF16)
            return carry

        lax.fori_loop(0, seqs, narrow, 0)
        loads["dt_w"].wait()

        pltpu.make_async_remote_copy(
            src_ref=hid_recv.at[pl.ds(1, n_tp - 1)], dst_ref=hid_recv.at[pl.ds(1, n_tp - 1)],
            send_sem=send_sem.at[0], recv_sem=recv_sem.at[0],
            device_id=device(0, 1 - core), device_id_type=MESH,
        ).wait_recv()

        @pl.when(core == 1)
        def _():
            relay().start()

        blocks = [
            hid_recv[2 * lax.rem(t // 2 - chip + chips, chips) + t % 2].astype(F32) for t in range(n_tp)
        ]
        whole = jnp.concatenate(blocks, axis=1)
        for k in range(tiles):
            at = slice(k * LANES, (k + 1) * LANES)
            xn[:, at] = (whole[:, at] * gain[k : k + 1, :]).astype(BF16)
        squares = whole[:, :LANES] * whole[:, :LANES]
        for k in range(1, tiles):
            part = whole[:, k * LANES : (k + 1) * LANES]
            squares = squares + part * part
        inv_col = lax.rsqrt(jnp.sum(squares, axis=1, keepdims=True) / width + EPS)
        inv = jnp.sum(jnp.where(diagonal, jnp.broadcast_to(inv_col, (seqs, seqs)), 0.0), axis=0, keepdims=True)

        def all_of(phase, dst_ref, count):
            return pltpu.make_async_remote_copy(
                src_ref=dst_ref.at[pl.ds(0, count)], dst_ref=dst_ref.at[pl.ds(0, count)],
                send_sem=send_sem.at[phase], recv_sem=recv_sem.at[phase],
                device_id=device(0, 1 - core), device_id_type=MESH,
            )

        @pl.when(core == 1)
        def _():
            for j, ref in ((0, side), (1, bcw)):
                lend(j, ref).wait_recv()
            both = 2 * bc_dev
            base = jnp.concatenate([side[0, 0], side[1, 0]], axis=0)[:, :seqs]
            tap = jnp.concatenate([side[0, 1], side[1, 1]], axis=0)[:, :seqs]
            proj = dot_nt(jnp.concatenate([bcw[0], bcw[1]], axis=0), xn[...])
            bc_conv = silu(base + (proj * inv).astype(BF16).astype(F32) * tap).astype(BF16).astype(F32)
            spread = jnp.concatenate([bc_conv, jnp.zeros((both, LANES - seqs), F32)], axis=1)
            spread = pltpu.roll(spread.reshape(both // SUBS, SUBS, LANES), 0, 2, stride=seqs, stride_axis=1)
            bc_send[...] = jnp.sum(spread, axis=1)
            for step, which in [(step, which) for step in steps_far for which in (0, 1)] + [(0, 0)]:
                pltpu.make_async_remote_copy(
                    src_ref=bc_send, dst_ref=bc_recv.at[chip], send_sem=send_sem.at[1], recv_sem=recv_sem.at[1],
                    device_id=device(step, which), device_id_type=MESH,
                ).start()
            bc_recv[chip] = bc_send[...]

        dt_proj = (dot_nt(dtw[...], xn[...]) * inv).astype(BF16).astype(F32)
        loads["x_w"].wait()
        x_proj = (dot_nt(xw[...], xn[...]) * inv).astype(BF16)
        loads["z_w"].wait()
        z_proj = (dot_nt(zw[...], xn[...]) * inv).astype(BF16)
        x_conv = silu(x_base + x_proj.astype(F32) * cols[:, 3:4] + cols[:, 4:5]).astype(BF16)
        x_f = x_conv.astype(F32)
        z_gate = silu(z_proj.astype(F32))
        steps, decays = [], []
        for h in range(heads):
            raw = dt_proj[h : h + 1, :] + dtb_m[h]
            step = jnp.maximum(raw, 0.0) + jnp.log1p(jnp.exp(-jnp.abs(raw)))
            rate = jnp.exp(jnp.full((1, seqs), rate_m[h], F32))
            steps.append(jnp.where(live_row, step, 0.0))
            decays.append(jnp.where(live_row, jnp.exp(-step * rate), 1.0))

        def per_channel(values):
            return jnp.concatenate([jnp.broadcast_to(v, (HP, seqs)) for v in values], axis=0)

        dtx = per_channel(steps) * x_f
        decay = per_channel(decays)
        skipped = jnp.concatenate([jnp.full((HP, seqs), skip_m[h], F32) for h in range(heads)], axis=0) * x_f

        @pl.when(core == 0)
        def _():
            all_of(1, bc_recv, chips).wait_recv()

        @pl.when(core == 1)
        def _():
            all_of(1, bc_recv, chips - 1).wait_recv()


        def unpacked(at):
            found = []
            for row in range(NS // SUBS):
                line = at // SUBS + row
                lines = 2 * bc_dev // SUBS
                packed = bc_recv[line // lines, pl.ds(line % lines, 1), :]
                found.append(
                    pltpu.roll(jnp.broadcast_to(packed, (SUBS, LANES)), 0, 1, stride=seqs, stride_axis=0)
                )
            return jnp.concatenate(found, axis=0)[:, :seqs]

        c_f, b_f = unpacked(NS), unpacked(0)
        lane = iota((NS, seqs), 1)
        c_big = jnp.concatenate([jnp.where(lane == b, c_f, 0.0).astype(BF16) for b in range(seqs)], axis=0)
        s_big = jnp.concatenate([stb[b] for b in range(seqs)], axis=1)
        s_c = dot(s_big, c_big)
        bc_dot = jnp.sum(b_f * c_f, axis=0, keepdims=True)
        y = (decay * s_c + dtx * bc_dot) + skipped
        gated = y * z_gate
        scaled = (gated * gain_col).astype(BF16)
        sq_row = jnp.broadcast_to(jnp.sum(gated * gated, axis=0, keepdims=True), (seqs, seqs))
        sq_col = jnp.sum(jnp.where(diagonal, sq_row, 0.0), axis=1, keepdims=True)
        sq_1 = sq_col.astype(BF16).astype(F32)
        sq_2 = (sq_col - sq_1).astype(BF16).astype(F32)
        sq_terms = (sq_1, sq_2, (sq_col - sq_1) - sq_2)
        loads["out_w"].wait()
        rows_seq = dot_nt(eye16, scaled).astype(BF16)
        lane_at = iota((seqs, LANES), 1)
        side_of = chip // half
        half_width = half * 2 * feats
        for part in range(2):
            which = 1 - side_of if part == 0 else side_of
            columns = ow[:, pl.ds(pl.multiple_of(which * half_width, LANES), half_width)]
            branch = dot(rows_seq, columns)
            for i in range(2 * half):
                first, start = (i * feats) // LANES, (i * feats) % LANES
                free = (start + feats) % (2 * LANES)
                for k in range(2):
                    tile = branch[:, (first + k) * LANES : (first + k + 1) * LANES]
                    if free // LANES == k:
                        for j, term in enumerate(sq_terms):
                            tile = jnp.where(lane_at == free % LANES + j, term, tile)
                    br_send[which * 2 * half + i, k] = tile.astype(BF16)
            for i in range(half):
                far = which * half + lax.rem(chip + i, half)
                for flip in (1, 0):
                    if part == 1 and i == 0 and not flip:
                        continue
                    peer = far * 2 + (1 - core if flip else core)
                    pltpu.make_async_remote_copy(
                        src_ref=br_send.at[peer], dst_ref=br_recv.at[me],
                        send_sem=send_sem.at[2], recv_sem=recv_sem.at[2],
                        device_id={"tp": peer}, device_id_type=MESH,
                    ).start()
        br_recv[me] = br_send[me]

        x_now = dot_nt(to_slot, x_proj)
        bc_proj = (dot_nt(bcw[core], xn[...]) * inv).astype(BF16)
        bc_now = dot(dot_nt(to_slot, bc_proj).astype(BF16), mirror)
        for out, old, now in ((out_cx, cxs, x_now), (out_cbc, cbcs, bc_now)):
            held = [old[k].astype(F32) for k in range(3)]
            for k, new in enumerate((held[1], held[2], now)):
                out[k] = jnp.where(live_slot, new, held[k]).astype(BF16)
        of_heads = jnp.concatenate(steps + decays + [jnp.zeros((-2 * heads % SUBS, seqs), F32)], axis=0)
        of_heads = exact_dot(of_heads, to_seq)
        steps_slot = [of_heads[h : h + 1, :] for h in range(heads)]
        decays_slot = [of_heads[heads + h : heads + h + 1, :] for h in range(heads)]
        dtx_slot = per_channel(steps_slot) * dot(x_conv, to_seq)
        decay_slot = per_channel(decays_slot)
        b_rows = dot_nt(to_slot, b_f.astype(BF16))
        for b in range(seqs):
            grown = dtx_slot[:, b : b + 1] * b_rows[b : b + 1, :]
            out_state[b] = decay_slot[:, b : b + 1] * st[b] + grown

        all_of(2, br_recv, others).wait_recv()
        sums = [br_recv[0, k].astype(F32) for k in range(2)]
        for t in range(1, n_tp):
            sums = [sums[k] + br_recv[t, k].astype(F32) for k in range(2)]
        shift = lax.rem(me * feats, LANES)
        summed = pltpu.roll(jnp.concatenate(sums, axis=1), lax.rem(2 * LANES - shift, 2 * LANES), 1)
        branch_sum = summed[:, :feats]
        sq_total = (summed[:, feats : feats + 1] + summed[:, feats + 1 : feats + 2]) + summed[:, feats + 2 : feats + 3]
        inv_out = lax.rsqrt(sq_total / INNER + EPS)
        kept = hid_recv[core].astype(F32)
        fresh = (kept + inv_out * branch_sum).astype(BF16).astype(F32)
        out_layer[...] = jnp.where(act_col, fresh, kept).astype(BF16)

        all_of(2, br_recv, others).wait_send()

        def hid_sent(count):
            return pltpu.make_async_remote_copy(
                src_ref=hid_recv.at[pl.ds(0, count)], dst_ref=hid_recv.at[pl.ds(0, count)],
                send_sem=send_sem.at[0], recv_sem=recv_sem.at[0],
                device_id=device(0, 1 - core), device_id_type=MESH,
            )

        @pl.when(core == 0)
        def _():
            hid_sent(chips).wait_send()
            for j, ref in ((0, side), (1, bcw)):
                lend(j, ref).wait_send()

        @pl.when(core == 1)
        def _():
            hid_sent(chips - 1).wait_send()
            relay().wait_send()
            all_of(1, bc_recv, others).wait_send()

    return body


def shards(
    hidden, in_gain, z_weight, x_weight, bc_weight, dt_weight, conv_x_weight, conv_x_bias,
    conv_bc_weight, conv_bc_bias, conv_x_state, conv_bc_state, dt_bias, log_rate, skip_gain,
    ssm_state, norm_gain, out_weight, pool_slot, active,
):
    n_tp = lax.axis_size("tp")
    seqs, feats = hidden.shape
    heads = ssm_state.shape[1]
    chans = z_weight.shape[1]
    bc_dev = bc_weight.shape[1]
    width = in_gain.shape[0]
    tiles = width // LANES
    vmem = pl.BlockSpec(memory_space=pltpu.VMEM)
    hbm = pl.BlockSpec(memory_space=pl.ANY)
    shape = jax.ShapeDtypeStruct
    results = (
        ((seqs, feats), BF16),
        ((3, seqs, chans), BF16),
        ((3, seqs, bc_dev), BF16),
        ((seqs, chans, NS), F32),
    )
    made = pl.pallas_call(
        make_kernel(n_tp, seqs, feats, heads, chans, bc_dev),
        out_shape=tuple(pltpu.VMEM(dims, kind) for dims, kind in results),
        in_specs=[hbm] * 20,
        out_specs=(vmem,) * 4,
        scratch_shapes=[
            pltpu.VMEM((chans, width), BF16),
            pltpu.VMEM((chans, width), BF16),
            pltpu.VMEM((2, bc_dev, width), BF16),
            pltpu.VMEM((heads, width), BF16),
            pltpu.VMEM((3, seqs, chans), BF16),
            pltpu.VMEM((3, seqs, bc_dev), BF16),
            pltpu.VMEM((seqs, chans, NS), F32),
            pltpu.VMEM((chans, width), BF16),
            pltpu.VMEM((tiles, LANES), F32),
            pltpu.VMEM((1, seqs), jnp.int32),
            pltpu.SMEM((1, seqs), jnp.int32),
            pltpu.VMEM((1, seqs), jnp.int32),
            pltpu.VMEM((4, chans), BF16),
            pltpu.VMEM((chans,), BF16),
            pltpu.VMEM((4, bc_dev), BF16),
            pltpu.VMEM((1, bc_dev), BF16),
            pltpu.VMEM((chans,), F32),
            pltpu.SMEM((heads,), F32),
            pltpu.SMEM((heads,), F32),
            pltpu.SMEM((heads,), F32),
            pltpu.VMEM((seqs, chans, NS), BF16),
            pltpu.VMEM((seqs, width), BF16),
            pltpu.VMEM((n_tp, seqs, feats), BF16),
            pltpu.VMEM((2, 2, bc_dev, LANES), F32),
            pltpu.VMEM((2 * bc_dev // SUBS, LANES), F32),
            pltpu.VMEM((n_tp, 2 * bc_dev // SUBS, LANES), F32),
            pltpu.VMEM((n_tp, 2, seqs, LANES), BF16),
            pltpu.VMEM((n_tp, 2, seqs, LANES), BF16),
            pltpu.SemaphoreType.DMA((20 + 1,)),
            pltpu.SemaphoreType.DMA((3,)),
            pltpu.SemaphoreType.DMA((3,)),
            pltpu.SemaphoreType.DMA((1,)),
            pltpu.SemaphoreType.DMA((2, 2)),
        ],
        compiler_params=pltpu.CompilerParams(
            collective_id=0, has_side_effects=True, vmem_limit_bytes=60 * 1024 * 1024
        ),
        name="step",
    )(
        hidden, pool_slot, active.reshape(1, seqs), in_gain.reshape(tiles, LANES),
        z_weight.T, x_weight.T, bc_weight.T, dt_weight.T,
        conv_x_weight, conv_x_bias, conv_bc_weight, conv_bc_bias.reshape(1, bc_dev),
        conv_x_state.transpose(1, 0, 2), conv_bc_state.transpose(1, 0, 2),
        dt_bias, log_rate, skip_gain, ssm_state.reshape(seqs, chans, NS),
        norm_gain, out_weight,
    )
    out_layer, out_cx, out_cbc, out_state = pl.pallas_call(
        put_out,
        out_shape=tuple(shape(dims, kind) for dims, kind in results),
        in_specs=[vmem] * 4,
        out_specs=(hbm,) * 4,
        scratch_shapes=[pltpu.SemaphoreType.DMA((4,))],
        name="put",
    )(*(pltpu.with_memory_space_constraint(x, pltpu.VMEM) for x in made))
    return (
        out_layer,
        out_cx.transpose(1, 0, 2),
        out_cbc.transpose(1, 0, 2),
        out_state.reshape(ssm_state.shape),
    )


def solution(mesh):
    rows = ("groups", "dp")
    placed = (
        P(rows, "tp"), P(), P(None, "tp"), P(None, "tp"), P(None, "tp"), P(None, "tp"), P(None, "tp"),
        P("tp"), P(None, "tp"), P("tp"), P(rows, None, "tp"), P(rows, None, "tp"), P("tp"), P("tp"),
        P("tp"), P(rows, "tp", None, None), P("tp"), P("tp", None), P(rows, None), P(rows),
    )
    return jax.shard_map(
        shards,
        mesh=mesh,
        in_specs=placed,
        out_specs=(P(rows, "tp"), P(rows, None, "tp"), P(rows, None, "tp"), P(rows, "tp", None, None)),
        check_vma=False,
    )
```

```python
import jax
import jax.numpy as jnp
from jax import lax
from jax.experimental import pallas as pl
from jax.experimental.pallas import tpu as pltpu
from jax.sharding import PartitionSpec as P

HP = 64
NS = 128
INNER = 5120
EPS = 1e-05
F32 = jnp.float32
BF16 = jnp.bfloat16
LANES = 128
SUBS = 8

NT = (((1,), (1,)), ((), ()))
MESH = pl.DeviceIdType.MESH


def dot(a, b):
    return jnp.dot(a, b, preferred_element_type=F32)


def dot_nt(a, b):
    return lax.dot_general(a, b, NT, preferred_element_type=F32)


def iota(shape, dim):
    return lax.broadcasted_iota(jnp.int32, shape, dim)


def one_hot(mask):
    return mask.astype(F32).astype(BF16)


def eye(n):
    return one_hot(iota((n, n), 0) == iota((n, n), 1))


def silu(x):
    return x * jax.nn.sigmoid(x)


def exact_dot(x, picks):
    first = x.astype(BF16)
    rest = x - first.astype(F32)
    second = rest.astype(BF16)
    third = (rest - second.astype(F32)).astype(BF16)
    return (dot(first, picks) + dot(second, picks)) + dot(third, picks)


def put_out(*refs):
    sems = refs[-1]
    pieces = 4
    rows = refs[3].shape[0] // pieces
    copies = [
        pltpu.make_async_copy(refs[3].at[pl.ds(k * rows, rows)], refs[7].at[pl.ds(k * rows, rows)], sems.at[3 + k])
        for k in range(pieces)
    ]
    copies += [pltpu.make_async_copy(refs[k], refs[4 + k], sems.at[k]) for k in range(3)]
    for copy in copies:
        copy.start()
    for copy in copies:
        copy.wait()


def make_kernel(n_tp, seqs, feats, heads, chans, bc_dev):
    width = n_tp * feats
    tiles = width // LANES
    chips = n_tp // 2
    half = chips // 2
    steps_far = [half]
    for far in range(half - 1, 0, -1):
        steps_far += [far, chips - far]
    others = n_tp - 1

    def body(
        hid, slot, act, in_gain, z_w, x_w, bc_w, dt_w, cx_w, cx_b, cbc_w, cbc_b, cx_s, cbc_s,
        dt_bias, log_rate, skip_gain, state, norm_gain, out_w,
        out_layer, out_cx, out_cbc, out_state,
        zw, xw, bcw, dtw, cxs, cbcs, st, ow, gain, slot_v, slot_m, act_v, cxw, cxb, cbcw, cbcb, ngain,
        dtb_m, rate_m, skip_m,
        stb, xn, hid_recv, side, bc_send, bc_recv, br_send, br_recv,
        in_sem, send_sem, recv_sem, relay_sem, side_sem,
    ):
        me = lax.axis_index("tp")
        chip, core = me // 2, lax.rem(me, 2)
        barrier = pltpu.get_barrier_semaphore()

        def device(step, which):
            return {"tp": lax.rem(chip + step, chips) * 2 + which}

        loads = {}

        def load(name, src, dst):
            loads[name] = pltpu.make_async_copy(src, dst, in_sem.at[len(loads)])
            loads[name].start()

        load("hid", hid, hid_recv.at[core])

        @pl.when(core == 0)
        def _():
            pl.semaphore_signal(barrier, inc=1, device_id=device(0, 1), device_id_type=MESH)

        @pl.when(core == 1)
        def _():
            for step in steps_far:
                pl.semaphore_signal(barrier, inc=1, device_id=device(step, 1), device_id_type=MESH)

        load("slot", slot, slot_v)
        load("slot_m", slot, slot_m)
        load("act", act, act_v)
        load("bc_w", bc_w, bcw.at[core])
        load("in_gain", in_gain, gain)
        load("cbc_s", cbc_s, cbcs)
        load("cbc_w", cbc_w, cbcw)
        load("cbc_b", cbc_b, cbcb)
        load("dt_w", dt_w, dtw)
        load("cx_s", cx_s, cxs)
        load("cx_w", cx_w, cxw)
        load("cx_b", cx_b, cxb)
        load("norm_gain", norm_gain, ngain)
        load("dt_bias", dt_bias, dtb_m)
        load("log_rate", log_rate, rate_m)
        load("skip_gain", skip_gain, skip_m)
        load("state", state, st)
        load("x_w", x_w, xw)
        load("z_w", z_w, zw)
        load("out_w", out_w, ow)

        def first_send(step, which, dst_slot):
            return pltpu.make_async_remote_copy(
                src_ref=hid_recv.at[core], dst_ref=hid_recv.at[dst_slot],
                send_sem=send_sem.at[0], recv_sem=recv_sem.at[0],
                device_id=device(step, which), device_id_type=MESH,
            )

        def relay():
            return pltpu.make_async_remote_copy(
                src_ref=hid_recv.at[pl.ds(1, n_tp - 1)], dst_ref=hid_recv.at[pl.ds(1, n_tp - 1)],
                send_sem=relay_sem.at[0], recv_sem=recv_sem.at[0],
                device_id=device(0, 0), device_id_type=MESH,
            )

        @pl.when(core == 0)
        def _():
            loads["hid"].wait()
            pl.semaphore_wait(barrier, 1)
            for step in steps_far:
                first_send(step, 1, 2 * (chips - step)).start()
            first_send(0, 1, 0).start()

        @pl.when(core == 1)
        def _():
            loads["hid"].wait()
            pl.semaphore_wait(barrier, chips)
            pl.semaphore_signal(barrier, inc=1, device_id=device(0, 0), device_id_type=MESH)
            for step in steps_far:
                first_send(step, 1, 2 * (chips - step) + 1).start()

        for name in ("slot", "slot_m", "act", "in_gain", "cbc_s", "cbc_w", "cbc_b"):
            loads[name].wait()
        slot_row = slot_v[...]
        by_slot = iota((seqs, seqs), 0) == jnp.broadcast_to(slot_row, (seqs, seqs))
        to_slot = one_hot(by_slot)
        eye16 = eye(seqs)
        diagonal = iota((seqs, seqs), 0) == iota((seqs, seqs), 1)
        to_seq = dot_nt(eye16, to_slot).astype(BF16)
        act_f = jnp.broadcast_to(act_v[...].astype(F32), (seqs, seqs))
        live_row = act_v[...] > 0
        act_col = jnp.sum(jnp.where(diagonal, act_f, 0.0), axis=1, keepdims=True) > 0
        live_slot = jnp.sum(jnp.where(by_slot, act_f, 0.0), axis=1, keepdims=True) > 0
        bc_rows = jnp.concatenate([cbcw[...].astype(F32), cbcb[...].astype(F32)], axis=0)
        row_at, col_at = iota((bc_dev, bc_dev), 0), iota((bc_dev, bc_dev), 1)
        mirror = one_hot(col_at == row_at // SUBS * SUBS + lax.rem(SUBS - lax.rem(row_at, SUBS), SUBS))
        bc_cols = dot_nt(mirror, bc_rows.astype(BF16))
        bc_old = [dot_nt(mirror, dot(to_seq, cbcs[k]).astype(BF16)) for k in range(3)]
        bc_base = (bc_old[0] * bc_cols[:, 0:1] + bc_old[1] * bc_cols[:, 1:2]) + bc_old[2] * bc_cols[:, 2:3]
        pad = jnp.zeros((bc_dev, LANES - seqs), F32)
        side[core, 0] = jnp.concatenate([bc_base + bc_cols[:, 4:5], pad], axis=1)
        side[core, 1] = jnp.broadcast_to(bc_cols[:, 3:4], (bc_dev, LANES))
        loads["bc_w"].wait()
        bcw[core] = dot(mirror, bcw[core]).astype(BF16)

        def lend(j, ref):
            return pltpu.make_async_remote_copy(
                src_ref=ref.at[0], dst_ref=ref.at[0], send_sem=side_sem.at[0, j], recv_sem=side_sem.at[1, j],
                device_id=device(0, 1), device_id_type=MESH,
            )

        @pl.when(core == 0)
        def _():
            lend(0, side).start()
            lend(1, bcw).start()

        for name in ("cx_s", "cx_w", "cx_b", "norm_gain", "dt_bias", "log_rate", "skip_gain"):
            loads[name].wait()
        eye_ch = eye(chans)
        g0 = ngain[...].reshape(1, chans)
        g1 = g0.astype(BF16).astype(F32)
        g2 = (g0 - g1).astype(BF16).astype(F32)
        g3 = (g0 - g1) - g2
        rows = jnp.concatenate([cxw[...].astype(F32), cxb[...].astype(F32).reshape(1, chans), g1, g2, g3], axis=0)
        cols = dot_nt(eye_ch, rows.astype(BF16))
        gain_col = (cols[:, 5:6] + cols[:, 6:7]) + cols[:, 7:8]
        x_old = [dot_nt(eye_ch, dot(to_seq, cxs[k]).astype(BF16)) for k in range(3)]
        x_base = (x_old[0] * cols[:, 0:1] + x_old[1] * cols[:, 1:2]) + x_old[2] * cols[:, 2:3]
        loads["state"].wait()

        def narrow(i, carry):
            stb[i] = st[slot_m[0, i]].astype(BF16)
            return carry

        lax.fori_loop(0, seqs, narrow, 0)
        loads["dt_w"].wait()

        pltpu.make_async_remote_copy(
            src_ref=hid_recv.at[pl.ds(1, n_tp - 1)], dst_ref=hid_recv.at[pl.ds(1, n_tp - 1)],
            send_sem=send_sem.at[0], recv_sem=recv_sem.at[0],
            device_id=device(0, 1 - core), device_id_type=MESH,
        ).wait_recv()

        @pl.when(core == 1)
        def _():
            relay().start()

        blocks = [
            hid_recv[2 * lax.rem(t // 2 - chip + chips, chips) + t % 2].astype(F32) for t in range(n_tp)
        ]
        whole = jnp.concatenate(blocks, axis=1)
        for k in range(tiles):
            at = slice(k * LANES, (k + 1) * LANES)
            xn[:, at] = (whole[:, at] * gain[k : k + 1, :]).astype(BF16)
        squares = whole[:, :LANES] * whole[:, :LANES]
        for k in range(1, tiles):
            part = whole[:, k * LANES : (k + 1) * LANES]
            squares = squares + part * part
        inv_col = lax.rsqrt(jnp.sum(squares, axis=1, keepdims=True) / width + EPS)
        inv = jnp.sum(jnp.where(diagonal, jnp.broadcast_to(inv_col, (seqs, seqs)), 0.0), axis=0, keepdims=True)

        def all_of(phase, dst_ref, count):
            return pltpu.make_async_remote_copy(
                src_ref=dst_ref.at[pl.ds(0, count)], dst_ref=dst_ref.at[pl.ds(0, count)],
                send_sem=send_sem.at[phase], recv_sem=recv_sem.at[phase],
                device_id=device(0, 1 - core), device_id_type=MESH,
            )

        @pl.when(core == 1)
        def _():
            for j, ref in ((0, side), (1, bcw)):
                lend(j, ref).wait_recv()
            both = 2 * bc_dev
            base = jnp.concatenate([side[0, 0], side[1, 0]], axis=0)[:, :seqs]
            tap = jnp.concatenate([side[0, 1], side[1, 1]], axis=0)[:, :seqs]
            weights = jnp.concatenate([bcw[0], bcw[1]], axis=0)
            proj = dot_nt(weights[:, : width // 2], xn[:, : width // 2]) + dot_nt(weights[:, width // 2 :], xn[:, width // 2 :])
            bc_conv = silu(base + (proj * inv).astype(BF16).astype(F32) * tap).astype(BF16).astype(F32)
            spread = jnp.concatenate([bc_conv, jnp.zeros((both, LANES - seqs), F32)], axis=1)
            spread = pltpu.roll(spread.reshape(both // SUBS, SUBS, LANES), 0, 2, stride=seqs, stride_axis=1)
            bc_send[...] = jnp.sum(spread, axis=1)
            for step, which in [(step, which) for step in steps_far for which in (0, 1)] + [(0, 0)]:
                pltpu.make_async_remote_copy(
                    src_ref=bc_send, dst_ref=bc_recv.at[chip], send_sem=send_sem.at[1], recv_sem=recv_sem.at[1],
                    device_id=device(step, which), device_id_type=MESH,
                ).start()
            bc_recv[chip] = bc_send[...]

        dt_proj = (dot_nt(dtw[...], xn[...]) * inv).astype(BF16).astype(F32)
        loads["x_w"].wait()
        loads["z_w"].wait()
        x_proj = (dot_nt(xw[...], xn[...]) * inv).astype(BF16)
        z_proj = (dot_nt(zw[...], xn[...]) * inv).astype(BF16)
        x_conv = silu(x_base + x_proj.astype(F32) * cols[:, 3:4] + cols[:, 4:5]).astype(BF16)
        x_f = x_conv.astype(F32)
        z_gate = silu(z_proj.astype(F32))
        steps, decays = [], []
        for h in range(heads):
            raw = dt_proj[h : h + 1, :] + dtb_m[h]
            step = jnp.maximum(raw, 0.0) + jnp.log1p(jnp.exp(-jnp.abs(raw)))
            rate = jnp.exp(jnp.full((1, seqs), rate_m[h], F32))
            steps.append(jnp.where(live_row, step, 0.0))
            decays.append(jnp.where(live_row, jnp.exp(-step * rate), 1.0))

        def per_channel(values):
            return jnp.concatenate([jnp.broadcast_to(v, (HP, seqs)) for v in values], axis=0)

        dtx = per_channel(steps) * x_f
        decay = per_channel(decays)
        skipped = jnp.concatenate([jnp.full((HP, seqs), skip_m[h], F32) for h in range(heads)], axis=0) * x_f

        @pl.when(core == 0)
        def _():
            all_of(1, bc_recv, chips).wait_recv()

        @pl.when(core == 1)
        def _():
            all_of(1, bc_recv, chips - 1).wait_recv()


        def unpacked(at):
            found = []
            for row in range(NS // SUBS):
                line = at // SUBS + row
                lines = 2 * bc_dev // SUBS
                packed = bc_recv[line // lines, pl.ds(line % lines, 1), :]
                found.append(
                    pltpu.roll(jnp.broadcast_to(packed, (SUBS, LANES)), 0, 1, stride=seqs, stride_axis=0)
                )
            return jnp.concatenate(found, axis=0)[:, :seqs]

        c_f, b_f = unpacked(NS), unpacked(0)
        lane = iota((NS, seqs), 1)
        c_big = jnp.concatenate([jnp.where(lane == b, c_f, 0.0).astype(BF16) for b in range(seqs)], axis=0)
        s_c = []
        for at in (0, chans // 2):
            s_big = jnp.concatenate([stb[b, at : at + chans // 2, :] for b in range(seqs)], axis=1)
            s_c.append(dot(s_big, c_big))
        s_c = jnp.concatenate(s_c, axis=0)
        bc_dot = jnp.sum(b_f * c_f, axis=0, keepdims=True)
        y = (decay * s_c + dtx * bc_dot) + skipped
        gated = y * z_gate
        scaled = (gated * gain_col).astype(BF16)
        sq_row = jnp.broadcast_to(jnp.sum(gated * gated, axis=0, keepdims=True), (seqs, seqs))
        sq_col = jnp.sum(jnp.where(diagonal, sq_row, 0.0), axis=1, keepdims=True)
        sq_1 = sq_col.astype(BF16).astype(F32)
        sq_2 = (sq_col - sq_1).astype(BF16).astype(F32)
        sq_terms = (sq_1, sq_2, (sq_col - sq_1) - sq_2)
        loads["out_w"].wait()
        rows_seq = dot_nt(eye16, scaled).astype(BF16)
        lane_at = iota((seqs, LANES), 1)
        side_of = chip // half
        half_width = half * 2 * feats
        for part in range(2):
            which = 1 - side_of if part == 0 else side_of
            step = 2 * LANES
            branch = jnp.concatenate(
                [
                    dot(rows_seq, ow[:, pl.ds(pl.multiple_of(which * half_width + at, LANES), step)])
                    for at in range(0, half_width, step)
                ],
                axis=1,
            )
            for i in range(2 * half):
                first, start = (i * feats) // LANES, (i * feats) % LANES
                free = (start + feats) % (2 * LANES)
                for k in range(2):
                    tile = branch[:, (first + k) * LANES : (first + k + 1) * LANES]
                    if free // LANES == k:
                        for j, term in enumerate(sq_terms):
                            tile = jnp.where(lane_at == free % LANES + j, term, tile)
                    br_send[which * 2 * half + i, k] = tile.astype(BF16)
            for i in range(half):
                far = which * half + lax.rem(chip + i, half)
                for flip in (1, 0):
                    if part == 1 and i == 0 and not flip:
                        continue
                    peer = far * 2 + (1 - core if flip else core)
                    pltpu.make_async_remote_copy(
                        src_ref=br_send.at[peer], dst_ref=br_recv.at[me],
                        send_sem=send_sem.at[2], recv_sem=recv_sem.at[2],
                        device_id={"tp": peer}, device_id_type=MESH,
                    ).start()
        br_recv[me] = br_send[me]

        x_now = dot_nt(to_slot, x_proj)
        bc_proj = (dot_nt(bcw[core], xn[...]) * inv).astype(BF16)
        bc_now = dot(dot_nt(to_slot, bc_proj).astype(BF16), mirror)
        for out, old, now in ((out_cx, cxs, x_now), (out_cbc, cbcs, bc_now)):
            held = [old[k].astype(F32) for k in range(3)]
            for k, new in enumerate((held[1], held[2], now)):
                out[k] = jnp.where(live_slot, new, held[k]).astype(BF16)
        of_heads = jnp.concatenate(steps + decays + [jnp.zeros((-2 * heads % SUBS, seqs), F32)], axis=0)
        of_heads = exact_dot(of_heads, to_seq)
        steps_slot = [of_heads[h : h + 1, :] for h in range(heads)]
        decays_slot = [of_heads[heads + h : heads + h + 1, :] for h in range(heads)]
        dtx_slot = per_channel(steps_slot) * dot(x_conv, to_seq)
        decay_slot = per_channel(decays_slot)
        b_rows = dot_nt(to_slot, b_f.astype(BF16))
        for b in range(seqs):
            grown = dtx_slot[:, b : b + 1] * b_rows[b : b + 1, :]
            out_state[b] = decay_slot[:, b : b + 1] * st[b] + grown

        all_of(2, br_recv, others).wait_recv()
        sums = [br_recv[0, k].astype(F32) for k in range(2)]
        for t in range(1, n_tp):
            sums = [sums[k] + br_recv[t, k].astype(F32) for k in range(2)]
        shift = lax.rem(me * feats, LANES)
        summed = pltpu.roll(jnp.concatenate(sums, axis=1), lax.rem(2 * LANES - shift, 2 * LANES), 1)
        branch_sum = summed[:, :feats]
        sq_total = (summed[:, feats : feats + 1] + summed[:, feats + 1 : feats + 2]) + summed[:, feats + 2 : feats + 3]
        inv_out = lax.rsqrt(sq_total / INNER + EPS)
        kept = hid_recv[core].astype(F32)
        fresh = (kept + inv_out * branch_sum).astype(BF16).astype(F32)
        out_layer[...] = jnp.where(act_col, fresh, kept).astype(BF16)

        all_of(2, br_recv, others).wait_send()

        def hid_sent(count):
            return pltpu.make_async_remote_copy(
                src_ref=hid_recv.at[pl.ds(0, count)], dst_ref=hid_recv.at[pl.ds(0, count)],
                send_sem=send_sem.at[0], recv_sem=recv_sem.at[0],
                device_id=device(0, 1 - core), device_id_type=MESH,
            )

        @pl.when(core == 0)
        def _():
            hid_sent(chips).wait_send()
            for j, ref in ((0, side), (1, bcw)):
                lend(j, ref).wait_send()

        @pl.when(core == 1)
        def _():
            hid_sent(chips - 1).wait_send()
            relay().wait_send()
            all_of(1, bc_recv, others).wait_send()

    return body


def shards(
    hidden, in_gain, z_weight, x_weight, bc_weight, dt_weight, conv_x_weight, conv_x_bias,
    conv_bc_weight, conv_bc_bias, conv_x_state, conv_bc_state, dt_bias, log_rate, skip_gain,
    ssm_state, norm_gain, out_weight, pool_slot, active,
):
    n_tp = lax.axis_size("tp")
    seqs, feats = hidden.shape
    heads = ssm_state.shape[1]
    chans = z_weight.shape[1]
    bc_dev = bc_weight.shape[1]
    width = in_gain.shape[0]
    tiles = width // LANES
    vmem = pl.BlockSpec(memory_space=pltpu.VMEM)
    hbm = pl.BlockSpec(memory_space=pl.ANY)
    shape = jax.ShapeDtypeStruct
    results = (
        ((seqs, feats), BF16),
        ((3, seqs, chans), BF16),
        ((3, seqs, bc_dev), BF16),
        ((seqs, chans, NS), F32),
    )
    made = pl.pallas_call(
        make_kernel(n_tp, seqs, feats, heads, chans, bc_dev),
        out_shape=tuple(pltpu.VMEM(dims, kind) for dims, kind in results),
        in_specs=[hbm] * 20,
        out_specs=(vmem,) * 4,
        scratch_shapes=[
            pltpu.VMEM((chans, width), BF16),
            pltpu.VMEM((chans, width), BF16),
            pltpu.VMEM((2, bc_dev, width), BF16),
            pltpu.VMEM((heads, width), BF16),
            pltpu.VMEM((3, seqs, chans), BF16),
            pltpu.VMEM((3, seqs, bc_dev), BF16),
            pltpu.VMEM((seqs, chans, NS), F32),
            pltpu.VMEM((chans, width), BF16),
            pltpu.VMEM((tiles, LANES), F32),
            pltpu.VMEM((1, seqs), jnp.int32),
            pltpu.SMEM((1, seqs), jnp.int32),
            pltpu.VMEM((1, seqs), jnp.int32),
            pltpu.VMEM((4, chans), BF16),
            pltpu.VMEM((chans,), BF16),
            pltpu.VMEM((4, bc_dev), BF16),
            pltpu.VMEM((1, bc_dev), BF16),
            pltpu.VMEM((chans,), F32),
            pltpu.SMEM((heads,), F32),
            pltpu.SMEM((heads,), F32),
            pltpu.SMEM((heads,), F32),
            pltpu.VMEM((seqs, chans, NS), BF16),
            pltpu.VMEM((seqs, width), BF16),
            pltpu.VMEM((n_tp, seqs, feats), BF16),
            pltpu.VMEM((2, 2, bc_dev, LANES), F32),
            pltpu.VMEM((2 * bc_dev // SUBS, LANES), F32),
            pltpu.VMEM((n_tp, 2 * bc_dev // SUBS, LANES), F32),
            pltpu.VMEM((n_tp, 2, seqs, LANES), BF16),
            pltpu.VMEM((n_tp, 2, seqs, LANES), BF16),
            pltpu.SemaphoreType.DMA((20 + 1,)),
            pltpu.SemaphoreType.DMA((3,)),
            pltpu.SemaphoreType.DMA((3,)),
            pltpu.SemaphoreType.DMA((1,)),
            pltpu.SemaphoreType.DMA((2, 2)),
        ],
        compiler_params=pltpu.CompilerParams(
            collective_id=0, has_side_effects=True, vmem_limit_bytes=60 * 1024 * 1024
        ),
        name="step",
    )(
        hidden, pool_slot, active.reshape(1, seqs), in_gain.reshape(tiles, LANES),
        z_weight.T, x_weight.T, bc_weight.T, dt_weight.T,
        conv_x_weight, conv_x_bias, conv_bc_weight, conv_bc_bias.reshape(1, bc_dev),
        conv_x_state.transpose(1, 0, 2), conv_bc_state.transpose(1, 0, 2),
        dt_bias, log_rate, skip_gain, ssm_state.reshape(seqs, chans, NS),
        norm_gain, out_weight,
    )
    out_layer, out_cx, out_cbc, out_state = pl.pallas_call(
        put_out,
        out_shape=tuple(shape(dims, kind) for dims, kind in results),
        in_specs=[vmem] * 4,
        out_specs=(hbm,) * 4,
        scratch_shapes=[pltpu.SemaphoreType.DMA((7,))],
        name="put",
    )(*(pltpu.with_memory_space_constraint(x, pltpu.VMEM) for x in made))
    return (
        out_layer,
        out_cx.transpose(1, 0, 2),
        out_cbc.transpose(1, 0, 2),
        out_state.reshape(ssm_state.shape),
    )


def solution(mesh):
    rows = ("groups", "dp")
    placed = (
        P(rows, "tp"), P(), P(None, "tp"), P(None, "tp"), P(None, "tp"), P(None, "tp"), P(None, "tp"),
        P("tp"), P(None, "tp"), P("tp"), P(rows, None, "tp"), P(rows, None, "tp"), P("tp"), P("tp"),
        P("tp"), P(rows, "tp", None, None), P("tp"), P("tp", None), P(rows, None), P(rows),
    )
    return jax.shard_map(
        shards,
        mesh=mesh,
        in_specs=placed,
        out_specs=(P(rows, "tp"), P(rows, None, "tp"), P(rows, None, "tp"), P(rows, "tp", None, None)),
        check_vma=False,
    )
```

```python
import jax
import jax.numpy as jnp
from jax import lax
from jax.experimental import pallas as pl
from jax.experimental.pallas import tpu as pltpu
from jax.sharding import PartitionSpec as P

HP = 64
NS = 128
INNER = 5120
EPS = 1e-05
F32 = jnp.float32
BF16 = jnp.bfloat16
LANES = 128
SUBS = 8

NT = (((1,), (1,)), ((), ()))
MESH = pl.DeviceIdType.MESH


def dot(a, b):
    return jnp.dot(a, b, preferred_element_type=F32)


def dot_nt(a, b):
    return lax.dot_general(a, b, NT, preferred_element_type=F32)


def iota(shape, dim):
    return lax.broadcasted_iota(jnp.int32, shape, dim)


def one_hot(mask):
    return mask.astype(F32).astype(BF16)


def eye(n):
    return one_hot(iota((n, n), 0) == iota((n, n), 1))


def silu(x):
    return x * jax.nn.sigmoid(x)


def exact_dot(x, picks):
    first = x.astype(BF16)
    rest = x - first.astype(F32)
    second = rest.astype(BF16)
    third = (rest - second.astype(F32)).astype(BF16)
    return (dot(first, picks) + dot(second, picks)) + dot(third, picks)


def put_out(*refs):
    sems = refs[-1]
    pieces = 4
    rows = refs[3].shape[0] // pieces
    copies = [
        pltpu.make_async_copy(refs[3].at[pl.ds(k * rows, rows)], refs[7].at[pl.ds(k * rows, rows)], sems.at[3 + k])
        for k in range(pieces)
    ]
    copies += [pltpu.make_async_copy(refs[k], refs[4 + k], sems.at[k]) for k in range(3)]
    for copy in copies:
        copy.start()
    for copy in copies:
        copy.wait()


def make_kernel(n_tp, seqs, feats, heads, chans, bc_dev):
    width = n_tp * feats
    tiles = width // LANES
    chips = n_tp // 2
    half = chips // 2
    steps_far = [half]
    for far in range(half - 1, 0, -1):
        steps_far += [far, chips - far]
    others = n_tp - 1

    def body(
        hid, slot, act, in_gain, z_w, x_w, bc_w, dt_w, cx_w, cx_b, cbc_w, cbc_b, cx_s, cbc_s,
        dt_bias, log_rate, skip_gain, state, norm_gain, out_w,
        out_layer, out_cx, out_cbc, out_state,
        zw, xw, bcw, dtw, cxs, cbcs, st, ow, gain, slot_v, slot_m, act_v, cxw, cxb, cbcw, cbcb, ngain,
        dtb_m, rate_m, skip_m,
        stb, xn, hid_recv, side, bc_send, bc_recv, br_send, br_recv,
        in_sem, send_sem, recv_sem, relay_sem, side_sem,
    ):
        me = lax.axis_index("tp")
        chip, core = me // 2, lax.rem(me, 2)
        barrier = pltpu.get_barrier_semaphore()

        def device(step, which):
            return {"tp": lax.rem(chip + step, chips) * 2 + which}

        loads = {}

        def load(name, src, dst):
            loads[name] = pltpu.make_async_copy(src, dst, in_sem.at[len(loads)])
            loads[name].start()

        load("hid", hid, hid_recv.at[core])

        @pl.when(core == 0)
        def _():
            pl.semaphore_signal(barrier, inc=1, device_id=device(0, 1), device_id_type=MESH)

        @pl.when(core == 1)
        def _():
            for step in steps_far:
                pl.semaphore_signal(barrier, inc=1, device_id=device(step, 1), device_id_type=MESH)

        load("slot", slot, slot_v)
        load("slot_m", slot, slot_m)
        load("act", act, act_v)
        load("bc_w", bc_w, bcw.at[core])
        load("in_gain", in_gain, gain)
        load("cbc_s", cbc_s, cbcs)
        load("cbc_w", cbc_w, cbcw)
        load("cbc_b", cbc_b, cbcb)
        load("dt_w", dt_w, dtw)
        load("cx_s", cx_s, cxs)
        load("cx_w", cx_w, cxw)
        load("cx_b", cx_b, cxb)
        load("norm_gain", norm_gain, ngain)
        load("dt_bias", dt_bias, dtb_m)
        load("log_rate", log_rate, rate_m)
        load("skip_gain", skip_gain, skip_m)
        load("state", state, st)
        load("x_w", x_w, xw)
        load("z_w", z_w, zw)
        load("out_w", out_w, ow)

        def first_send(step, which, dst_slot):
            return pltpu.make_async_remote_copy(
                src_ref=hid_recv.at[core], dst_ref=hid_recv.at[dst_slot],
                send_sem=send_sem.at[0], recv_sem=recv_sem.at[0],
                device_id=device(step, which), device_id_type=MESH,
            )

        def relay():
            return pltpu.make_async_remote_copy(
                src_ref=hid_recv.at[pl.ds(1, n_tp - 1)], dst_ref=hid_recv.at[pl.ds(1, n_tp - 1)],
                send_sem=relay_sem.at[0], recv_sem=recv_sem.at[0],
                device_id=device(0, 0), device_id_type=MESH,
            )

        @pl.when(core == 0)
        def _():
            loads["hid"].wait()
            pl.semaphore_wait(barrier, 1)
            for step in steps_far:
                first_send(step, 1, 2 * (chips - step)).start()
            first_send(0, 1, 0).start()

        @pl.when(core == 1)
        def _():
            loads["hid"].wait()
            pl.semaphore_wait(barrier, chips)
            pl.semaphore_signal(barrier, inc=1, device_id=device(0, 0), device_id_type=MESH)
            for step in steps_far:
                first_send(step, 1, 2 * (chips - step) + 1).start()

        for name in ("slot", "slot_m", "act", "in_gain", "cbc_s", "cbc_w", "cbc_b"):
            loads[name].wait()
        slot_row = slot_v[...]
        by_slot = iota((seqs, seqs), 0) == jnp.broadcast_to(slot_row, (seqs, seqs))
        to_slot = one_hot(by_slot)
        eye16 = eye(seqs)
        diagonal = iota((seqs, seqs), 0) == iota((seqs, seqs), 1)
        to_seq = dot_nt(eye16, to_slot).astype(BF16)
        act_f = jnp.broadcast_to(act_v[...].astype(F32), (seqs, seqs))
        live_row = act_v[...] > 0
        act_col = jnp.sum(jnp.where(diagonal, act_f, 0.0), axis=1, keepdims=True) > 0
        live_slot = jnp.sum(jnp.where(by_slot, act_f, 0.0), axis=1, keepdims=True) > 0
        bc_rows = jnp.concatenate([cbcw[...].astype(F32), cbcb[...].astype(F32)], axis=0)
        row_at, col_at = iota((bc_dev, bc_dev), 0), iota((bc_dev, bc_dev), 1)
        mirror = one_hot(col_at == row_at // SUBS * SUBS + lax.rem(SUBS - lax.rem(row_at, SUBS), SUBS))
        bc_cols = dot_nt(mirror, bc_rows.astype(BF16))
        bc_old = [dot_nt(mirror, dot(to_seq, cbcs[k]).astype(BF16)) for k in range(3)]
        bc_base = (bc_old[0] * bc_cols[:, 0:1] + bc_old[1] * bc_cols[:, 1:2]) + bc_old[2] * bc_cols[:, 2:3]
        pad = jnp.zeros((bc_dev, LANES - seqs), F32)
        side[core, 0] = jnp.concatenate([bc_base + bc_cols[:, 4:5], pad], axis=1)
        side[core, 1] = jnp.broadcast_to(bc_cols[:, 3:4], (bc_dev, LANES))
        loads["bc_w"].wait()
        bcw[core] = dot(mirror, bcw[core]).astype(BF16)

        def lend(j, ref):
            return pltpu.make_async_remote_copy(
                src_ref=ref.at[0], dst_ref=ref.at[0], send_sem=side_sem.at[0, j], recv_sem=side_sem.at[1, j],
                device_id=device(0, 1), device_id_type=MESH,
            )

        @pl.when(core == 0)
        def _():
            lend(0, side).start()
            lend(1, bcw).start()

        for name in ("cx_s", "cx_w", "cx_b", "norm_gain", "dt_bias", "log_rate", "skip_gain"):
            loads[name].wait()
        eye_ch = eye(chans)
        g0 = ngain[...].reshape(1, chans)
        g1 = g0.astype(BF16).astype(F32)
        g2 = (g0 - g1).astype(BF16).astype(F32)
        g3 = (g0 - g1) - g2
        rows = jnp.concatenate([cxw[...].astype(F32), cxb[...].astype(F32).reshape(1, chans), g1, g2, g3], axis=0)
        cols = dot_nt(eye_ch, rows.astype(BF16))
        gain_col = (cols[:, 5:6] + cols[:, 6:7]) + cols[:, 7:8]
        x_old = [dot_nt(eye_ch, dot(to_seq, cxs[k]).astype(BF16)) for k in range(3)]
        x_base = (x_old[0] * cols[:, 0:1] + x_old[1] * cols[:, 1:2]) + x_old[2] * cols[:, 2:3]
        loads["state"].wait()

        def narrow(i, carry):
            stb[i] = st[slot_m[0, i]].astype(BF16)
            return carry

        lax.fori_loop(0, seqs, narrow, 0)
        loads["dt_w"].wait()

        pltpu.make_async_remote_copy(
            src_ref=hid_recv.at[pl.ds(1, n_tp - 1)], dst_ref=hid_recv.at[pl.ds(1, n_tp - 1)],
            send_sem=send_sem.at[0], recv_sem=recv_sem.at[0],
            device_id=device(0, 1 - core), device_id_type=MESH,
        ).wait_recv()

        @pl.when(core == 1)
        def _():
            relay().start()

        blocks = [
            hid_recv[2 * lax.rem(t // 2 - chip + chips, chips) + t % 2].astype(F32) for t in range(n_tp)
        ]
        whole = jnp.concatenate(blocks, axis=1)
        for k in range(tiles):
            at = slice(k * LANES, (k + 1) * LANES)
            xn[:, at] = (whole[:, at] * gain[k : k + 1, :]).astype(BF16)
        squares = whole[:, :LANES] * whole[:, :LANES]
        for k in range(1, tiles):
            part = whole[:, k * LANES : (k + 1) * LANES]
            squares = squares + part * part
        inv_col = lax.rsqrt(jnp.sum(squares, axis=1, keepdims=True) / width + EPS)
        inv = jnp.sum(jnp.where(diagonal, jnp.broadcast_to(inv_col, (seqs, seqs)), 0.0), axis=0, keepdims=True)

        def all_of(phase, dst_ref, count):
            return pltpu.make_async_remote_copy(
                src_ref=dst_ref.at[pl.ds(0, count)], dst_ref=dst_ref.at[pl.ds(0, count)],
                send_sem=send_sem.at[phase], recv_sem=recv_sem.at[phase],
                device_id=device(0, 1 - core), device_id_type=MESH,
            )

        @pl.when(core == 1)
        def _():
            for j, ref in ((0, side), (1, bcw)):
                lend(j, ref).wait_recv()
            both = 2 * bc_dev
            base = jnp.concatenate([side[0, 0], side[1, 0]], axis=0)[:, :seqs]
            tap = jnp.concatenate([side[0, 1], side[1, 1]], axis=0)[:, :seqs]
            weights = jnp.concatenate([bcw[0], bcw[1]], axis=0)
            proj = dot_nt(weights[:, : width // 2], xn[:, : width // 2]) + dot_nt(weights[:, width // 2 :], xn[:, width // 2 :])
            bc_conv = silu(base + (proj * inv).astype(BF16).astype(F32) * tap).astype(BF16).astype(F32)
            spread = jnp.concatenate([bc_conv, jnp.zeros((both, LANES - seqs), F32)], axis=1)
            spread = pltpu.roll(spread.reshape(both // SUBS, SUBS, LANES), 0, 2, stride=seqs, stride_axis=1)
            bc_send[...] = jnp.sum(spread, axis=1)
            for step, which in [(step, which) for step in steps_far for which in (0, 1)] + [(0, 0)]:
                pltpu.make_async_remote_copy(
                    src_ref=bc_send, dst_ref=bc_recv.at[chip], send_sem=send_sem.at[1], recv_sem=recv_sem.at[1],
                    device_id=device(step, which), device_id_type=MESH,
                ).start()
            bc_recv[chip] = bc_send[...]

        dt_proj = (dot_nt(dtw[...], xn[...]) * inv).astype(BF16).astype(F32)
        loads["x_w"].wait()
        loads["z_w"].wait()
        x_proj = (dot_nt(xw[...], xn[...]) * inv).astype(BF16)
        z_proj = (dot_nt(zw[...], xn[...]) * inv).astype(BF16)
        x_conv = silu(x_base + x_proj.astype(F32) * cols[:, 3:4] + cols[:, 4:5]).astype(BF16)
        x_f = x_conv.astype(F32)
        z_gate = silu(z_proj.astype(F32))
        steps, decays = [], []
        for h in range(heads):
            raw = dt_proj[h : h + 1, :] + dtb_m[h]
            step = jnp.maximum(raw, 0.0) + jnp.log1p(jnp.exp(-jnp.abs(raw)))
            rate = jnp.exp(jnp.full((1, seqs), rate_m[h], F32))
            steps.append(jnp.where(live_row, step, 0.0))
            decays.append(jnp.where(live_row, jnp.exp(-step * rate), 1.0))

        def per_channel(values):
            return jnp.concatenate([jnp.broadcast_to(v, (HP, seqs)) for v in values], axis=0)

        dtx = per_channel(steps) * x_f
        decay = per_channel(decays)
        skipped = jnp.concatenate([jnp.full((HP, seqs), skip_m[h], F32) for h in range(heads)], axis=0) * x_f

        @pl.when(core == 0)
        def _():
            all_of(1, bc_recv, chips).wait_recv()

        @pl.when(core == 1)
        def _():
            all_of(1, bc_recv, chips - 1).wait_recv()


        def unpacked(at):
            found = []
            for row in range(NS // SUBS):
                line = at // SUBS + row
                lines = 2 * bc_dev // SUBS
                packed = bc_recv[line // lines, pl.ds(line % lines, 1), :]
                found.append(
                    pltpu.roll(jnp.broadcast_to(packed, (SUBS, LANES)), 0, 1, stride=seqs, stride_axis=0)
                )
            return jnp.concatenate(found, axis=0)[:, :seqs]

        c_f, b_f = unpacked(NS), unpacked(0)
        lane = iota((NS, seqs), 1)
        c_big = jnp.concatenate([jnp.where(lane == b, c_f, 0.0).astype(BF16) for b in range(seqs)], axis=0)
        s_c = []
        for at in (0, chans // 2):
            s_big = jnp.concatenate([stb[b, at : at + chans // 2, :] for b in range(seqs)], axis=1)
            s_c.append(dot(s_big, c_big))
        s_c = jnp.concatenate(s_c, axis=0)
        bc_dot = jnp.sum(b_f * c_f, axis=0, keepdims=True)
        y = (decay * s_c + dtx * bc_dot) + skipped
        gated = y * z_gate
        scaled = (gated * gain_col).astype(BF16)
        sq_row = jnp.broadcast_to(jnp.sum(gated * gated, axis=0, keepdims=True), (seqs, seqs))
        sq_col = jnp.sum(jnp.where(diagonal, sq_row, 0.0), axis=1, keepdims=True)
        sq_1 = sq_col.astype(BF16).astype(F32)
        sq_2 = (sq_col - sq_1).astype(BF16).astype(F32)
        sq_cols = [half_rows for term in (sq_1, sq_2, (sq_col - sq_1) - sq_2) for half_rows in (term[:SUBS], term[SUBS:])]
        loads["out_w"].wait()
        rows_seq = dot_nt(eye16, scaled).astype(BF16)
        lane_at = iota((SUBS, LANES), 1)
        spare = feats - LANES
        tails = {}
        for start in sorted({(t * feats) % LANES for t in range(n_tp)}):
            tail = jnp.zeros((SUBS, LANES), F32)
            for j, term in enumerate(sq_cols):
                tail = jnp.where(lane_at == (start + 2 * spare + j) % LANES, term, tail)
            tails[start] = tail

        def within(at):
            at = at % LANES
            return (lane_at >= at) & (lane_at < at + spare)

        side_of = chip // half
        half_width = half * 2 * feats
        for part in range(2):
            which = 1 - side_of if part == 0 else side_of
            step = 2 * LANES
            branch = jnp.concatenate(
                [
                    dot(rows_seq, ow[:, pl.ds(pl.multiple_of(which * half_width + at, LANES), step)])
                    for at in range(0, half_width, step)
                ],
                axis=1,
            )
            for i in range(2 * half):
                first, start = (i * feats) // LANES, (i * feats) % LANES
                tile_0 = branch[:, first * LANES : (first + 1) * LANES]
                tile_1 = branch[:, (first + 1) * LANES : (first + 2) * LANES]
                main = jnp.where(iota((seqs, LANES), 1) >= start, tile_0, tile_1)
                rest = jnp.where(within(start + spare), pltpu.roll(tile_1[SUBS:], spare, 1), tails[start])
                rest = jnp.where(within(start), tile_1[:SUBS], rest)
                br_send[which * 2 * half + i] = jnp.concatenate([main, rest], axis=0).astype(BF16)
            for i in range(half):
                far = which * half + lax.rem(chip + i, half)
                for flip in (1, 0):
                    if part == 1 and i == 0 and not flip:
                        continue
                    peer = far * 2 + (1 - core if flip else core)
                    pltpu.make_async_remote_copy(
                        src_ref=br_send.at[peer], dst_ref=br_recv.at[me],
                        send_sem=send_sem.at[2], recv_sem=recv_sem.at[2],
                        device_id={"tp": peer}, device_id_type=MESH,
                    ).start()
        br_recv[me] = br_send[me]

        x_now = dot_nt(to_slot, x_proj)
        bc_proj = (dot_nt(bcw[core], xn[...]) * inv).astype(BF16)
        bc_now = dot(dot_nt(to_slot, bc_proj).astype(BF16), mirror)
        for out, old, now in ((out_cx, cxs, x_now), (out_cbc, cbcs, bc_now)):
            held = [old[k].astype(F32) for k in range(3)]
            for k, new in enumerate((held[1], held[2], now)):
                out[k] = jnp.where(live_slot, new, held[k]).astype(BF16)
        of_heads = jnp.concatenate(steps + decays + [jnp.zeros((-2 * heads % SUBS, seqs), F32)], axis=0)
        of_heads = exact_dot(of_heads, to_seq)
        steps_slot = [of_heads[h : h + 1, :] for h in range(heads)]
        decays_slot = [of_heads[heads + h : heads + h + 1, :] for h in range(heads)]
        dtx_slot = per_channel(steps_slot) * dot(x_conv, to_seq)
        decay_slot = per_channel(decays_slot)
        b_rows = dot_nt(to_slot, b_f.astype(BF16))
        for b in range(seqs):
            grown = dtx_slot[:, b : b + 1] * b_rows[b : b + 1, :]
            out_state[b] = decay_slot[:, b : b + 1] * st[b] + grown

        all_of(2, br_recv, others).wait_recv()
        total = br_recv[0].astype(F32)
        for t in range(1, n_tp):
            total = total + br_recv[t].astype(F32)
        shift = lax.rem(me * feats, LANES)
        total = pltpu.roll(total, lax.rem(LANES - shift, LANES), 1)
        rest = total[seqs:]
        rest = jnp.concatenate([rest, pltpu.roll(rest, LANES - spare, 1)], axis=0)
        branch_sum = jnp.concatenate([total[:seqs], rest[:, :spare]], axis=1)
        sq_at = 2 * spare
        sq_rows = [
            (total[seqs:, at : at + 1] + total[seqs:, at + 2 : at + 3]) + total[seqs:, at + 4 : at + 5]
            for at in (sq_at, sq_at + 1)
        ]
        inv_out = lax.rsqrt(jnp.concatenate(sq_rows, axis=0) / INNER + EPS)
        kept = hid_recv[core].astype(F32)
        fresh = (kept + inv_out * branch_sum).astype(BF16).astype(F32)
        out_layer[...] = jnp.where(act_col, fresh, kept).astype(BF16)

        all_of(2, br_recv, others).wait_send()

        def hid_sent(count):
            return pltpu.make_async_remote_copy(
                src_ref=hid_recv.at[pl.ds(0, count)], dst_ref=hid_recv.at[pl.ds(0, count)],
                send_sem=send_sem.at[0], recv_sem=recv_sem.at[0],
                device_id=device(0, 1 - core), device_id_type=MESH,
            )

        @pl.when(core == 0)
        def _():
            hid_sent(chips).wait_send()
            for j, ref in ((0, side), (1, bcw)):
                lend(j, ref).wait_send()

        @pl.when(core == 1)
        def _():
            hid_sent(chips - 1).wait_send()
            relay().wait_send()
            all_of(1, bc_recv, others).wait_send()

    return body


def shards(
    hidden, in_gain, z_weight, x_weight, bc_weight, dt_weight, conv_x_weight, conv_x_bias,
    conv_bc_weight, conv_bc_bias, conv_x_state, conv_bc_state, dt_bias, log_rate, skip_gain,
    ssm_state, norm_gain, out_weight, pool_slot, active,
):
    n_tp = lax.axis_size("tp")
    seqs, feats = hidden.shape
    heads = ssm_state.shape[1]
    chans = z_weight.shape[1]
    bc_dev = bc_weight.shape[1]
    width = in_gain.shape[0]
    tiles = width // LANES
    vmem = pl.BlockSpec(memory_space=pltpu.VMEM)
    hbm = pl.BlockSpec(memory_space=pl.ANY)
    shape = jax.ShapeDtypeStruct
    results = (
        ((seqs, feats), BF16),
        ((3, seqs, chans), BF16),
        ((3, seqs, bc_dev), BF16),
        ((seqs, chans, NS), F32),
    )
    made = pl.pallas_call(
        make_kernel(n_tp, seqs, feats, heads, chans, bc_dev),
        out_shape=tuple(pltpu.VMEM(dims, kind) for dims, kind in results),
        in_specs=[hbm] * 20,
        out_specs=(vmem,) * 4,
        scratch_shapes=[
            pltpu.VMEM((chans, width), BF16),
            pltpu.VMEM((chans, width), BF16),
            pltpu.VMEM((2, bc_dev, width), BF16),
            pltpu.VMEM((heads, width), BF16),
            pltpu.VMEM((3, seqs, chans), BF16),
            pltpu.VMEM((3, seqs, bc_dev), BF16),
            pltpu.VMEM((seqs, chans, NS), F32),
            pltpu.VMEM((chans, width), BF16),
            pltpu.VMEM((tiles, LANES), F32),
            pltpu.VMEM((1, seqs), jnp.int32),
            pltpu.SMEM((1, seqs), jnp.int32),
            pltpu.VMEM((1, seqs), jnp.int32),
            pltpu.VMEM((4, chans), BF16),
            pltpu.VMEM((chans,), BF16),
            pltpu.VMEM((4, bc_dev), BF16),
            pltpu.VMEM((1, bc_dev), BF16),
            pltpu.VMEM((chans,), F32),
            pltpu.SMEM((heads,), F32),
            pltpu.SMEM((heads,), F32),
            pltpu.SMEM((heads,), F32),
            pltpu.VMEM((seqs, chans, NS), BF16),
            pltpu.VMEM((seqs, width), BF16),
            pltpu.VMEM((n_tp, seqs, feats), BF16),
            pltpu.VMEM((2, 2, bc_dev, LANES), F32),
            pltpu.VMEM((2 * bc_dev // SUBS, LANES), F32),
            pltpu.VMEM((n_tp, 2 * bc_dev // SUBS, LANES), F32),
            pltpu.VMEM((n_tp, seqs + SUBS, LANES), BF16),
            pltpu.VMEM((n_tp, seqs + SUBS, LANES), BF16),
            pltpu.SemaphoreType.DMA((20 + 1,)),
            pltpu.SemaphoreType.DMA((3,)),
            pltpu.SemaphoreType.DMA((3,)),
            pltpu.SemaphoreType.DMA((1,)),
            pltpu.SemaphoreType.DMA((2, 2)),
        ],
        compiler_params=pltpu.CompilerParams(
            collective_id=0, has_side_effects=True, vmem_limit_bytes=60 * 1024 * 1024
        ),
        name="step",
    )(
        hidden, pool_slot, active.reshape(1, seqs), in_gain.reshape(tiles, LANES),
        z_weight.T, x_weight.T, bc_weight.T, dt_weight.T,
        conv_x_weight, conv_x_bias, conv_bc_weight, conv_bc_bias.reshape(1, bc_dev),
        conv_x_state.transpose(1, 0, 2), conv_bc_state.transpose(1, 0, 2),
        dt_bias, log_rate, skip_gain, ssm_state.reshape(seqs, chans, NS),
        norm_gain, out_weight,
    )
    out_layer, out_cx, out_cbc, out_state = pl.pallas_call(
        put_out,
        out_shape=tuple(shape(dims, kind) for dims, kind in results),
        in_specs=[vmem] * 4,
        out_specs=(hbm,) * 4,
        scratch_shapes=[pltpu.SemaphoreType.DMA((7,))],
        name="put",
    )(*(pltpu.with_memory_space_constraint(x, pltpu.VMEM) for x in made))
    return (
        out_layer,
        out_cx.transpose(1, 0, 2),
        out_cbc.transpose(1, 0, 2),
        out_state.reshape(ssm_state.shape),
    )


def solution(mesh):
    rows = ("groups", "dp")
    placed = (
        P(rows, "tp"), P(), P(None, "tp"), P(None, "tp"), P(None, "tp"), P(None, "tp"), P(None, "tp"),
        P("tp"), P(None, "tp"), P("tp"), P(rows, None, "tp"), P(rows, None, "tp"), P("tp"), P("tp"),
        P("tp"), P(rows, "tp", None, None), P("tp"), P("tp", None), P(rows, None), P(rows),
    )
    return jax.shard_map(
        shards,
        mesh=mesh,
        in_specs=placed,
        out_specs=(P(rows, "tp"), P(rows, None, "tp"), P(rows, None, "tp"), P(rows, "tp", None, None)),
        check_vma=False,
    )
```

```python
import jax
import jax.numpy as jnp
from jax import lax
from jax.experimental import pallas as pl
from jax.experimental.pallas import tpu as pltpu
from jax.sharding import PartitionSpec as P

HP = 64
NS = 128
INNER = 5120
EPS = 1e-05
F32 = jnp.float32
BF16 = jnp.bfloat16
LANES = 128
SUBS = 8

NT = (((1,), (1,)), ((), ()))
MESH = pl.DeviceIdType.MESH


def dot(a, b):
    return jnp.dot(a, b, preferred_element_type=F32)


def dot_nt(a, b):
    return lax.dot_general(a, b, NT, preferred_element_type=F32)


def iota(shape, dim):
    return lax.broadcasted_iota(jnp.int32, shape, dim)


def one_hot(mask):
    return mask.astype(F32).astype(BF16)


def eye(n):
    return one_hot(iota((n, n), 0) == iota((n, n), 1))


def silu(x):
    return x * jax.nn.sigmoid(x)


def exact_dot(x, picks):
    first = x.astype(BF16)
    rest = x - first.astype(F32)
    second = rest.astype(BF16)
    third = (rest - second.astype(F32)).astype(BF16)
    return (dot(first, picks) + dot(second, picks)) + dot(third, picks)


def put_out(*refs):
    sems = refs[-1]
    pieces = 4
    rows = refs[3].shape[0] // pieces
    copies = [
        pltpu.make_async_copy(refs[3].at[pl.ds(k * rows, rows)], refs[7].at[pl.ds(k * rows, rows)], sems.at[3 + k])
        for k in range(pieces)
    ]
    copies += [pltpu.make_async_copy(refs[k], refs[4 + k], sems.at[k]) for k in range(3)]
    for copy in copies:
        copy.start()
    for copy in copies:
        copy.wait()


def make_kernel(n_tp, seqs, feats, heads, chans, bc_dev):
    width = n_tp * feats
    tiles = width // LANES
    chips = n_tp // 2
    half = chips // 2
    steps_far = [half]
    for far in range(half - 1, 0, -1):
        steps_far += [far, chips - far]
    others = n_tp - 1

    def body(
        hid, slot, act, in_gain, z_w, x_w, bc_w, dt_w, cx_w, cx_b, cbc_w, cbc_b, cx_s, cbc_s,
        dt_bias, log_rate, skip_gain, state, norm_gain, out_w,
        out_layer, out_cx, out_cbc, out_state,
        zw, xw, bcw, dtw, cxs, cbcs, st, ow, gain, slot_v, slot_m, act_v, cxw, cxb, cbcw, cbcb, ngain,
        dtb_m, rate_m, skip_m,
        stb, xn, hid_recv, side, bcw_send, bcw_recv, bc_sums, br_send, br_recv,
        in_sem, send_sem, recv_sem, relay_sem, side_sem,
    ):
        me = lax.axis_index("tp")
        chip, core = me // 2, lax.rem(me, 2)
        row = lax.axis_index("dp")
        odd = lax.rem(row, 2)
        barrier = pltpu.get_barrier_semaphore()

        def device(step, which):
            return {"tp": lax.rem(chip + step, chips) * 2 + which}

        loads = {}

        def load(name, src, dst):
            loads[name] = pltpu.make_async_copy(src, dst, in_sem.at[len(loads)])
            loads[name].start()

        load("hid", hid, hid_recv.at[core])

        @pl.when(core == 0)
        def _():
            pl.semaphore_signal(barrier, inc=1, device_id=device(0, 1), device_id_type=MESH)

        @pl.when(core == 1)
        def _():
            for step in steps_far:
                pl.semaphore_signal(barrier, inc=1, device_id=device(step, 1), device_id_type=MESH)

            @pl.when(odd == 0)
            def _():
                for t in range(n_tp):
                    pl.semaphore_signal(barrier, inc=1, device_id={"tp": t, "dp": row + 1}, device_id_type=MESH)

            @pl.when(odd == 1)
            def _():
                for step in steps_far:
                    pl.semaphore_signal(barrier, inc=1, device_id=device(step, 0), device_id_type=MESH)

        load("slot", slot, slot_v)
        load("slot_m", slot, slot_m)
        load("act", act, act_v)
        load("bc_w", bc_w, bcw)
        load("in_gain", in_gain, gain)
        load("cbc_s", cbc_s, cbcs)
        load("cbc_w", cbc_w, cbcw)
        load("cbc_b", cbc_b, cbcb)
        load("dt_w", dt_w, dtw)
        load("cx_s", cx_s, cxs)
        load("cx_w", cx_w, cxw)
        load("cx_b", cx_b, cxb)
        load("norm_gain", norm_gain, ngain)
        load("dt_bias", dt_bias, dtb_m)
        load("log_rate", log_rate, rate_m)
        load("skip_gain", skip_gain, skip_m)
        load("state", state, st)
        load("x_w", x_w, xw)
        load("z_w", z_w, zw)
        load("out_w", out_w, ow)

        def first_send(step, which, dst_slot, phase=0):
            return pltpu.make_async_remote_copy(
                src_ref=hid_recv.at[core], dst_ref=hid_recv.at[dst_slot],
                send_sem=send_sem.at[phase], recv_sem=recv_sem.at[phase],
                device_id=device(step, which), device_id_type=MESH,
            )

        def relay():
            return pltpu.make_async_remote_copy(
                src_ref=hid_recv.at[pl.ds(1, n_tp - 1)], dst_ref=hid_recv.at[pl.ds(1, n_tp - 1)],
                send_sem=relay_sem.at[0], recv_sem=recv_sem.at[0],
                device_id=device(0, 0), device_id_type=MESH,
            )

        @pl.when(core == 0)
        def _():
            loads["hid"].wait()
            pl.semaphore_wait(barrier, 1 + odd * (2 * chips - 1))
            first_send(0, 1, 0, 4).start()
            for step in steps_far:
                first_send(step, 1, 2 * (chips - step)).start()

        @pl.when(core == 1)
        def _():
            loads["hid"].wait()
            pl.semaphore_wait(barrier, chips + odd * chips)
            pl.semaphore_signal(barrier, inc=1, device_id=device(0, 0), device_id_type=MESH)
            for step in steps_far:
                first_send(step, 1, 2 * (chips - step) + 1).start()

        for name in ("slot", "slot_m", "act", "in_gain", "cbc_s", "cbc_w", "cbc_b"):
            loads[name].wait()
        slot_row = slot_v[...]
        by_slot = iota((seqs, seqs), 0) == jnp.broadcast_to(slot_row, (seqs, seqs))
        to_slot = one_hot(by_slot)
        eye16 = eye(seqs)
        diagonal = iota((seqs, seqs), 0) == iota((seqs, seqs), 1)
        to_seq = dot_nt(eye16, to_slot).astype(BF16)
        act_f = jnp.broadcast_to(act_v[...].astype(F32), (seqs, seqs))
        live_row = act_v[...] > 0
        act_col = jnp.sum(jnp.where(diagonal, act_f, 0.0), axis=1, keepdims=True) > 0
        live_slot = jnp.sum(jnp.where(by_slot, act_f, 0.0), axis=1, keepdims=True) > 0
        bc_rows = jnp.concatenate([cbcw[...].astype(F32), cbcb[...].astype(F32)], axis=0)
        row_at, col_at = iota((bc_dev, bc_dev), 0), iota((bc_dev, bc_dev), 1)
        mirror = one_hot(col_at == row_at // SUBS * SUBS + lax.rem(SUBS - lax.rem(row_at, SUBS), SUBS))
        bc_cols = dot_nt(mirror, bc_rows.astype(BF16))
        bc_old = [dot_nt(mirror, dot(to_seq, cbcs[k]).astype(BF16)) for k in range(3)]
        bc_base = (bc_old[0] * bc_cols[:, 0:1] + bc_old[1] * bc_cols[:, 1:2]) + bc_old[2] * bc_cols[:, 2:3]
        pad = jnp.zeros((bc_dev, LANES - seqs), F32)
        side[core, 0] = jnp.concatenate([bc_base + bc_cols[:, 4:5], pad], axis=1)
        side[core, 1] = jnp.broadcast_to(bc_cols[:, 3:4], (bc_dev, LANES))
        def lend():
            return pltpu.make_async_remote_copy(
                src_ref=side.at[0], dst_ref=side.at[0], send_sem=side_sem.at[0], recv_sem=side_sem.at[1],
                device_id=device(0, 1), device_id_type=MESH,
            )

        @pl.when(core == 0)
        def _():
            lend().start()

        loads["bc_w"].wait()
        turned = dot(mirror, bcw[...]).astype(BF16)
        bcw[...] = turned
        for k in range(tiles):
            bcw_send[k] = turned[:, k * LANES : (k + 1) * LANES]

        def share_tile(of_chip):
            return (of_chip * 2 * feats) // LANES

        def share(of_chip, to_row):
            return pltpu.make_async_remote_copy(
                src_ref=bcw_send.at[pl.ds(share_tile(of_chip), 3)], dst_ref=bcw_recv.at[me],
                send_sem=send_sem.at[3], recv_sem=recv_sem.at[3],
                device_id={"tp": 2 * of_chip + 1, "dp": to_row}, device_id_type=MESH,
            )

        @pl.when(odd == 1)
        def _():
            for step in steps_far:
                for to_row in (row - 1, row):
                    share(lax.rem(chip + step, chips), to_row).start()
            share(chip, row - 1).start()

            @pl.when(core == 0)
            def _():
                share(chip, row).start()

            @pl.when(core == 1)
            def _():
                bcw_recv[me] = bcw_send[pl.ds(share_tile(chip), 3)]

        for name in ("cx_s", "cx_w", "cx_b", "norm_gain", "dt_bias", "log_rate", "skip_gain"):
            loads[name].wait()
        eye_ch = eye(chans)
        g0 = ngain[...].reshape(1, chans)
        g1 = g0.astype(BF16).astype(F32)
        g2 = (g0 - g1).astype(BF16).astype(F32)
        g3 = (g0 - g1) - g2
        rows = jnp.concatenate([cxw[...].astype(F32), cxb[...].astype(F32).reshape(1, chans), g1, g2, g3], axis=0)
        cols = dot_nt(eye_ch, rows.astype(BF16))
        gain_col = (cols[:, 5:6] + cols[:, 6:7]) + cols[:, 7:8]
        x_old = [dot_nt(eye_ch, dot(to_seq, cxs[k]).astype(BF16)) for k in range(3)]
        x_base = (x_old[0] * cols[:, 0:1] + x_old[1] * cols[:, 1:2]) + x_old[2] * cols[:, 2:3]
        loads["state"].wait()

        def narrow(i, carry):
            stb[i] = st[slot_m[0, i]].astype(BF16)
            return carry

        lax.fori_loop(0, seqs, narrow, 0)
        loads["dt_w"].wait()

        def all_of(phase, dst_ref, count):
            return pltpu.make_async_remote_copy(
                src_ref=dst_ref.at[pl.ds(0, count)], dst_ref=dst_ref.at[pl.ds(0, count)],
                send_sem=send_sem.at[phase], recv_sem=recv_sem.at[phase],
                device_id=device(0, 1 - core), device_id_type=MESH,
            )

        lines = n_tp * bc_dev // SUBS
        own_lines = 2 * bc_dev // SUBS

        def packed(x):
            count = x.shape[0]
            spread = jnp.concatenate([x, jnp.zeros((count, LANES - seqs), F32)], axis=1)
            spread = pltpu.roll(spread.reshape(count // SUBS, SUBS, LANES), 0, 2, stride=seqs, stride_axis=1)
            return jnp.sum(spread, axis=1)

        def relay_sums():
            return pltpu.make_async_remote_copy(
                src_ref=bc_sums, dst_ref=bc_sums, send_sem=relay_sem.at[1], recv_sem=recv_sem.at[1],
                device_id=device(0, 0), device_id_type=MESH,
            )

        @pl.when(core == 1)
        def _():
            @pl.when(odd == 0)
            def _():
                all_of(3, bcw_recv, n_tp).wait_recv()

            @pl.when(odd == 1)
            def _():
                all_of(3, bcw_recv, n_tp - 1).wait_recv()

            first = share_tile(chip)
            first_send(0, 1, 0, 4).wait_recv()
            pair = jnp.concatenate([hid_recv[0].astype(F32), hid_recv[1].astype(F32), jnp.zeros((seqs, 3 * LANES - 2 * feats), F32)], axis=1)
            pair = pltpu.roll(pair, lax.rem(chip * 2 * feats, LANES), 1)
            terms = 0.0
            for k in range(3):
                scaled_k = (pair[:, k * LANES : (k + 1) * LANES] * gain[pl.ds(first + k, 1), :]).astype(BF16)
                weights = jnp.concatenate([bcw_recv[t, k] for t in range(n_tp)], axis=0)
                terms = terms + dot_nt(weights, scaled_k)
            bc_sums[chip, 0:lines, :] = packed(terms)
            lend().wait_recv()
            for j in range(2):
                own = packed(jnp.concatenate([side[0, j], side[1, j]], axis=0)[:, :seqs])
                bc_sums[chip, lines + j * own_lines : lines + (j + 1) * own_lines, :] = own
            for step in steps_far:
                pltpu.make_async_remote_copy(
                    src_ref=bc_sums.at[chip], dst_ref=bc_sums.at[chip], send_sem=send_sem.at[1], recv_sem=recv_sem.at[1],
                    device_id=device(step, 1), device_id_type=MESH,
                ).start()

        @pl.when(core == 0)
        def _():
            all_of(0, hid_recv, n_tp - 1).wait_recv()

        @pl.when(core == 1)
        def _():
            all_of(0, hid_recv, n_tp - 2).wait_recv()
            relay().start()

        blocks = [
            hid_recv[2 * lax.rem(t // 2 - chip + chips, chips) + t % 2].astype(F32) for t in range(n_tp)
        ]
        whole = jnp.concatenate(blocks, axis=1)
        for k in range(tiles):
            at = slice(k * LANES, (k + 1) * LANES)
            xn[:, at] = (whole[:, at] * gain[k : k + 1, :]).astype(BF16)
        squares = whole[:, :LANES] * whole[:, :LANES]
        for k in range(1, tiles):
            part = whole[:, k * LANES : (k + 1) * LANES]
            squares = squares + part * part
        inv_col = lax.rsqrt(jnp.sum(squares, axis=1, keepdims=True) / width + EPS)
        inv = jnp.sum(jnp.where(diagonal, jnp.broadcast_to(inv_col, (seqs, seqs)), 0.0), axis=0, keepdims=True)

        of_seq = lax.rem(iota((seqs, LANES), 1), seqs) == iota((seqs, LANES), 0)
        inv_lanes = jnp.sum(jnp.where(of_seq, jnp.broadcast_to(inv_col, (seqs, LANES)), 0.0), axis=0, keepdims=True)

        @pl.when(core == 1)
        def _():
            all_of(1, bc_sums, chips - 1).wait_recv()
            relay_sums().start()

        dt_proj = (dot_nt(dtw[...], xn[...]) * inv).astype(BF16).astype(F32)
        loads["x_w"].wait()
        loads["z_w"].wait()
        x_proj = (dot_nt(xw[...], xn[...]) * inv).astype(BF16)
        z_proj = (dot_nt(zw[...], xn[...]) * inv).astype(BF16)
        x_conv = silu(x_base + x_proj.astype(F32) * cols[:, 3:4] + cols[:, 4:5]).astype(BF16)
        x_f = x_conv.astype(F32)
        z_gate = silu(z_proj.astype(F32))
        steps, decays = [], []
        for h in range(heads):
            raw = dt_proj[h : h + 1, :] + dtb_m[h]
            step = jnp.maximum(raw, 0.0) + jnp.log1p(jnp.exp(-jnp.abs(raw)))
            rate = jnp.exp(jnp.full((1, seqs), rate_m[h], F32))
            steps.append(jnp.where(live_row, step, 0.0))
            decays.append(jnp.where(live_row, jnp.exp(-step * rate), 1.0))

        def per_channel(values):
            return jnp.concatenate([jnp.broadcast_to(v, (HP, seqs)) for v in values], axis=0)

        dtx = per_channel(steps) * x_f
        decay = per_channel(decays)
        skipped = jnp.concatenate([jnp.full((HP, seqs), skip_m[h], F32) for h in range(heads)], axis=0) * x_f

        @pl.when(core == 0)
        def _():
            all_of(1, bc_sums, chips).wait_recv()

        sums = bc_sums[0, 0:lines, :]
        for c in range(1, chips):
            sums = sums + bc_sums[c, 0:lines, :]
        base, tap = [
            jnp.concatenate([bc_sums[c, at : at + own_lines, :] for c in range(chips)], axis=0)
            for at in (lines, lines + own_lines)
        ]
        bc_conv = silu(base + (sums * inv_lanes).astype(BF16).astype(F32) * tap).astype(BF16).astype(F32)

        def unpacked(at):
            found = []
            for eight in range(NS // SUBS):
                line = bc_conv[at // SUBS + eight : at // SUBS + eight + 1, :]
                found.append(pltpu.roll(jnp.broadcast_to(line, (SUBS, LANES)), 0, 1, stride=seqs, stride_axis=0))
            return jnp.concatenate(found, axis=0)[:, :seqs]

        c_f, b_f = unpacked(NS), unpacked(0)
        lane = iota((NS, seqs), 1)
        c_big = jnp.concatenate([jnp.where(lane == b, c_f, 0.0).astype(BF16) for b in range(seqs)], axis=0)
        s_c = []
        for at in (0, chans // 2):
            s_big = jnp.concatenate([stb[b, at : at + chans // 2, :] for b in range(seqs)], axis=1)
            s_c.append(dot(s_big, c_big))
        s_c = jnp.concatenate(s_c, axis=0)
        bc_dot = jnp.sum(b_f * c_f, axis=0, keepdims=True)
        y = (decay * s_c + dtx * bc_dot) + skipped
        gated = y * z_gate
        scaled = (gated * gain_col).astype(BF16)
        sq_row = jnp.broadcast_to(jnp.sum(gated * gated, axis=0, keepdims=True), (seqs, seqs))
        sq_col = jnp.sum(jnp.where(diagonal, sq_row, 0.0), axis=1, keepdims=True)
        sq_1 = sq_col.astype(BF16).astype(F32)
        sq_2 = (sq_col - sq_1).astype(BF16).astype(F32)
        sq_cols = [half_rows for term in (sq_1, sq_2, (sq_col - sq_1) - sq_2) for half_rows in (term[:SUBS], term[SUBS:])]
        loads["out_w"].wait()
        rows_seq = dot_nt(eye16, scaled).astype(BF16)
        lane_at = iota((SUBS, LANES), 1)
        spare = feats - LANES
        tails = {}
        for start in sorted({(t * feats) % LANES for t in range(n_tp)}):
            tail = jnp.zeros((SUBS, LANES), F32)
            for j, term in enumerate(sq_cols):
                tail = jnp.where(lane_at == (start + 2 * spare + j) % LANES, term, tail)
            tails[start] = tail

        def within(at):
            at = at % LANES
            return (lane_at >= at) & (lane_at < at + spare)

        side_of = chip // half
        half_width = half * 2 * feats
        for part in range(2):
            which = 1 - side_of if part == 0 else side_of
            step = 2 * LANES
            branch = jnp.concatenate(
                [
                    dot(rows_seq, ow[:, pl.ds(pl.multiple_of(which * half_width + at, LANES), step)])
                    for at in range(0, half_width, step)
                ],
                axis=1,
            )
            for i in range(2 * half):
                first, start = (i * feats) // LANES, (i * feats) % LANES
                tile_0 = branch[:, first * LANES : (first + 1) * LANES]
                tile_1 = branch[:, (first + 1) * LANES : (first + 2) * LANES]
                main = jnp.where(iota((seqs, LANES), 1) >= start, tile_0, tile_1)
                rest = jnp.where(within(start + spare), pltpu.roll(tile_1[SUBS:], spare, 1), tails[start])
                rest = jnp.where(within(start), tile_1[:SUBS], rest)
                br_send[which * 2 * half + i] = jnp.concatenate([main, rest], axis=0).astype(BF16)
            for i in range(half):
                far = which * half + lax.rem(chip + i, half)
                for flip in (1, 0):
                    if part == 1 and i == 0 and not flip:
                        continue
                    peer = far * 2 + (1 - core if flip else core)
                    pltpu.make_async_remote_copy(
                        src_ref=br_send.at[peer], dst_ref=br_recv.at[me],
                        send_sem=send_sem.at[2], recv_sem=recv_sem.at[2],
                        device_id={"tp": peer}, device_id_type=MESH,
                    ).start()
        br_recv[me] = br_send[me]

        x_now = dot_nt(to_slot, x_proj)
        bc_proj = (dot_nt(bcw[...], xn[...]) * inv).astype(BF16)
        bc_now = dot(dot_nt(to_slot, bc_proj).astype(BF16), mirror)
        for out, old, now in ((out_cx, cxs, x_now), (out_cbc, cbcs, bc_now)):
            held = [old[k].astype(F32) for k in range(3)]
            for k, new in enumerate((held[1], held[2], now)):
                out[k] = jnp.where(live_slot, new, held[k]).astype(BF16)
        of_heads = jnp.concatenate(steps + decays + [jnp.zeros((-2 * heads % SUBS, seqs), F32)], axis=0)
        of_heads = exact_dot(of_heads, to_seq)
        steps_slot = [of_heads[h : h + 1, :] for h in range(heads)]
        decays_slot = [of_heads[heads + h : heads + h + 1, :] for h in range(heads)]
        dtx_slot = per_channel(steps_slot) * dot(x_conv, to_seq)
        decay_slot = per_channel(decays_slot)
        b_rows = dot_nt(to_slot, b_f.astype(BF16))
        for b in range(seqs):
            grown = dtx_slot[:, b : b + 1] * b_rows[b : b + 1, :]
            out_state[b] = decay_slot[:, b : b + 1] * st[b] + grown

        all_of(2, br_recv, others).wait_recv()
        total = br_recv[0].astype(F32)
        for t in range(1, n_tp):
            total = total + br_recv[t].astype(F32)
        shift = lax.rem(me * feats, LANES)
        total = pltpu.roll(total, lax.rem(LANES - shift, LANES), 1)
        rest = total[seqs:]
        rest = jnp.concatenate([rest, pltpu.roll(rest, LANES - spare, 1)], axis=0)
        branch_sum = jnp.concatenate([total[:seqs], rest[:, :spare]], axis=1)
        sq_at = 2 * spare
        sq_rows = [
            (total[seqs:, at : at + 1] + total[seqs:, at + 2 : at + 3]) + total[seqs:, at + 4 : at + 5]
            for at in (sq_at, sq_at + 1)
        ]
        inv_out = lax.rsqrt(jnp.concatenate(sq_rows, axis=0) / INNER + EPS)
        kept = hid_recv[core].astype(F32)
        fresh = (kept + inv_out * branch_sum).astype(BF16).astype(F32)
        out_layer[...] = jnp.where(act_col, fresh, kept).astype(BF16)

        all_of(2, br_recv, others).wait_send()

        def hid_sent(count):
            return pltpu.make_async_remote_copy(
                src_ref=hid_recv.at[pl.ds(0, count)], dst_ref=hid_recv.at[pl.ds(0, count)],
                send_sem=send_sem.at[0], recv_sem=recv_sem.at[0],
                device_id=device(0, 1 - core), device_id_type=MESH,
            )

        @pl.when((odd == 1) & (core == 0))
        def _():
            all_of(3, bcw_recv, n_tp).wait_send()

        @pl.when((odd == 1) & (core == 1))
        def _():
            all_of(3, bcw_recv, n_tp - 1).wait_send()

        @pl.when(core == 0)
        def _():
            hid_sent(chips - 1).wait_send()
            first_send(0, 1, 0, 4).wait_send()
            lend().wait_send()

        @pl.when(core == 1)
        def _():
            hid_sent(chips - 1).wait_send()
            relay().wait_send()
            relay_sums().wait_send()
            all_of(1, bc_sums, chips - 1).wait_send()

    return body


def shards(
    hidden, in_gain, z_weight, x_weight, bc_weight, dt_weight, conv_x_weight, conv_x_bias,
    conv_bc_weight, conv_bc_bias, conv_x_state, conv_bc_state, dt_bias, log_rate, skip_gain,
    ssm_state, norm_gain, out_weight, pool_slot, active,
):
    n_tp = lax.axis_size("tp")
    seqs, feats = hidden.shape
    heads = ssm_state.shape[1]
    chans = z_weight.shape[1]
    bc_dev = bc_weight.shape[1]
    width = in_gain.shape[0]
    tiles = width // LANES
    vmem = pl.BlockSpec(memory_space=pltpu.VMEM)
    hbm = pl.BlockSpec(memory_space=pl.ANY)
    shape = jax.ShapeDtypeStruct
    results = (
        ((seqs, feats), BF16),
        ((3, seqs, chans), BF16),
        ((3, seqs, bc_dev), BF16),
        ((seqs, chans, NS), F32),
    )
    made = pl.pallas_call(
        make_kernel(n_tp, seqs, feats, heads, chans, bc_dev),
        out_shape=tuple(pltpu.VMEM(dims, kind) for dims, kind in results),
        in_specs=[hbm] * 20,
        out_specs=(vmem,) * 4,
        scratch_shapes=[
            pltpu.VMEM((chans, width), BF16),
            pltpu.VMEM((chans, width), BF16),
            pltpu.VMEM((bc_dev, width), BF16),
            pltpu.VMEM((heads, width), BF16),
            pltpu.VMEM((3, seqs, chans), BF16),
            pltpu.VMEM((3, seqs, bc_dev), BF16),
            pltpu.VMEM((seqs, chans, NS), F32),
            pltpu.VMEM((chans, width), BF16),
            pltpu.VMEM((tiles, LANES), F32),
            pltpu.VMEM((1, seqs), jnp.int32),
            pltpu.SMEM((1, seqs), jnp.int32),
            pltpu.VMEM((1, seqs), jnp.int32),
            pltpu.VMEM((4, chans), BF16),
            pltpu.VMEM((chans,), BF16),
            pltpu.VMEM((4, bc_dev), BF16),
            pltpu.VMEM((1, bc_dev), BF16),
            pltpu.VMEM((chans,), F32),
            pltpu.SMEM((heads,), F32),
            pltpu.SMEM((heads,), F32),
            pltpu.SMEM((heads,), F32),
            pltpu.VMEM((seqs, chans, NS), BF16),
            pltpu.VMEM((seqs, width), BF16),
            pltpu.VMEM((n_tp, seqs, feats), BF16),
            pltpu.VMEM((2, 2, bc_dev, LANES), F32),
            pltpu.VMEM((tiles, bc_dev, LANES), BF16),
            pltpu.VMEM((n_tp, 3, bc_dev, LANES), BF16),
            pltpu.VMEM((n_tp // 2, (n_tp + 4) * bc_dev // SUBS, LANES), F32),
            pltpu.VMEM((n_tp, seqs + SUBS, LANES), BF16),
            pltpu.VMEM((n_tp, seqs + SUBS, LANES), BF16),
            pltpu.SemaphoreType.DMA((20 + 1,)),
            pltpu.SemaphoreType.DMA((5,)),
            pltpu.SemaphoreType.DMA((5,)),
            pltpu.SemaphoreType.DMA((2,)),
            pltpu.SemaphoreType.DMA((2,)),
        ],
        compiler_params=pltpu.CompilerParams(
            collective_id=0, has_side_effects=True, vmem_limit_bytes=60 * 1024 * 1024
        ),
        name="step",
    )(
        hidden, pool_slot, active.reshape(1, seqs), in_gain.reshape(tiles, LANES),
        z_weight.T, x_weight.T, bc_weight.T, dt_weight.T,
        conv_x_weight, conv_x_bias, conv_bc_weight, conv_bc_bias.reshape(1, bc_dev),
        conv_x_state.transpose(1, 0, 2), conv_bc_state.transpose(1, 0, 2),
        dt_bias, log_rate, skip_gain, ssm_state.reshape(seqs, chans, NS),
        norm_gain, out_weight,
    )
    out_layer, out_cx, out_cbc, out_state = pl.pallas_call(
        put_out,
        out_shape=tuple(shape(dims, kind) for dims, kind in results),
        in_specs=[vmem] * 4,
        out_specs=(hbm,) * 4,
        scratch_shapes=[pltpu.SemaphoreType.DMA((7,))],
        name="put",
    )(*(pltpu.with_memory_space_constraint(x, pltpu.VMEM) for x in made))
    return (
        out_layer,
        out_cx.transpose(1, 0, 2),
        out_cbc.transpose(1, 0, 2),
        out_state.reshape(ssm_state.shape),
    )


def solution(mesh):
    rows = ("groups", "dp")
    placed = (
        P(rows, "tp"), P(), P(None, "tp"), P(None, "tp"), P(None, "tp"), P(None, "tp"), P(None, "tp"),
        P("tp"), P(None, "tp"), P("tp"), P(rows, None, "tp"), P(rows, None, "tp"), P("tp"), P("tp"),
        P("tp"), P(rows, "tp", None, None), P("tp"), P("tp", None), P(rows, None), P(rows),
    )
    return jax.shard_map(
        shards,
        mesh=mesh,
        in_specs=placed,
        out_specs=(P(rows, "tp"), P(rows, None, "tp"), P(rows, None, "tp"), P(rows, "tp", None, None)),
        check_vma=False,
    )
```

```python
import jax
import jax.numpy as jnp
from jax import lax
from jax.experimental import pallas as pl
from jax.experimental.pallas import tpu as pltpu
from jax.sharding import PartitionSpec as P

HP = 64
NS = 128
INNER = 5120
EPS = 1e-05
F32 = jnp.float32
BF16 = jnp.bfloat16
LANES = 128
SUBS = 8

NT = (((1,), (1,)), ((), ()))
MESH = pl.DeviceIdType.MESH


def dot(a, b):
    return jnp.dot(a, b, preferred_element_type=F32)


def dot_nt(a, b):
    return lax.dot_general(a, b, NT, preferred_element_type=F32)


def iota(shape, dim):
    return lax.broadcasted_iota(jnp.int32, shape, dim)


def one_hot(mask):
    return mask.astype(F32).astype(BF16)


def eye(n):
    return one_hot(iota((n, n), 0) == iota((n, n), 1))


def silu(x):
    return x * jax.nn.sigmoid(x)


def exact_dot(x, picks):
    first = x.astype(BF16)
    rest = x - first.astype(F32)
    second = rest.astype(BF16)
    third = (rest - second.astype(F32)).astype(BF16)
    return (dot(first, picks) + dot(second, picks)) + dot(third, picks)


def put_out(*refs):
    sems = refs[-1]
    pieces = 4
    rows = refs[3].shape[0] // pieces
    copies = [
        pltpu.make_async_copy(refs[3].at[pl.ds(k * rows, rows)], refs[7].at[pl.ds(k * rows, rows)], sems.at[3 + k])
        for k in range(pieces)
    ]
    copies += [pltpu.make_async_copy(refs[k], refs[4 + k], sems.at[k]) for k in range(3)]
    for copy in copies:
        copy.start()
    for copy in copies:
        copy.wait()


def make_kernel(n_tp, seqs, feats, heads, chans, bc_dev):
    width = n_tp * feats
    tiles = width // LANES
    chips = n_tp // 2
    half = chips // 2
    steps_far = [half]
    for far in range(half - 1, 0, -1):
        steps_far += [far, chips - far]
    others = n_tp - 1

    def body(
        hid, slot, act, in_gain, z_w, x_w, bc_w, dt_w, cx_w, cx_b, cbc_w, cbc_b, cx_s, cbc_s,
        dt_bias, log_rate, skip_gain, state, norm_gain, out_w,
        out_layer, out_cx, out_cbc, out_state,
        zw, xw, bcw, dtw, cxs, cbcs, st, ow, gain, slot_v, slot_m, act_v, cxw, cxb, cbcw, cbcb, ngain,
        dtb_m, rate_m, skip_m,
        stb, xn, hid_recv, side, bcw_send, bcw_recv, bc_sums, bc_made, br_send, br_recv,
        in_sem, send_sem, recv_sem, relay_sem, side_sem,
    ):
        me = lax.axis_index("tp")
        chip, core = me // 2, lax.rem(me, 2)
        row = lax.axis_index("dp")
        odd = lax.rem(row, 2)
        barrier = pltpu.get_barrier_semaphore()

        def device(step, which):
            return {"tp": lax.rem(chip + step, chips) * 2 + which}

        loads = {}

        def load(name, src, dst):
            loads[name] = pltpu.make_async_copy(src, dst, in_sem.at[len(loads)])
            loads[name].start()

        load("hid", hid, hid_recv.at[core])

        @pl.when(core == 0)
        def _():
            pl.semaphore_signal(barrier, inc=1, device_id=device(0, 1), device_id_type=MESH)

        @pl.when(core == 1)
        def _():
            for step in steps_far:
                pl.semaphore_signal(barrier, inc=1, device_id=device(step, 1), device_id_type=MESH)

            @pl.when(odd == 0)
            def _():
                for t in range(n_tp):
                    pl.semaphore_signal(barrier, inc=1, device_id={"tp": t, "dp": row + 1}, device_id_type=MESH)

            @pl.when(odd == 1)
            def _():
                for step in steps_far:
                    pl.semaphore_signal(barrier, inc=1, device_id=device(step, 0), device_id_type=MESH)

        load("slot", slot, slot_v)
        load("slot_m", slot, slot_m)
        load("act", act, act_v)
        load("bc_w", bc_w, bcw)
        load("in_gain", in_gain, gain)
        load("cbc_s", cbc_s, cbcs)
        load("cbc_w", cbc_w, cbcw)
        load("cbc_b", cbc_b, cbcb)
        load("dt_w", dt_w, dtw)
        load("cx_s", cx_s, cxs)
        load("cx_w", cx_w, cxw)
        load("cx_b", cx_b, cxb)
        load("norm_gain", norm_gain, ngain)
        load("dt_bias", dt_bias, dtb_m)
        load("log_rate", log_rate, rate_m)
        load("skip_gain", skip_gain, skip_m)
        load("state", state, st)
        load("x_w", x_w, xw)
        load("z_w", z_w, zw)
        load("out_w", out_w, ow)

        def first_send(step, which, dst_slot, phase=0):
            return pltpu.make_async_remote_copy(
                src_ref=hid_recv.at[core], dst_ref=hid_recv.at[dst_slot],
                send_sem=send_sem.at[phase], recv_sem=recv_sem.at[phase],
                device_id=device(step, which), device_id_type=MESH,
            )

        def relay():
            return pltpu.make_async_remote_copy(
                src_ref=hid_recv.at[pl.ds(1, n_tp - 1)], dst_ref=hid_recv.at[pl.ds(1, n_tp - 1)],
                send_sem=relay_sem.at[0], recv_sem=recv_sem.at[0],
                device_id=device(0, 0), device_id_type=MESH,
            )

        @pl.when(core == 0)
        def _():
            loads["hid"].wait()
            pl.semaphore_wait(barrier, 1 + odd * (2 * chips - 1))
            first_send(0, 1, 0, 4).start()
            for step in steps_far:
                first_send(step, 1, 2 * (chips - step)).start()

        for name in ("slot", "slot_m", "act", "in_gain", "cbc_s", "cbc_w", "cbc_b"):
            loads[name].wait()
        slot_row = slot_v[...]
        by_slot = iota((seqs, seqs), 0) == jnp.broadcast_to(slot_row, (seqs, seqs))
        to_slot = one_hot(by_slot)
        eye16 = eye(seqs)
        diagonal = iota((seqs, seqs), 0) == iota((seqs, seqs), 1)
        to_seq = dot_nt(eye16, to_slot).astype(BF16)
        act_f = jnp.broadcast_to(act_v[...].astype(F32), (seqs, seqs))
        live_row = act_v[...] > 0
        act_col = jnp.sum(jnp.where(diagonal, act_f, 0.0), axis=1, keepdims=True) > 0
        live_slot = jnp.sum(jnp.where(by_slot, act_f, 0.0), axis=1, keepdims=True) > 0
        bc_rows = jnp.concatenate([cbcw[...].astype(F32), cbcb[...].astype(F32)], axis=0)
        row_at, col_at = iota((bc_dev, bc_dev), 0), iota((bc_dev, bc_dev), 1)
        mirror = one_hot(col_at == row_at // SUBS * SUBS + lax.rem(SUBS - lax.rem(row_at, SUBS), SUBS))
        bc_cols = dot_nt(mirror, bc_rows.astype(BF16))
        bc_old = [dot_nt(mirror, dot(to_seq, cbcs[k]).astype(BF16)) for k in range(3)]
        bc_base = (bc_old[0] * bc_cols[:, 0:1] + bc_old[1] * bc_cols[:, 1:2]) + bc_old[2] * bc_cols[:, 2:3]
        pad = jnp.zeros((bc_dev, LANES - seqs), F32)
        side[core, 0] = jnp.concatenate([bc_base + bc_cols[:, 4:5], pad], axis=1)
        side[core, 1] = jnp.broadcast_to(bc_cols[:, 3:4], (bc_dev, LANES))
        def lend():
            return pltpu.make_async_remote_copy(
                src_ref=side.at[0], dst_ref=side.at[0], send_sem=side_sem.at[0], recv_sem=side_sem.at[1],
                device_id=device(0, 1), device_id_type=MESH,
            )

        @pl.when(core == 0)
        def _():
            lend().start()

        loads["bc_w"].wait()
        turned = dot(mirror, bcw[...]).astype(BF16)
        bcw[...] = turned
        for k in range(tiles):
            bcw_send[k] = turned[:, k * LANES : (k + 1) * LANES]

        def share_tile(of_chip):
            return (of_chip * 2 * feats) // LANES

        def share(of_chip, to_row):
            return pltpu.make_async_remote_copy(
                src_ref=bcw_send.at[pl.ds(share_tile(of_chip), 3)], dst_ref=bcw_recv.at[me],
                send_sem=send_sem.at[3], recv_sem=recv_sem.at[3],
                device_id={"tp": 2 * of_chip + 1, "dp": to_row}, device_id_type=MESH,
            )

        for name in ("cx_s", "cx_w", "cx_b", "norm_gain", "dt_bias", "log_rate", "skip_gain"):
            loads[name].wait()
        eye_ch = eye(chans)
        g0 = ngain[...].reshape(1, chans)
        g1 = g0.astype(BF16).astype(F32)
        g2 = (g0 - g1).astype(BF16).astype(F32)
        g3 = (g0 - g1) - g2
        rows = jnp.concatenate([cxw[...].astype(F32), cxb[...].astype(F32).reshape(1, chans), g1, g2, g3], axis=0)
        cols = dot_nt(eye_ch, rows.astype(BF16))
        gain_col = (cols[:, 5:6] + cols[:, 6:7]) + cols[:, 7:8]
        x_old = [dot_nt(eye_ch, dot(to_seq, cxs[k]).astype(BF16)) for k in range(3)]
        x_base = (x_old[0] * cols[:, 0:1] + x_old[1] * cols[:, 1:2]) + x_old[2] * cols[:, 2:3]
        loads["state"].wait()

        def narrow(i, carry):
            stb[i] = st[slot_m[0, i]].astype(BF16)
            return carry

        lax.fori_loop(0, seqs, narrow, 0)
        loads["dt_w"].wait()

        @pl.when(core == 1)
        def _():
            loads["hid"].wait()
            pl.semaphore_wait(barrier, chips + odd * chips)
            pl.semaphore_signal(barrier, inc=1, device_id=device(0, 0), device_id_type=MESH)
            for step in steps_far:
                first_send(step, 1, 2 * (chips - step) + 1).start()

        @pl.when(odd == 1)
        def _():
            for step in steps_far:
                for to_row in (row - 1, row):
                    share(lax.rem(chip + step, chips), to_row).start()
            share(chip, row - 1).start()

            @pl.when(core == 0)
            def _():
                share(chip, row).start()

            @pl.when(core == 1)
            def _():
                bcw_recv[me] = bcw_send[pl.ds(share_tile(chip), 3)]


        def all_of(phase, dst_ref, count):
            return pltpu.make_async_remote_copy(
                src_ref=dst_ref.at[pl.ds(0, count)], dst_ref=dst_ref.at[pl.ds(0, count)],
                send_sem=send_sem.at[phase], recv_sem=recv_sem.at[phase],
                device_id=device(0, 1 - core), device_id_type=MESH,
            )

        lines = n_tp * bc_dev // SUBS
        own_lines = 2 * bc_dev // SUBS

        def packed(x):
            count = x.shape[0]
            spread = jnp.concatenate([x, jnp.zeros((count, LANES - seqs), F32)], axis=1)
            spread = pltpu.roll(spread.reshape(count // SUBS, SUBS, LANES), 0, 2, stride=seqs, stride_axis=1)
            return jnp.sum(spread, axis=1)

        def relay_made():
            return pltpu.make_async_remote_copy(
                src_ref=bc_made, dst_ref=bc_made, send_sem=relay_sem.at[1], recv_sem=recv_sem.at[1],
                device_id=device(0, 0), device_id_type=MESH,
            )

        @pl.when(core == 1)
        def _():
            @pl.when(odd == 0)
            def _():
                all_of(3, bcw_recv, n_tp).wait_recv()

            @pl.when(odd == 1)
            def _():
                all_of(3, bcw_recv, n_tp - 1).wait_recv()

            first = share_tile(chip)
            first_send(0, 1, 0, 4).wait_recv()
            pair = jnp.concatenate([hid_recv[0].astype(F32), hid_recv[1].astype(F32), jnp.zeros((seqs, 3 * LANES - 2 * feats), F32)], axis=1)
            pair = pltpu.roll(pair, lax.rem(chip * 2 * feats, LANES), 1)
            terms = 0.0
            for k in range(3):
                scaled_k = (pair[:, k * LANES : (k + 1) * LANES] * gain[pl.ds(first + k, 1), :]).astype(BF16)
                weights = jnp.concatenate([bcw_recv[t, k] for t in range(n_tp)], axis=0)
                terms = terms + dot_nt(weights, scaled_k)
            bc_sums[chip, 0:lines, :] = packed(terms)
            lend().wait_recv()
            for j in range(2):
                own = packed(jnp.concatenate([side[0, j], side[1, j]], axis=0)[:, :seqs])
                bc_sums[chip, lines + j * own_lines : lines + (j + 1) * own_lines, :] = own
            for step in steps_far:
                pltpu.make_async_remote_copy(
                    src_ref=bc_sums.at[chip], dst_ref=bc_sums.at[chip], send_sem=send_sem.at[1], recv_sem=recv_sem.at[1],
                    device_id=device(step, 1), device_id_type=MESH,
                ).start()

        @pl.when(core == 0)
        def _():
            all_of(0, hid_recv, n_tp - 1).wait_recv()

        @pl.when(core == 1)
        def _():
            all_of(0, hid_recv, n_tp - 2).wait_recv()
            relay().start()

        blocks = [
            hid_recv[2 * lax.rem(t // 2 - chip + chips, chips) + t % 2].astype(F32) for t in range(n_tp)
        ]
        whole = jnp.concatenate(blocks, axis=1)
        for k in range(tiles):
            at = slice(k * LANES, (k + 1) * LANES)
            xn[:, at] = (whole[:, at] * gain[k : k + 1, :]).astype(BF16)
        squares = whole[:, :LANES] * whole[:, :LANES]
        for k in range(1, tiles):
            part = whole[:, k * LANES : (k + 1) * LANES]
            squares = squares + part * part
        inv_col = lax.rsqrt(jnp.sum(squares, axis=1, keepdims=True) / width + EPS)
        inv = jnp.sum(jnp.where(diagonal, jnp.broadcast_to(inv_col, (seqs, seqs)), 0.0), axis=0, keepdims=True)

        of_seq = lax.rem(iota((seqs, LANES), 1), seqs) == iota((seqs, LANES), 0)
        inv_lanes = jnp.sum(jnp.where(of_seq, jnp.broadcast_to(inv_col, (seqs, LANES)), 0.0), axis=0, keepdims=True)

        dt_proj = (dot_nt(dtw[...], xn[...]) * inv).astype(BF16).astype(F32)
        loads["x_w"].wait()
        loads["z_w"].wait()
        x_proj = (dot_nt(xw[...], xn[...]) * inv).astype(BF16)
        z_proj = (dot_nt(zw[...], xn[...]) * inv).astype(BF16)
        x_conv = silu(x_base + x_proj.astype(F32) * cols[:, 3:4] + cols[:, 4:5]).astype(BF16)
        x_f = x_conv.astype(F32)
        z_gate = silu(z_proj.astype(F32))
        steps, decays = [], []
        for h in range(heads):
            raw = dt_proj[h : h + 1, :] + dtb_m[h]
            step = jnp.maximum(raw, 0.0) + jnp.log1p(jnp.exp(-jnp.abs(raw)))
            rate = jnp.exp(jnp.full((1, seqs), rate_m[h], F32))
            steps.append(jnp.where(live_row, step, 0.0))
            decays.append(jnp.where(live_row, jnp.exp(-step * rate), 1.0))

        def per_channel(values):
            return jnp.concatenate([jnp.broadcast_to(v, (HP, seqs)) for v in values], axis=0)

        dtx = per_channel(steps) * x_f
        decay = per_channel(decays)
        skipped = jnp.concatenate([jnp.full((HP, seqs), skip_m[h], F32) for h in range(heads)], axis=0) * x_f

        @pl.when(core == 1)
        def _():
            all_of(1, bc_sums, chips - 1).wait_recv()
            sums = bc_sums[0, 0:lines, :]
            for c in range(1, chips):
                sums = sums + bc_sums[c, 0:lines, :]
            base, tap = [
                jnp.concatenate([bc_sums[c, at : at + own_lines, :] for c in range(chips)], axis=0)
                for at in (lines, lines + own_lines)
            ]
            made = silu(base + (sums * inv_lanes).astype(BF16).astype(F32) * tap)
            bc_made[...] = made.astype(BF16).astype(F32)
            relay_made().start()

        @pl.when(core == 0)
        def _():
            relay_made().wait_recv()

        bc_conv = bc_made[...]

        def unpacked(at):
            found = []
            for eight in range(NS // SUBS):
                line = bc_conv[at // SUBS + eight : at // SUBS + eight + 1, :]
                found.append(pltpu.roll(jnp.broadcast_to(line, (SUBS, LANES)), 0, 1, stride=seqs, stride_axis=0))
            return jnp.concatenate(found, axis=0)[:, :seqs]

        c_f, b_f = unpacked(NS), unpacked(0)
        lane = iota((NS, seqs), 1)
        c_big = jnp.concatenate([jnp.where(lane == b, c_f, 0.0).astype(BF16) for b in range(seqs)], axis=0)
        s_c = []
        for at in (0, chans // 2):
            s_big = jnp.concatenate([stb[b, at : at + chans // 2, :] for b in range(seqs)], axis=1)
            s_c.append(dot(s_big, c_big))
        s_c = jnp.concatenate(s_c, axis=0)
        bc_dot = jnp.sum(b_f * c_f, axis=0, keepdims=True)
        y = (decay * s_c + dtx * bc_dot) + skipped
        gated = y * z_gate
        scaled = (gated * gain_col).astype(BF16)
        sq_row = jnp.broadcast_to(jnp.sum(gated * gated, axis=0, keepdims=True), (seqs, seqs))
        sq_col = jnp.sum(jnp.where(diagonal, sq_row, 0.0), axis=1, keepdims=True)
        sq_1 = sq_col.astype(BF16).astype(F32)
        sq_2 = (sq_col - sq_1).astype(BF16).astype(F32)
        sq_cols = [half_rows for term in (sq_1, sq_2, (sq_col - sq_1) - sq_2) for half_rows in (term[:SUBS], term[SUBS:])]
        loads["out_w"].wait()
        rows_seq = dot_nt(eye16, scaled).astype(BF16)
        lane_at = iota((SUBS, LANES), 1)
        spare = feats - LANES
        tails = {}
        for start in sorted({(t * feats) % LANES for t in range(n_tp)}):
            tail = jnp.zeros((SUBS, LANES), F32)
            for j, term in enumerate(sq_cols):
                tail = jnp.where(lane_at == (start + 2 * spare + j) % LANES, term, tail)
            tails[start] = tail

        def within(at):
            at = at % LANES
            return (lane_at >= at) & (lane_at < at + spare)

        side_of = chip // half
        half_width = half * 2 * feats
        for part in range(2):
            which = 1 - side_of if part == 0 else side_of
            step = 2 * LANES
            branch = jnp.concatenate(
                [
                    dot(rows_seq, ow[:, pl.ds(pl.multiple_of(which * half_width + at, LANES), step)])
                    for at in range(0, half_width, step)
                ],
                axis=1,
            )
            for i in range(2 * half):
                first, start = (i * feats) // LANES, (i * feats) % LANES
                tile_0 = branch[:, first * LANES : (first + 1) * LANES]
                tile_1 = branch[:, (first + 1) * LANES : (first + 2) * LANES]
                main = jnp.where(iota((seqs, LANES), 1) >= start, tile_0, tile_1)
                rest = jnp.where(within(start + spare), pltpu.roll(tile_1[SUBS:], spare, 1), tails[start])
                rest = jnp.where(within(start), tile_1[:SUBS], rest)
                br_send[which * 2 * half + i] = jnp.concatenate([main, rest], axis=0).astype(BF16)
            for i in range(half):
                far = which * half + lax.rem(chip + i, half)
                for flip in (1, 0):
                    if part == 1 and i == 0 and not flip:
                        continue
                    peer = far * 2 + (1 - core if flip else core)
                    pltpu.make_async_remote_copy(
                        src_ref=br_send.at[peer], dst_ref=br_recv.at[me],
                        send_sem=send_sem.at[2], recv_sem=recv_sem.at[2],
                        device_id={"tp": peer}, device_id_type=MESH,
                    ).start()
        br_recv[me] = br_send[me]

        x_now = dot_nt(to_slot, x_proj)
        bc_proj = (dot_nt(bcw[...], xn[...]) * inv).astype(BF16)
        bc_now = dot(dot_nt(to_slot, bc_proj).astype(BF16), mirror)
        for out, old, now in ((out_cx, cxs, x_now), (out_cbc, cbcs, bc_now)):
            held = [old[k].astype(F32) for k in range(3)]
            for k, new in enumerate((held[1], held[2], now)):
                out[k] = jnp.where(live_slot, new, held[k]).astype(BF16)
        of_heads = jnp.concatenate(steps + decays + [jnp.zeros((-2 * heads % SUBS, seqs), F32)], axis=0)
        of_heads = exact_dot(of_heads, to_seq)
        steps_slot = [of_heads[h : h + 1, :] for h in range(heads)]
        decays_slot = [of_heads[heads + h : heads + h + 1, :] for h in range(heads)]
        dtx_slot = per_channel(steps_slot) * dot(x_conv, to_seq)
        decay_slot = per_channel(decays_slot)
        b_rows = dot_nt(to_slot, b_f.astype(BF16))
        for b in range(seqs):
            grown = dtx_slot[:, b : b + 1] * b_rows[b : b + 1, :]
            out_state[b] = decay_slot[:, b : b + 1] * st[b] + grown

        all_of(2, br_recv, others).wait_recv()
        total = br_recv[0].astype(F32)
        for t in range(1, n_tp):
            total = total + br_recv[t].astype(F32)
        shift = lax.rem(me * feats, LANES)
        total = pltpu.roll(total, lax.rem(LANES - shift, LANES), 1)
        rest = total[seqs:]
        rest = jnp.concatenate([rest, pltpu.roll(rest, LANES - spare, 1)], axis=0)
        branch_sum = jnp.concatenate([total[:seqs], rest[:, :spare]], axis=1)
        sq_at = 2 * spare
        sq_rows = [
            (total[seqs:, at : at + 1] + total[seqs:, at + 2 : at + 3]) + total[seqs:, at + 4 : at + 5]
            for at in (sq_at, sq_at + 1)
        ]
        inv_out = lax.rsqrt(jnp.concatenate(sq_rows, axis=0) / INNER + EPS)
        kept = hid_recv[core].astype(F32)
        fresh = (kept + inv_out * branch_sum).astype(BF16).astype(F32)
        out_layer[...] = jnp.where(act_col, fresh, kept).astype(BF16)

        all_of(2, br_recv, others).wait_send()

        def hid_sent(count):
            return pltpu.make_async_remote_copy(
                src_ref=hid_recv.at[pl.ds(0, count)], dst_ref=hid_recv.at[pl.ds(0, count)],
                send_sem=send_sem.at[0], recv_sem=recv_sem.at[0],
                device_id=device(0, 1 - core), device_id_type=MESH,
            )

        @pl.when((odd == 1) & (core == 0))
        def _():
            all_of(3, bcw_recv, n_tp).wait_send()

        @pl.when((odd == 1) & (core == 1))
        def _():
            all_of(3, bcw_recv, n_tp - 1).wait_send()

        @pl.when(core == 0)
        def _():
            hid_sent(chips - 1).wait_send()
            first_send(0, 1, 0, 4).wait_send()
            lend().wait_send()

        @pl.when(core == 1)
        def _():
            hid_sent(chips - 1).wait_send()
            relay().wait_send()
            relay_made().wait_send()
            all_of(1, bc_sums, chips - 1).wait_send()

    return body


def shards(
    hidden, in_gain, z_weight, x_weight, bc_weight, dt_weight, conv_x_weight, conv_x_bias,
    conv_bc_weight, conv_bc_bias, conv_x_state, conv_bc_state, dt_bias, log_rate, skip_gain,
    ssm_state, norm_gain, out_weight, pool_slot, active,
):
    n_tp = lax.axis_size("tp")
    seqs, feats = hidden.shape
    heads = ssm_state.shape[1]
    chans = z_weight.shape[1]
    bc_dev = bc_weight.shape[1]
    width = in_gain.shape[0]
    tiles = width // LANES
    vmem = pl.BlockSpec(memory_space=pltpu.VMEM)
    hbm = pl.BlockSpec(memory_space=pl.ANY)
    shape = jax.ShapeDtypeStruct
    results = (
        ((seqs, feats), BF16),
        ((3, seqs, chans), BF16),
        ((3, seqs, bc_dev), BF16),
        ((seqs, chans, NS), F32),
    )
    made = pl.pallas_call(
        make_kernel(n_tp, seqs, feats, heads, chans, bc_dev),
        out_shape=tuple(pltpu.VMEM(dims, kind) for dims, kind in results),
        in_specs=[hbm] * 20,
        out_specs=(vmem,) * 4,
        scratch_shapes=[
            pltpu.VMEM((chans, width), BF16),
            pltpu.VMEM((chans, width), BF16),
            pltpu.VMEM((bc_dev, width), BF16),
            pltpu.VMEM((heads, width), BF16),
            pltpu.VMEM((3, seqs, chans), BF16),
            pltpu.VMEM((3, seqs, bc_dev), BF16),
            pltpu.VMEM((seqs, chans, NS), F32),
            pltpu.VMEM((chans, width), BF16),
            pltpu.VMEM((tiles, LANES), F32),
            pltpu.VMEM((1, seqs), jnp.int32),
            pltpu.SMEM((1, seqs), jnp.int32),
            pltpu.VMEM((1, seqs), jnp.int32),
            pltpu.VMEM((4, chans), BF16),
            pltpu.VMEM((chans,), BF16),
            pltpu.VMEM((4, bc_dev), BF16),
            pltpu.VMEM((1, bc_dev), BF16),
            pltpu.VMEM((chans,), F32),
            pltpu.SMEM((heads,), F32),
            pltpu.SMEM((heads,), F32),
            pltpu.SMEM((heads,), F32),
            pltpu.VMEM((seqs, chans, NS), BF16),
            pltpu.VMEM((seqs, width), BF16),
            pltpu.VMEM((n_tp, seqs, feats), BF16),
            pltpu.VMEM((2, 2, bc_dev, LANES), F32),
            pltpu.VMEM((tiles, bc_dev, LANES), BF16),
            pltpu.VMEM((n_tp, 3, bc_dev, LANES), BF16),
            pltpu.VMEM((n_tp // 2, (n_tp + 4) * bc_dev // SUBS, LANES), F32),
            pltpu.VMEM((n_tp * bc_dev // SUBS, LANES), F32),
            pltpu.VMEM((n_tp, seqs + SUBS, LANES), BF16),
            pltpu.VMEM((n_tp, seqs + SUBS, LANES), BF16),
            pltpu.SemaphoreType.DMA((20 + 1,)),
            pltpu.SemaphoreType.DMA((5,)),
            pltpu.SemaphoreType.DMA((5,)),
            pltpu.SemaphoreType.DMA((2,)),
            pltpu.SemaphoreType.DMA((2,)),
        ],
        compiler_params=pltpu.CompilerParams(
            collective_id=0, has_side_effects=True, vmem_limit_bytes=60 * 1024 * 1024
        ),
        name="step",
    )(
        hidden, pool_slot, active.reshape(1, seqs), in_gain.reshape(tiles, LANES),
        z_weight.T, x_weight.T, bc_weight.T, dt_weight.T,
        conv_x_weight, conv_x_bias, conv_bc_weight, conv_bc_bias.reshape(1, bc_dev),
        conv_x_state.transpose(1, 0, 2), conv_bc_state.transpose(1, 0, 2),
        dt_bias, log_rate, skip_gain, ssm_state.reshape(seqs, chans, NS),
        norm_gain, out_weight,
    )
    out_layer, out_cx, out_cbc, out_state = pl.pallas_call(
        put_out,
        out_shape=tuple(shape(dims, kind) for dims, kind in results),
        in_specs=[vmem] * 4,
        out_specs=(hbm,) * 4,
        scratch_shapes=[pltpu.SemaphoreType.DMA((7,))],
        name="put",
    )(*(pltpu.with_memory_space_constraint(x, pltpu.VMEM) for x in made))
    return (
        out_layer,
        out_cx.transpose(1, 0, 2),
        out_cbc.transpose(1, 0, 2),
        out_state.reshape(ssm_state.shape),
    )


def solution(mesh):
    rows = ("groups", "dp")
    placed = (
        P(rows, "tp"), P(), P(None, "tp"), P(None, "tp"), P(None, "tp"), P(None, "tp"), P(None, "tp"),
        P("tp"), P(None, "tp"), P("tp"), P(rows, None, "tp"), P(rows, None, "tp"), P("tp"), P("tp"),
        P("tp"), P(rows, "tp", None, None), P("tp"), P("tp", None), P(rows, None), P(rows),
    )
    return jax.shard_map(
        shards,
        mesh=mesh,
        in_specs=placed,
        out_specs=(P(rows, "tp"), P(rows, None, "tp"), P(rows, None, "tp"), P(rows, "tp", None, None)),
        check_vma=False,
    )
```

```python
import jax
import jax.numpy as jnp
from jax import lax
from jax.experimental import pallas as pl
from jax.experimental.pallas import tpu as pltpu
from jax.sharding import PartitionSpec as P

HP = 64
NS = 128
INNER = 5120
EPS = 1e-05
F32 = jnp.float32
BF16 = jnp.bfloat16
LANES = 128
SUBS = 8

NT = (((1,), (1,)), ((), ()))
MESH = pl.DeviceIdType.MESH


def dot(a, b):
    return jnp.dot(a, b, preferred_element_type=F32)


def dot_nt(a, b):
    return lax.dot_general(a, b, NT, preferred_element_type=F32)


def iota(shape, dim):
    return lax.broadcasted_iota(jnp.int32, shape, dim)


def one_hot(mask):
    return mask.astype(F32).astype(BF16)


def eye(n):
    return one_hot(iota((n, n), 0) == iota((n, n), 1))


def silu(x):
    return x * jax.nn.sigmoid(x)


def exact_dot(x, picks):
    first = x.astype(BF16)
    rest = x - first.astype(F32)
    second = rest.astype(BF16)
    third = (rest - second.astype(F32)).astype(BF16)
    return (dot(first, picks) + dot(second, picks)) + dot(third, picks)


def put_out(*refs):
    sems = refs[-1]
    pieces = 4
    rows = refs[3].shape[0] // pieces
    copies = [
        pltpu.make_async_copy(refs[3].at[pl.ds(k * rows, rows)], refs[7].at[pl.ds(k * rows, rows)], sems.at[3 + k])
        for k in range(pieces)
    ]
    copies += [pltpu.make_async_copy(refs[k], refs[4 + k], sems.at[k]) for k in range(3)]
    for copy in copies:
        copy.start()
    for copy in copies:
        copy.wait()


def make_kernel(n_tp, seqs, feats, heads, chans, bc_dev):
    width = n_tp * feats
    tiles = width // LANES
    chips = n_tp // 2
    half = chips // 2
    steps_far = [half]
    for far in range(half - 1, 0, -1):
        steps_far += [far, chips - far]
    others = n_tp - 1

    def body(
        hid, slot, act, in_gain, z_w, x_w, bc_w, dt_w, cx_w, cx_b, cbc_w, cbc_b, cx_s, cbc_s,
        dt_bias, log_rate, skip_gain, state, norm_gain, out_w,
        out_layer, out_cx, out_cbc, out_state,
        zw, xw, bcw, dtw, cxs, cbcs, st, ow, gain, slot_v, slot_m, act_v, cxw, cxb, cbcw, cbcb, ngain,
        dtb_m, rate_m, skip_m,
        stb, xn, hid_recv, side, bcw_send, bcw_recv, bc_sums, bc_made, br_far, br_send, br_recv,
        in_sem, send_sem, recv_sem, relay_sem, side_sem,
    ):
        me = lax.axis_index("tp")
        chip, core = me // 2, lax.rem(me, 2)
        row = lax.axis_index("dp")
        odd = lax.rem(row, 2)
        barrier = pltpu.get_barrier_semaphore()

        def device(step, which):
            return {"tp": lax.rem(chip + step, chips) * 2 + which}

        loads = {}

        def load(name, src, dst):
            loads[name] = pltpu.make_async_copy(src, dst, in_sem.at[len(loads)])
            loads[name].start()

        load("hid", hid, hid_recv.at[core])

        @pl.when(core == 0)
        def _():
            pl.semaphore_signal(barrier, inc=1, device_id=device(0, 1), device_id_type=MESH)

        @pl.when(core == 1)
        def _():
            for step in steps_far:
                pl.semaphore_signal(barrier, inc=1, device_id=device(step, 1), device_id_type=MESH)

            @pl.when(odd == 0)
            def _():
                for t in range(n_tp):
                    pl.semaphore_signal(barrier, inc=1, device_id={"tp": t, "dp": row + 1}, device_id_type=MESH)

            @pl.when(odd == 1)
            def _():
                for step in steps_far:
                    pl.semaphore_signal(barrier, inc=1, device_id=device(step, 0), device_id_type=MESH)

        load("slot", slot, slot_v)
        load("slot_m", slot, slot_m)
        load("act", act, act_v)
        load("bc_w", bc_w, bcw)
        load("in_gain", in_gain, gain)
        load("cbc_s", cbc_s, cbcs)
        load("cbc_w", cbc_w, cbcw)
        load("cbc_b", cbc_b, cbcb)
        load("dt_w", dt_w, dtw)
        load("cx_s", cx_s, cxs)
        load("cx_w", cx_w, cxw)
        load("cx_b", cx_b, cxb)
        load("norm_gain", norm_gain, ngain)
        load("dt_bias", dt_bias, dtb_m)
        load("log_rate", log_rate, rate_m)
        load("skip_gain", skip_gain, skip_m)
        load("state", state, st)
        load("x_w", x_w, xw)
        load("z_w", z_w, zw)
        load("out_w", out_w, ow)

        def first_send(step, which, dst_slot, phase=0):
            arrival = 5 if step == half else phase
            return pltpu.make_async_remote_copy(
                src_ref=hid_recv.at[core], dst_ref=hid_recv.at[dst_slot],
                send_sem=send_sem.at[phase], recv_sem=recv_sem.at[arrival],
                device_id=device(step, which), device_id_type=MESH,
            )

        def relay(first=1, count=n_tp - 1):
            return pltpu.make_async_remote_copy(
                src_ref=hid_recv.at[pl.ds(first, count)], dst_ref=hid_recv.at[pl.ds(first, count)],
                send_sem=relay_sem.at[0], recv_sem=recv_sem.at[0],
                device_id=device(0, 0), device_id_type=MESH,
            )

        @pl.when(core == 0)
        def _():
            loads["hid"].wait()
            pl.semaphore_wait(barrier, 1 + odd * (2 * chips - 1))
            first_send(0, 1, 0, 4).start()
            for step in steps_far:
                first_send(step, 1, 2 * (chips - step)).start()

        for name in ("slot", "slot_m", "act", "in_gain", "cbc_s", "cbc_w", "cbc_b"):
            loads[name].wait()
        slot_row = slot_v[...]
        by_slot = iota((seqs, seqs), 0) == jnp.broadcast_to(slot_row, (seqs, seqs))
        to_slot = one_hot(by_slot)
        eye16 = eye(seqs)
        diagonal = iota((seqs, seqs), 0) == iota((seqs, seqs), 1)
        to_seq = dot_nt(eye16, to_slot).astype(BF16)
        act_f = jnp.broadcast_to(act_v[...].astype(F32), (seqs, seqs))
        live_row = act_v[...] > 0
        act_col = jnp.sum(jnp.where(diagonal, act_f, 0.0), axis=1, keepdims=True) > 0
        live_slot = jnp.sum(jnp.where(by_slot, act_f, 0.0), axis=1, keepdims=True) > 0
        bc_rows = jnp.concatenate([cbcw[...].astype(F32), cbcb[...].astype(F32)], axis=0)
        row_at, col_at = iota((bc_dev, bc_dev), 0), iota((bc_dev, bc_dev), 1)
        mirror = one_hot(col_at == row_at // SUBS * SUBS + lax.rem(SUBS - lax.rem(row_at, SUBS), SUBS))
        bc_cols = dot_nt(mirror, bc_rows.astype(BF16))
        bc_old = [dot(dot_nt(mirror, cbcs[k]).astype(BF16), to_slot) for k in range(3)]
        bc_base = (bc_old[0] * bc_cols[:, 0:1] + bc_old[1] * bc_cols[:, 1:2]) + bc_old[2] * bc_cols[:, 2:3]
        pad = jnp.zeros((bc_dev, LANES - seqs), F32)
        side[core, 0] = jnp.concatenate([bc_base + bc_cols[:, 4:5], pad], axis=1)
        side[core, 1] = jnp.broadcast_to(bc_cols[:, 3:4], (bc_dev, LANES))
        def lend():
            return pltpu.make_async_remote_copy(
                src_ref=side.at[0], dst_ref=side.at[0], send_sem=side_sem.at[0], recv_sem=side_sem.at[1],
                device_id=device(0, 1), device_id_type=MESH,
            )

        @pl.when(core == 0)
        def _():
            lend().start()

        loads["bc_w"].wait()
        turned = dot(mirror, bcw[...]).astype(BF16)
        bcw[...] = turned
        for k in range(tiles):
            bcw_send[k] = turned[:, k * LANES : (k + 1) * LANES]

        def share_tile(of_chip):
            return (of_chip * 2 * feats) // LANES

        def share(of_chip, to_row):
            return pltpu.make_async_remote_copy(
                src_ref=bcw_send.at[pl.ds(share_tile(of_chip), 3)], dst_ref=bcw_recv.at[me],
                send_sem=send_sem.at[3], recv_sem=recv_sem.at[3],
                device_id={"tp": 2 * of_chip + 1, "dp": to_row}, device_id_type=MESH,
            )

        for name in ("cx_s", "cx_w", "cx_b", "norm_gain", "dt_bias", "log_rate", "skip_gain"):
            loads[name].wait()
        eye_ch = eye(chans)
        g0 = ngain[...].reshape(1, chans)
        g1 = g0.astype(BF16).astype(F32)
        g2 = (g0 - g1).astype(BF16).astype(F32)
        g3 = (g0 - g1) - g2
        rows = jnp.concatenate([cxw[...].astype(F32), cxb[...].astype(F32).reshape(1, chans), g1, g2, g3], axis=0)
        cols = dot_nt(eye_ch, rows.astype(BF16))
        gain_col = (cols[:, 5:6] + cols[:, 6:7]) + cols[:, 7:8]
        x_old = [dot(dot_nt(eye_ch, cxs[k]).astype(BF16), to_slot) for k in range(3)]
        x_base = (x_old[0] * cols[:, 0:1] + x_old[1] * cols[:, 1:2]) + x_old[2] * cols[:, 2:3]
        loads["state"].wait()

        def narrow(i, carry):
            stb[i] = st[slot_m[0, i]].astype(BF16)
            return carry

        lax.fori_loop(0, seqs, narrow, 0)
        loads["dt_w"].wait()

        @pl.when(core == 1)
        def _():
            loads["hid"].wait()
            pl.semaphore_wait(barrier, chips + odd * chips)
            pl.semaphore_signal(barrier, inc=1, device_id=device(0, 0), device_id_type=MESH)
            for step in steps_far:
                first_send(step, 1, 2 * (chips - step) + 1).start()

        @pl.when(odd == 1)
        def _():
            for step in steps_far:
                for to_row in (row - 1, row):
                    share(lax.rem(chip + step, chips), to_row).start()
            share(chip, row - 1).start()

            @pl.when(core == 0)
            def _():
                share(chip, row).start()

            @pl.when(core == 1)
            def _():
                bcw_recv[me] = bcw_send[pl.ds(share_tile(chip), 3)]


        def all_of(phase, dst_ref, count):
            return pltpu.make_async_remote_copy(
                src_ref=dst_ref.at[pl.ds(0, count)], dst_ref=dst_ref.at[pl.ds(0, count)],
                send_sem=send_sem.at[phase], recv_sem=recv_sem.at[phase],
                device_id=device(0, 1 - core), device_id_type=MESH,
            )

        lines = n_tp * bc_dev // SUBS
        own_lines = 2 * bc_dev // SUBS

        def packed(x):
            count = x.shape[0]
            spread = jnp.concatenate([x, jnp.zeros((count, LANES - seqs), F32)], axis=1)
            spread = pltpu.roll(spread.reshape(count // SUBS, SUBS, LANES), 0, 2, stride=seqs, stride_axis=1)
            return jnp.sum(spread, axis=1)

        def relay_made():
            return pltpu.make_async_remote_copy(
                src_ref=bc_made, dst_ref=bc_made, send_sem=relay_sem.at[1], recv_sem=recv_sem.at[1],
                device_id=device(0, 0), device_id_type=MESH,
            )

        @pl.when(core == 1)
        def _():
            @pl.when(odd == 0)
            def _():
                all_of(3, bcw_recv, n_tp).wait_recv()

            @pl.when(odd == 1)
            def _():
                all_of(3, bcw_recv, n_tp - 1).wait_recv()

            first = share_tile(chip)
            first_send(0, 1, 0, 4).wait_recv()
            pair = jnp.concatenate([hid_recv[0].astype(F32), hid_recv[1].astype(F32), jnp.zeros((seqs, 3 * LANES - 2 * feats), F32)], axis=1)
            pair = pltpu.roll(pair, lax.rem(chip * 2 * feats, LANES), 1)
            terms = 0.0
            for k in range(3):
                scaled_k = (pair[:, k * LANES : (k + 1) * LANES] * gain[pl.ds(first + k, 1), :]).astype(BF16)
                weights = jnp.concatenate([bcw_recv[t, k] for t in range(n_tp)], axis=0)
                terms = terms + dot_nt(weights, scaled_k)
            bc_sums[chip, 0:lines, :] = packed(terms)
            lend().wait_recv()
            for j in range(2):
                own = packed(jnp.concatenate([side[0, j], side[1, j]], axis=0)[:, :seqs])
                bc_sums[chip, lines + j * own_lines : lines + (j + 1) * own_lines, :] = own
            for step in steps_far:
                pltpu.make_async_remote_copy(
                    src_ref=bc_sums.at[chip], dst_ref=bc_sums.at[chip], send_sem=send_sem.at[1], recv_sem=recv_sem.at[1],
                    device_id=device(step, 1), device_id_type=MESH,
                ).start()

        @pl.when(core == 0)
        def _():
            all_of(0, hid_recv, n_tp - 1).wait_recv()

        @pl.when(core == 1)
        def _():
            all_of(0, hid_recv, n_tp - 4).wait_recv()
            relay(1, 2 * half - 1).start()
            relay(2 * half + 2, n_tp - 2 * half - 2).start()
            pltpu.make_async_remote_copy(
                src_ref=hid_recv.at[pl.ds(2 * half, 2)], dst_ref=hid_recv.at[pl.ds(2 * half, 2)],
                send_sem=send_sem.at[0], recv_sem=recv_sem.at[5],
                device_id=device(half, 1), device_id_type=MESH,
            ).wait_recv()
            relay(2 * half, 2).start()

        blocks = [
            hid_recv[2 * lax.rem(t // 2 - chip + chips, chips) + t % 2].astype(F32) for t in range(n_tp)
        ]
        whole = jnp.concatenate(blocks, axis=1)
        for k in range(tiles):
            at = slice(k * LANES, (k + 1) * LANES)
            xn[:, at] = (whole[:, at] * gain[k : k + 1, :]).astype(BF16)
        squares = whole[:, :LANES] * whole[:, :LANES]
        for k in range(1, tiles):
            part = whole[:, k * LANES : (k + 1) * LANES]
            squares = squares + part * part
        inv_col = lax.rsqrt(jnp.sum(squares, axis=1, keepdims=True) / width + EPS)
        inv = jnp.sum(jnp.where(diagonal, jnp.broadcast_to(inv_col, (seqs, seqs)), 0.0), axis=0, keepdims=True)

        of_seq = lax.rem(iota((seqs, LANES), 1), seqs) == iota((seqs, LANES), 0)
        inv_lanes = jnp.sum(jnp.where(of_seq, jnp.broadcast_to(inv_col, (seqs, LANES)), 0.0), axis=0, keepdims=True)

        dt_proj = (dot_nt(dtw[...], xn[...]) * inv).astype(BF16).astype(F32)
        loads["x_w"].wait()
        loads["z_w"].wait()
        x_proj = (dot_nt(xw[...], xn[...]) * inv).astype(BF16)
        z_proj = (dot_nt(zw[...], xn[...]) * inv).astype(BF16)
        @pl.when(core == 1)
        def _():
            all_of(1, bc_sums, chips - 1).wait_recv()
            sums = bc_sums[0, 0:lines, :]
            for c in range(1, chips):
                sums = sums + bc_sums[c, 0:lines, :]
            base, tap = [
                jnp.concatenate([bc_sums[c, at : at + own_lines, :] for c in range(chips)], axis=0)
                for at in (lines, lines + own_lines)
            ]
            made = silu(base + (sums * inv_lanes).astype(BF16).astype(F32) * tap)
            bc_made[...] = made.astype(BF16).astype(F32)
            relay_made().start()

        @pl.when(core == 0)
        def _():
            relay_made().wait_recv()

        bc_conv = bc_made[...]

        def unpacked(at):
            found = []
            for eight in range(NS // SUBS):
                line = bc_conv[at // SUBS + eight : at // SUBS + eight + 1, :]
                found.append(pltpu.roll(jnp.broadcast_to(line, (SUBS, LANES)), 0, 1, stride=seqs, stride_axis=0))
            return jnp.concatenate(found, axis=0)[:, :seqs]

        c_f, b_f = unpacked(NS), unpacked(0)
        lane = iota((NS, seqs), 1)
        c_big = jnp.concatenate([jnp.where(lane == b, c_f, 0.0).astype(BF16) for b in range(seqs)], axis=0)
        s_c = []
        for at in (0, chans // 2):
            s_big = jnp.concatenate([stb[b, at : at + chans // 2, :] for b in range(seqs)], axis=1)
            s_c.append(dot(s_big, c_big))
        s_c = jnp.concatenate(s_c, axis=0)
        x_conv = silu(x_base + x_proj.astype(F32) * cols[:, 3:4] + cols[:, 4:5]).astype(BF16)
        x_f = x_conv.astype(F32)
        z_gate = silu(z_proj.astype(F32))
        steps, decays = [], []
        for h in range(heads):
            raw = dt_proj[h : h + 1, :] + dtb_m[h]
            step = jnp.maximum(raw, 0.0) + jnp.log1p(jnp.exp(-jnp.abs(raw)))
            rate = jnp.exp(jnp.full((1, seqs), rate_m[h], F32))
            steps.append(jnp.where(live_row, step, 0.0))
            decays.append(jnp.where(live_row, jnp.exp(-step * rate), 1.0))

        def per_channel(values):
            return jnp.concatenate([jnp.broadcast_to(v, (HP, seqs)) for v in values], axis=0)

        dtx = per_channel(steps) * x_f
        decay = per_channel(decays)
        skipped = jnp.concatenate([jnp.full((HP, seqs), skip_m[h], F32) for h in range(heads)], axis=0) * x_f
        bc_dot = jnp.sum(b_f * c_f, axis=0, keepdims=True)
        y = (decay * s_c + dtx * bc_dot) + skipped
        gated = y * z_gate
        scaled = (gated * gain_col).astype(BF16)
        sq_row = jnp.broadcast_to(jnp.sum(gated * gated, axis=0, keepdims=True), (seqs, seqs))
        sq_col = jnp.sum(jnp.where(diagonal, sq_row, 0.0), axis=1, keepdims=True)
        sq_1 = sq_col.astype(BF16).astype(F32)
        sq_2 = (sq_col - sq_1).astype(BF16).astype(F32)
        sq_cols = [half_rows for term in (sq_1, sq_2, (sq_col - sq_1) - sq_2) for half_rows in (term[:SUBS], term[SUBS:])]
        loads["out_w"].wait()
        rows_seq = dot_nt(eye16, scaled).astype(BF16)
        lane_at = iota((SUBS, LANES), 1)
        spare = feats - LANES
        tails = {}
        for start in sorted({(t * feats) % LANES for t in range(n_tp)}):
            tail = jnp.zeros((SUBS, LANES), F32)
            for j, term in enumerate(sq_cols):
                tail = jnp.where(lane_at == (start + 2 * spare + j) % LANES, term, tail)
            tails[start] = tail

        def within(at):
            at = lax.rem(at, LANES)
            return (lane_at >= at) & (lane_at < at + spare)

        def folded(tile_0, tile_1, start, tail):
            main = jnp.where(iota((seqs, LANES), 1) >= start, tile_0, tile_1)
            rest = jnp.where(within(start + spare), pltpu.roll(tile_1[SUBS:], spare, 1), tail)
            rest = jnp.where(within(start), tile_1[:SUBS], rest)
            return jnp.concatenate([main, rest], axis=0).astype(BF16)

        def window_send(src, peer):
            pltpu.make_async_remote_copy(
                src_ref=src, dst_ref=br_recv.at[me], send_sem=send_sem.at[2], recv_sem=recv_sem.at[2],
                device_id={"tp": peer}, device_id_type=MESH,
            ).start()

        opposite = lax.rem(chip + half, chips)
        far_tile = share_tile(opposite)
        far_start = lax.rem(opposite * 2 * feats, LANES)
        far_branch = [
            dot(rows_seq, ow[:, pl.ds(pl.multiple_of((far_tile + k) * LANES, LANES), LANES)]) for k in range(3)
        ]
        for j in range(2):
            begin = far_start + (j * feats) % LANES
            tail = jnp.zeros((SUBS, LANES), F32)
            for at, found in tails.items():
                tail = jnp.where(begin == at, found, tail)
            br_far[j] = folded(far_branch[j], far_branch[j + 1], begin, tail)
        for j in (0, 1):
            window_send(br_far.at[j], 2 * opposite + j)

        side_of = chip // half
        half_width = half * 2 * feats
        for part in range(2):
            which = 1 - side_of if part == 0 else side_of
            step = 2 * LANES
            branch = jnp.concatenate(
                [
                    dot(rows_seq, ow[:, pl.ds(pl.multiple_of(which * half_width + at, LANES), step)])
                    for at in range(0, half_width, step)
                ],
                axis=1,
            )
            for i in range(2 * half):
                first, start = (i * feats) // LANES, (i * feats) % LANES
                tile_0 = branch[:, first * LANES : (first + 1) * LANES]
                tile_1 = branch[:, (first + 1) * LANES : (first + 2) * LANES]
                br_send[which * 2 * half + i] = folded(tile_0, tile_1, start, tails[start])
            for i in range(1 - part, half):
                far = which * half + lax.rem(chip + i, half)
                for flip in (1, 0):
                    if part == 1 and i == 0 and not flip:
                        continue
                    peer = far * 2 + (1 - core if flip else core)
                    window_send(br_send.at[peer], peer)
        br_recv[me] = br_send[me]

        x_now = dot_nt(to_slot, x_proj)
        bc_proj = (dot_nt(bcw[...], xn[...]) * inv).astype(BF16)
        bc_now = dot(dot_nt(to_slot, bc_proj).astype(BF16), mirror)
        for out, old, now in ((out_cx, cxs, x_now), (out_cbc, cbcs, bc_now)):
            held = [old[k].astype(F32) for k in range(3)]
            for k, new in enumerate((held[1], held[2], now)):
                out[k] = jnp.where(live_slot, new, held[k]).astype(BF16)
        of_heads = jnp.concatenate(steps + decays + [jnp.zeros((-2 * heads % SUBS, seqs), F32)], axis=0)
        of_heads = exact_dot(of_heads, to_seq)
        steps_slot = [of_heads[h : h + 1, :] for h in range(heads)]
        decays_slot = [of_heads[heads + h : heads + h + 1, :] for h in range(heads)]
        dtx_slot = per_channel(steps_slot) * dot(x_conv, to_seq)
        decay_slot = per_channel(decays_slot)
        b_rows = dot_nt(to_slot, b_f.astype(BF16))
        for b in range(seqs):
            grown = dtx_slot[:, b : b + 1] * b_rows[b : b + 1, :]
            out_state[b] = decay_slot[:, b : b + 1] * st[b] + grown

        all_of(2, br_recv, others).wait_recv()
        total = br_recv[0].astype(F32)
        for t in range(1, n_tp):
            total = total + br_recv[t].astype(F32)
        shift = lax.rem(me * feats, LANES)
        total = pltpu.roll(total, lax.rem(LANES - shift, LANES), 1)
        rest = total[seqs:]
        rest = jnp.concatenate([rest, pltpu.roll(rest, LANES - spare, 1)], axis=0)
        branch_sum = jnp.concatenate([total[:seqs], rest[:, :spare]], axis=1)
        sq_at = 2 * spare
        sq_rows = [
            (total[seqs:, at : at + 1] + total[seqs:, at + 2 : at + 3]) + total[seqs:, at + 4 : at + 5]
            for at in (sq_at, sq_at + 1)
        ]
        inv_out = lax.rsqrt(jnp.concatenate(sq_rows, axis=0) / INNER + EPS)
        kept = hid_recv[core].astype(F32)
        fresh = (kept + inv_out * branch_sum).astype(BF16).astype(F32)
        out_layer[...] = jnp.where(act_col, fresh, kept).astype(BF16)

        all_of(2, br_recv, others).wait_send()

        def hid_sent(count):
            return pltpu.make_async_remote_copy(
                src_ref=hid_recv.at[pl.ds(0, count)], dst_ref=hid_recv.at[pl.ds(0, count)],
                send_sem=send_sem.at[0], recv_sem=recv_sem.at[0],
                device_id=device(0, 1 - core), device_id_type=MESH,
            )

        @pl.when((odd == 1) & (core == 0))
        def _():
            all_of(3, bcw_recv, n_tp).wait_send()

        @pl.when((odd == 1) & (core == 1))
        def _():
            all_of(3, bcw_recv, n_tp - 1).wait_send()

        @pl.when(core == 0)
        def _():
            hid_sent(chips - 1).wait_send()
            first_send(0, 1, 0, 4).wait_send()
            lend().wait_send()

        @pl.when(core == 1)
        def _():
            hid_sent(chips - 1).wait_send()
            relay().wait_send()
            relay_made().wait_send()
            all_of(1, bc_sums, chips - 1).wait_send()

    return body


def shards(
    hidden, in_gain, z_weight, x_weight, bc_weight, dt_weight, conv_x_weight, conv_x_bias,
    conv_bc_weight, conv_bc_bias, conv_x_state, conv_bc_state, dt_bias, log_rate, skip_gain,
    ssm_state, norm_gain, out_weight, pool_slot, active,
):
    n_tp = lax.axis_size("tp")
    seqs, feats = hidden.shape
    heads = ssm_state.shape[1]
    chans = z_weight.shape[1]
    bc_dev = bc_weight.shape[1]
    width = in_gain.shape[0]
    tiles = width // LANES
    vmem = pl.BlockSpec(memory_space=pltpu.VMEM)
    hbm = pl.BlockSpec(memory_space=pl.ANY)
    shape = jax.ShapeDtypeStruct
    results = (
        ((seqs, feats), BF16),
        ((3, seqs, chans), BF16),
        ((3, seqs, bc_dev), BF16),
        ((seqs, chans, NS), F32),
    )
    made = pl.pallas_call(
        make_kernel(n_tp, seqs, feats, heads, chans, bc_dev),
        out_shape=tuple(pltpu.VMEM(dims, kind) for dims, kind in results),
        in_specs=[hbm] * 20,
        out_specs=(vmem,) * 4,
        scratch_shapes=[
            pltpu.VMEM((chans, width), BF16),
            pltpu.VMEM((chans, width), BF16),
            pltpu.VMEM((bc_dev, width), BF16),
            pltpu.VMEM((heads, width), BF16),
            pltpu.VMEM((3, seqs, chans), BF16),
            pltpu.VMEM((3, seqs, bc_dev), BF16),
            pltpu.VMEM((seqs, chans, NS), F32),
            pltpu.VMEM((chans, width), BF16),
            pltpu.VMEM((tiles, LANES), F32),
            pltpu.VMEM((1, seqs), jnp.int32),
            pltpu.SMEM((1, seqs), jnp.int32),
            pltpu.VMEM((1, seqs), jnp.int32),
            pltpu.VMEM((4, chans), BF16),
            pltpu.VMEM((chans,), BF16),
            pltpu.VMEM((4, bc_dev), BF16),
            pltpu.VMEM((1, bc_dev), BF16),
            pltpu.VMEM((chans,), F32),
            pltpu.SMEM((heads,), F32),
            pltpu.SMEM((heads,), F32),
            pltpu.SMEM((heads,), F32),
            pltpu.VMEM((seqs, chans, NS), BF16),
            pltpu.VMEM((seqs, width), BF16),
            pltpu.VMEM((n_tp, seqs, feats), BF16),
            pltpu.VMEM((2, 2, bc_dev, LANES), F32),
            pltpu.VMEM((tiles, bc_dev, LANES), BF16),
            pltpu.VMEM((n_tp, 3, bc_dev, LANES), BF16),
            pltpu.VMEM((n_tp // 2, (n_tp + 4) * bc_dev // SUBS, LANES), F32),
            pltpu.VMEM((n_tp * bc_dev // SUBS, LANES), F32),
            pltpu.VMEM((2, seqs + SUBS, LANES), BF16),
            pltpu.VMEM((n_tp, seqs + SUBS, LANES), BF16),
            pltpu.VMEM((n_tp, seqs + SUBS, LANES), BF16),
            pltpu.SemaphoreType.DMA((20 + 1,)),
            pltpu.SemaphoreType.DMA((5,)),
            pltpu.SemaphoreType.DMA((6,)),
            pltpu.SemaphoreType.DMA((2,)),
            pltpu.SemaphoreType.DMA((2,)),
        ],
        compiler_params=pltpu.CompilerParams(
            collective_id=0, has_side_effects=True, vmem_limit_bytes=60 * 1024 * 1024
        ),
        name="step",
    )(
        hidden, pool_slot, active.reshape(1, seqs), in_gain.reshape(tiles, LANES),
        z_weight.T, x_weight.T, bc_weight.T, dt_weight.T,
        conv_x_weight, conv_x_bias, conv_bc_weight, conv_bc_bias.reshape(1, bc_dev),
        conv_x_state.transpose(1, 0, 2), conv_bc_state.transpose(1, 0, 2),
        dt_bias, log_rate, skip_gain, ssm_state.reshape(seqs, chans, NS),
        norm_gain, out_weight,
    )
    out_layer, out_cx, out_cbc, out_state = pl.pallas_call(
        put_out,
        out_shape=tuple(shape(dims, kind) for dims, kind in results),
        in_specs=[vmem] * 4,
        out_specs=(hbm,) * 4,
        scratch_shapes=[pltpu.SemaphoreType.DMA((7,))],
        name="put",
    )(*(pltpu.with_memory_space_constraint(x, pltpu.VMEM) for x in made))
    return (
        out_layer,
        out_cx.transpose(1, 0, 2),
        out_cbc.transpose(1, 0, 2),
        out_state.reshape(ssm_state.shape),
    )


def solution(mesh):
    rows = ("groups", "dp")
    placed = (
        P(rows, "tp"), P(), P(None, "tp"), P(None, "tp"), P(None, "tp"), P(None, "tp"), P(None, "tp"),
        P("tp"), P(None, "tp"), P("tp"), P(rows, None, "tp"), P(rows, None, "tp"), P("tp"), P("tp"),
        P("tp"), P(rows, "tp", None, None), P("tp"), P("tp", None), P(rows, None), P(rows),
    )
    return jax.shard_map(
        shards,
        mesh=mesh,
        in_specs=placed,
        out_specs=(P(rows, "tp"), P(rows, None, "tp"), P(rows, None, "tp"), P(rows, "tp", None, None)),
        check_vma=False,
    )
```

```python
import jax
import jax.numpy as jnp
from jax import lax
from jax.experimental import pallas as pl
from jax.experimental.pallas import tpu as pltpu
from jax.sharding import PartitionSpec as P

HP = 64
NS = 128
INNER = 5120
EPS = 1e-05
F32 = jnp.float32
BF16 = jnp.bfloat16
LANES = 128
SUBS = 8

NT = (((1,), (1,)), ((), ()))
MESH = pl.DeviceIdType.MESH


def dot(a, b):
    return jnp.dot(a, b, preferred_element_type=F32)


def dot_nt(a, b):
    return lax.dot_general(a, b, NT, preferred_element_type=F32)


def iota(shape, dim):
    return lax.broadcasted_iota(jnp.int32, shape, dim)


def one_hot(mask):
    return mask.astype(F32).astype(BF16)


def eye(n):
    return one_hot(iota((n, n), 0) == iota((n, n), 1))


def silu(x):
    return x * jax.nn.sigmoid(x)


def exact_dot(x, picks):
    first = x.astype(BF16)
    rest = x - first.astype(F32)
    second = rest.astype(BF16)
    third = (rest - second.astype(F32)).astype(BF16)
    return (dot(first, picks) + dot(second, picks)) + dot(third, picks)


def put_out(*refs):
    sems = refs[-1]
    pieces = 4
    rows = refs[3].shape[0] // pieces
    copies = [
        pltpu.make_async_copy(refs[3].at[pl.ds(k * rows, rows)], refs[7].at[pl.ds(k * rows, rows)], sems.at[3 + k])
        for k in range(pieces)
    ]
    copies += [pltpu.make_async_copy(refs[k], refs[4 + k], sems.at[k]) for k in range(3)]
    for copy in copies:
        copy.start()
    for copy in copies:
        copy.wait()


def make_kernel(n_tp, seqs, feats, heads, chans, bc_dev):
    width = n_tp * feats
    tiles = width // LANES
    chips = n_tp // 2
    half = chips // 2
    steps_far = [half]
    for far in range(half - 1, 0, -1):
        steps_far += [far, chips - far]
    others = n_tp - 1

    def body(
        hid, slot, act, in_gain, z_w, x_w, bc_w, dt_w, cx_w, cx_b, cbc_w, cbc_b, cx_s, cbc_s,
        dt_bias, log_rate, skip_gain, state, norm_gain, out_w,
        out_layer, out_cx, out_cbc, out_state,
        zw, xw, bcw, dtw, cxs, cbcs, st, ow, gain, slot_v, slot_m, act_v, cxw, cxb, cbcw, cbcb, ngain,
        dtb_m, rate_m, skip_m,
        stb, xn, hid_recv, side, bcw_send, bcw_recv, bc_sums, bc_made, br_send, br_recv,
        in_sem, send_sem, recv_sem, relay_sem, side_sem,
    ):
        me = lax.axis_index("tp")
        chip, core = me // 2, lax.rem(me, 2)
        row = lax.axis_index("dp")
        odd = lax.rem(row, 2)
        barrier = pltpu.get_barrier_semaphore()

        def device(step, which):
            return {"tp": lax.rem(chip + step, chips) * 2 + which}

        loads = {}

        def load(name, src, dst):
            loads[name] = pltpu.make_async_copy(src, dst, in_sem.at[len(loads)])
            loads[name].start()

        load("hid", hid, hid_recv.at[core])

        @pl.when(core == 0)
        def _():
            pl.semaphore_signal(barrier, inc=1, device_id=device(0, 1), device_id_type=MESH)

        @pl.when(core == 1)
        def _():
            for step in steps_far:
                pl.semaphore_signal(barrier, inc=1, device_id=device(step, 1), device_id_type=MESH)

            @pl.when(odd == 0)
            def _():
                for t in range(n_tp):
                    pl.semaphore_signal(barrier, inc=1, device_id={"tp": t, "dp": row + 1}, device_id_type=MESH)

            @pl.when(odd == 1)
            def _():
                for step in steps_far:
                    pl.semaphore_signal(barrier, inc=1, device_id=device(step, 0), device_id_type=MESH)

        load("slot", slot, slot_v)
        load("slot_m", slot, slot_m)
        load("act", act, act_v)
        load("bc_w", bc_w, bcw)
        load("in_gain", in_gain, gain)
        load("cbc_s", cbc_s, cbcs)
        load("cbc_w", cbc_w, cbcw)
        load("cbc_b", cbc_b, cbcb)
        load("dt_w", dt_w, dtw)
        load("cx_s", cx_s, cxs)
        load("cx_w", cx_w, cxw)
        load("cx_b", cx_b, cxb)
        load("norm_gain", norm_gain, ngain)
        load("dt_bias", dt_bias, dtb_m)
        load("log_rate", log_rate, rate_m)
        load("skip_gain", skip_gain, skip_m)
        load("state", state, st)
        load("x_w", x_w, xw)
        load("z_w", z_w, zw)
        load("out_w", out_w, ow)

        def first_send(step, which, dst_slot, phase=0):
            arrival = 5 if step == half else phase
            return pltpu.make_async_remote_copy(
                src_ref=hid_recv.at[core], dst_ref=hid_recv.at[dst_slot],
                send_sem=send_sem.at[phase], recv_sem=recv_sem.at[arrival],
                device_id=device(step, which), device_id_type=MESH,
            )

        def relay(first=1, count=n_tp - 1):
            return pltpu.make_async_remote_copy(
                src_ref=hid_recv.at[pl.ds(first, count)], dst_ref=hid_recv.at[pl.ds(first, count)],
                send_sem=relay_sem.at[0], recv_sem=recv_sem.at[0],
                device_id=device(0, 0), device_id_type=MESH,
            )

        @pl.when(core == 0)
        def _():
            loads["hid"].wait()
            pl.semaphore_wait(barrier, 1 + odd * (2 * chips - 1))
            first_send(0, 1, 0, 4).start()
            for step in steps_far:
                first_send(step, 1, 2 * (chips - step)).start()

        for name in ("slot", "slot_m", "act", "in_gain", "cbc_s", "cbc_w", "cbc_b"):
            loads[name].wait()
        slot_row = slot_v[...]
        by_slot = iota((seqs, seqs), 0) == jnp.broadcast_to(slot_row, (seqs, seqs))
        to_slot = one_hot(by_slot)
        eye16 = eye(seqs)
        diagonal = iota((seqs, seqs), 0) == iota((seqs, seqs), 1)
        to_seq = dot_nt(eye16, to_slot).astype(BF16)
        act_f = jnp.broadcast_to(act_v[...].astype(F32), (seqs, seqs))
        live_row = act_v[...] > 0
        act_col = jnp.sum(jnp.where(diagonal, act_f, 0.0), axis=1, keepdims=True) > 0
        live_slot = jnp.sum(jnp.where(by_slot, act_f, 0.0), axis=1, keepdims=True) > 0
        bc_rows = jnp.concatenate([cbcw[...].astype(F32), cbcb[...].astype(F32)], axis=0)
        row_at, col_at = iota((bc_dev, bc_dev), 0), iota((bc_dev, bc_dev), 1)
        mirror = one_hot(col_at == row_at // SUBS * SUBS + lax.rem(SUBS - lax.rem(row_at, SUBS), SUBS))
        bc_cols = dot_nt(mirror, bc_rows.astype(BF16))
        bc_old = [dot(dot_nt(mirror, cbcs[k]).astype(BF16), to_slot) for k in range(3)]
        bc_base = (bc_old[0] * bc_cols[:, 0:1] + bc_old[1] * bc_cols[:, 1:2]) + bc_old[2] * bc_cols[:, 2:3]
        pad = jnp.zeros((bc_dev, LANES - seqs), F32)
        side[core, 0] = jnp.concatenate([bc_base + bc_cols[:, 4:5], pad], axis=1)
        side[core, 1] = jnp.broadcast_to(bc_cols[:, 3:4], (bc_dev, LANES))
        def lend():
            return pltpu.make_async_remote_copy(
                src_ref=side.at[0], dst_ref=side.at[0], send_sem=side_sem.at[0], recv_sem=side_sem.at[1],
                device_id=device(0, 1), device_id_type=MESH,
            )

        @pl.when(core == 0)
        def _():
            lend().start()

        loads["bc_w"].wait()
        turned = dot(mirror, bcw[...]).astype(BF16)
        bcw[...] = turned
        for k in range(tiles):
            bcw_send[k] = turned[:, k * LANES : (k + 1) * LANES]

        def share_tile(of_chip):
            return (of_chip * 2 * feats) // LANES

        def share(of_chip, to_row):
            return pltpu.make_async_remote_copy(
                src_ref=bcw_send.at[pl.ds(share_tile(of_chip), 3)], dst_ref=bcw_recv.at[me],
                send_sem=send_sem.at[3], recv_sem=recv_sem.at[3],
                device_id={"tp": 2 * of_chip + 1, "dp": to_row}, device_id_type=MESH,
            )

        for name in ("cx_s", "cx_w", "cx_b", "norm_gain", "dt_bias", "log_rate", "skip_gain"):
            loads[name].wait()
        eye_ch = eye(chans)
        g0 = ngain[...].reshape(1, chans)
        g1 = g0.astype(BF16).astype(F32)
        g2 = (g0 - g1).astype(BF16).astype(F32)
        g3 = (g0 - g1) - g2
        rows = jnp.concatenate([cxw[...].astype(F32), cxb[...].astype(F32).reshape(1, chans), g1, g2, g3], axis=0)
        cols = dot_nt(eye_ch, rows.astype(BF16))
        gain_col = (cols[:, 5:6] + cols[:, 6:7]) + cols[:, 7:8]
        x_old = [dot(dot_nt(eye_ch, cxs[k]).astype(BF16), to_slot) for k in range(3)]
        x_base = (x_old[0] * cols[:, 0:1] + x_old[1] * cols[:, 1:2]) + x_old[2] * cols[:, 2:3]
        loads["state"].wait()

        def narrow(i, carry):
            stb[i] = st[slot_m[0, i]].astype(BF16)
            return carry

        lax.fori_loop(0, seqs, narrow, 0)
        loads["dt_w"].wait()

        @pl.when(core == 1)
        def _():
            loads["hid"].wait()
            pl.semaphore_wait(barrier, chips + odd * chips)
            pl.semaphore_signal(barrier, inc=1, device_id=device(0, 0), device_id_type=MESH)
            for step in steps_far:
                first_send(step, 1, 2 * (chips - step) + 1).start()

        @pl.when(odd == 1)
        def _():
            for step in steps_far:
                for to_row in (row - 1, row):
                    share(lax.rem(chip + step, chips), to_row).start()
            share(chip, row - 1).start()

            @pl.when(core == 0)
            def _():
                share(chip, row).start()

            @pl.when(core == 1)
            def _():
                bcw_recv[me] = bcw_send[pl.ds(share_tile(chip), 3)]


        def all_of(phase, dst_ref, count):
            return pltpu.make_async_remote_copy(
                src_ref=dst_ref.at[pl.ds(0, count)], dst_ref=dst_ref.at[pl.ds(0, count)],
                send_sem=send_sem.at[phase], recv_sem=recv_sem.at[phase],
                device_id=device(0, 1 - core), device_id_type=MESH,
            )

        lines = n_tp * bc_dev // SUBS
        own_lines = 2 * bc_dev // SUBS

        def packed(x):
            count = x.shape[0]
            spread = jnp.concatenate([x, jnp.zeros((count, LANES - seqs), F32)], axis=1)
            spread = pltpu.roll(spread.reshape(count // SUBS, SUBS, LANES), 0, 2, stride=seqs, stride_axis=1)
            return jnp.sum(spread, axis=1)

        def relay_made():
            return pltpu.make_async_remote_copy(
                src_ref=bc_made, dst_ref=bc_made, send_sem=relay_sem.at[1], recv_sem=recv_sem.at[1],
                device_id=device(0, 0), device_id_type=MESH,
            )

        @pl.when(core == 1)
        def _():
            @pl.when(odd == 0)
            def _():
                all_of(3, bcw_recv, n_tp).wait_recv()

            @pl.when(odd == 1)
            def _():
                all_of(3, bcw_recv, n_tp - 1).wait_recv()

            first = share_tile(chip)
            first_send(0, 1, 0, 4).wait_recv()
            pair = jnp.concatenate([hid_recv[0].astype(F32), hid_recv[1].astype(F32), jnp.zeros((seqs, 3 * LANES - 2 * feats), F32)], axis=1)
            pair = pltpu.roll(pair, lax.rem(chip * 2 * feats, LANES), 1)
            terms = 0.0
            for k in range(3):
                scaled_k = (pair[:, k * LANES : (k + 1) * LANES] * gain[pl.ds(first + k, 1), :]).astype(BF16)
                weights = jnp.concatenate([bcw_recv[t, k] for t in range(n_tp)], axis=0)
                terms = terms + dot_nt(weights, scaled_k)
            bc_sums[chip, 0:lines, :] = packed(terms)
            lend().wait_recv()
            for j in range(2):
                own = packed(jnp.concatenate([side[0, j], side[1, j]], axis=0)[:, :seqs])
                bc_sums[chip, lines + j * own_lines : lines + (j + 1) * own_lines, :] = own
            for step in steps_far:
                pltpu.make_async_remote_copy(
                    src_ref=bc_sums.at[chip], dst_ref=bc_sums.at[chip], send_sem=send_sem.at[1], recv_sem=recv_sem.at[1],
                    device_id=device(step, 1), device_id_type=MESH,
                ).start()

        @pl.when(core == 0)
        def _():
            all_of(0, hid_recv, n_tp - 1).wait_recv()

        @pl.when(core == 1)
        def _():
            all_of(0, hid_recv, n_tp - 4).wait_recv()
            relay(1, 2 * half - 1).start()
            relay(2 * half + 2, n_tp - 2 * half - 2).start()
            pltpu.make_async_remote_copy(
                src_ref=hid_recv.at[pl.ds(2 * half, 2)], dst_ref=hid_recv.at[pl.ds(2 * half, 2)],
                send_sem=send_sem.at[0], recv_sem=recv_sem.at[5],
                device_id=device(half, 1), device_id_type=MESH,
            ).wait_recv()
            relay(2 * half, 2).start()

        blocks = [
            hid_recv[2 * lax.rem(t // 2 - chip + chips, chips) + t % 2].astype(F32) for t in range(n_tp)
        ]
        whole = jnp.concatenate(blocks, axis=1)
        for k in range(tiles):
            at = slice(k * LANES, (k + 1) * LANES)
            xn[:, at] = (whole[:, at] * gain[k : k + 1, :]).astype(BF16)
        squares = whole[:, :LANES] * whole[:, :LANES]
        for k in range(1, tiles):
            part = whole[:, k * LANES : (k + 1) * LANES]
            squares = squares + part * part
        inv_col = lax.rsqrt(jnp.sum(squares, axis=1, keepdims=True) / width + EPS)
        inv = jnp.sum(jnp.where(diagonal, jnp.broadcast_to(inv_col, (seqs, seqs)), 0.0), axis=0, keepdims=True)

        of_seq = lax.rem(iota((seqs, LANES), 1), seqs) == iota((seqs, LANES), 0)
        inv_lanes = jnp.sum(jnp.where(of_seq, jnp.broadcast_to(inv_col, (seqs, LANES)), 0.0), axis=0, keepdims=True)

        dt_proj = (dot_nt(dtw[...], xn[...]) * inv).astype(BF16).astype(F32)
        loads["x_w"].wait()
        loads["z_w"].wait()
        x_proj = (dot_nt(xw[...], xn[...]) * inv).astype(BF16)
        z_proj = (dot_nt(zw[...], xn[...]) * inv).astype(BF16)
        @pl.when(core == 1)
        def _():
            all_of(1, bc_sums, chips - 1).wait_recv()
            sums = bc_sums[0, 0:lines, :]
            for c in range(1, chips):
                sums = sums + bc_sums[c, 0:lines, :]
            base, tap = [
                jnp.concatenate([bc_sums[c, at : at + own_lines, :] for c in range(chips)], axis=0)
                for at in (lines, lines + own_lines)
            ]
            made = silu(base + (sums * inv_lanes).astype(BF16).astype(F32) * tap)
            bc_made[...] = made.astype(BF16).astype(F32)
            relay_made().start()

        @pl.when(core == 0)
        def _():
            relay_made().wait_recv()

        bc_conv = bc_made[...]

        def unpacked(at):
            found = []
            for eight in range(NS // SUBS):
                line = bc_conv[at // SUBS + eight : at // SUBS + eight + 1, :]
                found.append(pltpu.roll(jnp.broadcast_to(line, (SUBS, LANES)), 0, 1, stride=seqs, stride_axis=0))
            return jnp.concatenate(found, axis=0)[:, :seqs]

        c_f, b_f = unpacked(NS), unpacked(0)
        lane = iota((NS, seqs), 1)
        c_big = jnp.concatenate([jnp.where(lane == b, c_f, 0.0).astype(BF16) for b in range(seqs)], axis=0)
        s_c = []
        for at in (0, chans // 2):
            s_big = jnp.concatenate([stb[b, at : at + chans // 2, :] for b in range(seqs)], axis=1)
            s_c.append(dot(s_big, c_big))
        s_c = jnp.concatenate(s_c, axis=0)
        x_conv = silu(x_base + x_proj.astype(F32) * cols[:, 3:4] + cols[:, 4:5]).astype(BF16)
        x_f = x_conv.astype(F32)
        z_gate = silu(z_proj.astype(F32))
        steps, decays = [], []
        for h in range(heads):
            raw = dt_proj[h : h + 1, :] + dtb_m[h]
            step = jnp.maximum(raw, 0.0) + jnp.log1p(jnp.exp(-jnp.abs(raw)))
            rate = jnp.exp(jnp.full((1, seqs), rate_m[h], F32))
            steps.append(jnp.where(live_row, step, 0.0))
            decays.append(jnp.where(live_row, jnp.exp(-step * rate), 1.0))

        def per_channel(values):
            return jnp.concatenate([jnp.broadcast_to(v, (HP, seqs)) for v in values], axis=0)

        dtx = per_channel(steps) * x_f
        decay = per_channel(decays)
        skipped = jnp.concatenate([jnp.full((HP, seqs), skip_m[h], F32) for h in range(heads)], axis=0) * x_f
        bc_dot = jnp.sum(b_f * c_f, axis=0, keepdims=True)
        y = (decay * s_c + dtx * bc_dot) + skipped
        gated = y * z_gate
        scaled = (gated * gain_col).astype(BF16)
        sq_row = jnp.broadcast_to(jnp.sum(gated * gated, axis=0, keepdims=True), (seqs, seqs))
        sq_col = jnp.sum(jnp.where(diagonal, sq_row, 0.0), axis=1, keepdims=True)
        sq_1 = sq_col.astype(BF16).astype(F32)
        sq_2 = (sq_col - sq_1).astype(BF16).astype(F32)
        sq_cols = [half_rows for term in (sq_1, sq_2, (sq_col - sq_1) - sq_2) for half_rows in (term[:SUBS], term[SUBS:])]
        loads["out_w"].wait()
        rows_seq = dot_nt(eye16, scaled).astype(BF16)
        lane_at = iota((SUBS, LANES), 1)
        spare = feats - LANES
        tails = {}
        for start in sorted({(t * feats) % LANES for t in range(n_tp)}):
            tail = jnp.zeros((SUBS, LANES), F32)
            for j, term in enumerate(sq_cols):
                tail = jnp.where(lane_at == (start + 2 * spare + j) % LANES, term, tail)
            tails[start] = tail

        def within(at):
            at = lax.rem(at, LANES)
            return (lane_at >= at) & (lane_at < at + spare)

        def folded(tile_0, tile_1, start, tail):
            main = jnp.where(iota((seqs, LANES), 1) >= start, tile_0, tile_1)
            rest = jnp.where(within(start + spare), pltpu.roll(tile_1[SUBS:], spare, 1), tail)
            rest = jnp.where(within(start), tile_1[:SUBS], rest)
            return jnp.concatenate([main, rest], axis=0).astype(BF16)

        def window_send(src, peer):
            pltpu.make_async_remote_copy(
                src_ref=src, dst_ref=br_recv.at[me], send_sem=send_sem.at[2], recv_sem=recv_sem.at[2],
                device_id={"tp": peer}, device_id_type=MESH,
            ).start()

        def windows(step):
            to = lax.rem(chip + step, chips)
            first, start = share_tile(to), lax.rem(to * 2 * feats, LANES)
            branch = [dot(rows_seq, ow[:, pl.ds(pl.multiple_of((first + k) * LANES, LANES), LANES)]) for k in range(3)]
            for j in range(2):
                begin = start + (j * feats) % LANES
                tail = jnp.zeros((SUBS, LANES), F32)
                for at, found in tails.items():
                    tail = jnp.where(begin == at, found, tail)
                br_send[2 * to + j] = folded(branch[j], branch[j + 1], begin, tail)

        for group in ([half], [half - 1, half + 1], [k for k in steps_far if abs(k - half) > 1] + [0]):
            for step in group:
                windows(step)
            for step in group:
                for which in (0, 1) if step else (1 - core,):
                    peer = lax.rem(chip + step, chips) * 2 + which
                    window_send(br_send.at[peer], peer)
        br_recv[me] = br_send[me]

        x_now = dot_nt(to_slot, x_proj)
        bc_proj = (dot_nt(bcw[...], xn[...]) * inv).astype(BF16)
        bc_now = dot(dot_nt(to_slot, bc_proj).astype(BF16), mirror)
        for out, old, now in ((out_cx, cxs, x_now), (out_cbc, cbcs, bc_now)):
            held = [old[k].astype(F32) for k in range(3)]
            for k, new in enumerate((held[1], held[2], now)):
                out[k] = jnp.where(live_slot, new, held[k]).astype(BF16)
        of_heads = jnp.concatenate(steps + decays + [jnp.zeros((-2 * heads % SUBS, seqs), F32)], axis=0)
        of_heads = exact_dot(of_heads, to_seq)
        steps_slot = [of_heads[h : h + 1, :] for h in range(heads)]
        decays_slot = [of_heads[heads + h : heads + h + 1, :] for h in range(heads)]
        dtx_slot = per_channel(steps_slot) * dot(x_conv, to_seq)
        decay_slot = per_channel(decays_slot)
        b_rows = dot_nt(to_slot, b_f.astype(BF16))
        for b in range(seqs):
            grown = dtx_slot[:, b : b + 1] * b_rows[b : b + 1, :]
            out_state[b] = decay_slot[:, b : b + 1] * st[b] + grown

        all_of(2, br_recv, others).wait_recv()
        total = br_recv[0].astype(F32)
        for t in range(1, n_tp):
            total = total + br_recv[t].astype(F32)
        shift = lax.rem(me * feats, LANES)
        total = pltpu.roll(total, lax.rem(LANES - shift, LANES), 1)
        rest = total[seqs:]
        rest = jnp.concatenate([rest, pltpu.roll(rest, LANES - spare, 1)], axis=0)
        branch_sum = jnp.concatenate([total[:seqs], rest[:, :spare]], axis=1)
        sq_at = 2 * spare
        sq_rows = [
            (total[seqs:, at : at + 1] + total[seqs:, at + 2 : at + 3]) + total[seqs:, at + 4 : at + 5]
            for at in (sq_at, sq_at + 1)
        ]
        inv_out = lax.rsqrt(jnp.concatenate(sq_rows, axis=0) / INNER + EPS)
        kept = hid_recv[core].astype(F32)
        fresh = (kept + inv_out * branch_sum).astype(BF16).astype(F32)
        out_layer[...] = jnp.where(act_col, fresh, kept).astype(BF16)

        all_of(2, br_recv, others).wait_send()

        def hid_sent(count):
            return pltpu.make_async_remote_copy(
                src_ref=hid_recv.at[pl.ds(0, count)], dst_ref=hid_recv.at[pl.ds(0, count)],
                send_sem=send_sem.at[0], recv_sem=recv_sem.at[0],
                device_id=device(0, 1 - core), device_id_type=MESH,
            )

        @pl.when((odd == 1) & (core == 0))
        def _():
            all_of(3, bcw_recv, n_tp).wait_send()

        @pl.when((odd == 1) & (core == 1))
        def _():
            all_of(3, bcw_recv, n_tp - 1).wait_send()

        @pl.when(core == 0)
        def _():
            hid_sent(chips - 1).wait_send()
            first_send(0, 1, 0, 4).wait_send()
            lend().wait_send()

        @pl.when(core == 1)
        def _():
            hid_sent(chips - 1).wait_send()
            relay().wait_send()
            relay_made().wait_send()
            all_of(1, bc_sums, chips - 1).wait_send()

    return body


def shards(
    hidden, in_gain, z_weight, x_weight, bc_weight, dt_weight, conv_x_weight, conv_x_bias,
    conv_bc_weight, conv_bc_bias, conv_x_state, conv_bc_state, dt_bias, log_rate, skip_gain,
    ssm_state, norm_gain, out_weight, pool_slot, active,
):
    n_tp = lax.axis_size("tp")
    seqs, feats = hidden.shape
    heads = ssm_state.shape[1]
    chans = z_weight.shape[1]
    bc_dev = bc_weight.shape[1]
    width = in_gain.shape[0]
    tiles = width // LANES
    vmem = pl.BlockSpec(memory_space=pltpu.VMEM)
    hbm = pl.BlockSpec(memory_space=pl.ANY)
    shape = jax.ShapeDtypeStruct
    results = (
        ((seqs, feats), BF16),
        ((3, seqs, chans), BF16),
        ((3, seqs, bc_dev), BF16),
        ((seqs, chans, NS), F32),
    )
    made = pl.pallas_call(
        make_kernel(n_tp, seqs, feats, heads, chans, bc_dev),
        out_shape=tuple(pltpu.VMEM(dims, kind) for dims, kind in results),
        in_specs=[hbm] * 20,
        out_specs=(vmem,) * 4,
        scratch_shapes=[
            pltpu.VMEM((chans, width), BF16),
            pltpu.VMEM((chans, width), BF16),
            pltpu.VMEM((bc_dev, width), BF16),
            pltpu.VMEM((heads, width), BF16),
            pltpu.VMEM((3, seqs, chans), BF16),
            pltpu.VMEM((3, seqs, bc_dev), BF16),
            pltpu.VMEM((seqs, chans, NS), F32),
            pltpu.VMEM((chans, width), BF16),
            pltpu.VMEM((tiles, LANES), F32),
            pltpu.VMEM((1, seqs), jnp.int32),
            pltpu.SMEM((1, seqs), jnp.int32),
            pltpu.VMEM((1, seqs), jnp.int32),
            pltpu.VMEM((4, chans), BF16),
            pltpu.VMEM((chans,), BF16),
            pltpu.VMEM((4, bc_dev), BF16),
            pltpu.VMEM((1, bc_dev), BF16),
            pltpu.VMEM((chans,), F32),
            pltpu.SMEM((heads,), F32),
            pltpu.SMEM((heads,), F32),
            pltpu.SMEM((heads,), F32),
            pltpu.VMEM((seqs, chans, NS), BF16),
            pltpu.VMEM((seqs, width), BF16),
            pltpu.VMEM((n_tp, seqs, feats), BF16),
            pltpu.VMEM((2, 2, bc_dev, LANES), F32),
            pltpu.VMEM((tiles, bc_dev, LANES), BF16),
            pltpu.VMEM((n_tp, 3, bc_dev, LANES), BF16),
            pltpu.VMEM((n_tp // 2, (n_tp + 4) * bc_dev // SUBS, LANES), F32),
            pltpu.VMEM((n_tp * bc_dev // SUBS, LANES), F32),
            pltpu.VMEM((n_tp, seqs + SUBS, LANES), BF16),
            pltpu.VMEM((n_tp, seqs + SUBS, LANES), BF16),
            pltpu.SemaphoreType.DMA((20 + 1,)),
            pltpu.SemaphoreType.DMA((5,)),
            pltpu.SemaphoreType.DMA((6,)),
            pltpu.SemaphoreType.DMA((2,)),
            pltpu.SemaphoreType.DMA((2,)),
        ],
        compiler_params=pltpu.CompilerParams(
            collective_id=0, has_side_effects=True, vmem_limit_bytes=60 * 1024 * 1024
        ),
        name="step",
    )(
        hidden, pool_slot, active.reshape(1, seqs), in_gain.reshape(tiles, LANES),
        z_weight.T, x_weight.T, bc_weight.T, dt_weight.T,
        conv_x_weight, conv_x_bias, conv_bc_weight, conv_bc_bias.reshape(1, bc_dev),
        conv_x_state.transpose(1, 0, 2), conv_bc_state.transpose(1, 0, 2),
        dt_bias, log_rate, skip_gain, ssm_state.reshape(seqs, chans, NS),
        norm_gain, out_weight,
    )
    out_layer, out_cx, out_cbc, out_state = pl.pallas_call(
        put_out,
        out_shape=tuple(shape(dims, kind) for dims, kind in results),
        in_specs=[vmem] * 4,
        out_specs=(hbm,) * 4,
        scratch_shapes=[pltpu.SemaphoreType.DMA((7,))],
        name="put",
    )(*(pltpu.with_memory_space_constraint(x, pltpu.VMEM) for x in made))
    return (
        out_layer,
        out_cx.transpose(1, 0, 2),
        out_cbc.transpose(1, 0, 2),
        out_state.reshape(ssm_state.shape),
    )


def solution(mesh):
    rows = ("groups", "dp")
    placed = (
        P(rows, "tp"), P(), P(None, "tp"), P(None, "tp"), P(None, "tp"), P(None, "tp"), P(None, "tp"),
        P("tp"), P(None, "tp"), P("tp"), P(rows, None, "tp"), P(rows, None, "tp"), P("tp"), P("tp"),
        P("tp"), P(rows, "tp", None, None), P("tp"), P("tp", None), P(rows, None), P(rows),
    )
    return jax.shard_map(
        shards,
        mesh=mesh,
        in_specs=placed,
        out_specs=(P(rows, "tp"), P(rows, None, "tp"), P(rows, None, "tp"), P(rows, "tp", None, None)),
        check_vma=False,
    )
```

```python
import jax
import jax.numpy as jnp
from jax import lax
from jax.experimental import pallas as pl
from jax.experimental.pallas import tpu as pltpu
from jax.sharding import PartitionSpec as P

HP = 64
NS = 128
INNER = 5120
EPS = 1e-05
F32 = jnp.float32
BF16 = jnp.bfloat16
LANES = 128
SUBS = 8

NT = (((1,), (1,)), ((), ()))
MESH = pl.DeviceIdType.MESH


def dot(a, b):
    return jnp.dot(a, b, preferred_element_type=F32)


def dot_nt(a, b):
    return lax.dot_general(a, b, NT, preferred_element_type=F32)


def iota(shape, dim):
    return lax.broadcasted_iota(jnp.int32, shape, dim)


def one_hot(mask):
    return mask.astype(F32).astype(BF16)


def eye(n):
    return one_hot(iota((n, n), 0) == iota((n, n), 1))


def silu(x):
    return x * jax.nn.sigmoid(x)


def exact_dot(x, picks):
    first = x.astype(BF16)
    rest = x - first.astype(F32)
    second = rest.astype(BF16)
    third = (rest - second.astype(F32)).astype(BF16)
    return (dot(first, picks) + dot(second, picks)) + dot(third, picks)


def put_out(*refs):
    sems = refs[-1]
    pieces = 4
    rows = refs[3].shape[0] // pieces
    copies = [
        pltpu.make_async_copy(refs[3].at[pl.ds(k * rows, rows)], refs[7].at[pl.ds(k * rows, rows)], sems.at[3 + k])
        for k in range(pieces)
    ]
    copies += [pltpu.make_async_copy(refs[k], refs[4 + k], sems.at[k]) for k in range(3)]
    for copy in copies:
        copy.start()
    for copy in copies:
        copy.wait()


def make_kernel(n_tp, seqs, feats, heads, chans, bc_dev):
    width = n_tp * feats
    tiles = width // LANES
    chips = n_tp // 2
    half = chips // 2
    steps_far = [half]
    for far in range(half - 1, 0, -1):
        steps_far += [far, chips - far]
    others = n_tp - 1

    def body(
        hid, slot, act, in_gain, z_w, x_w, bc_w, dt_w, cx_w, cx_b, cbc_w, cbc_b, cx_s, cbc_s,
        dt_bias, log_rate, skip_gain, state, norm_gain, out_w,
        out_layer, out_cx, out_cbc, out_state,
        zw, xw, bcw, dtw, cxs, cbcs, st, ow, gain, slot_v, slot_m, act_v, cxw, cxb, cbcw, cbcb, ngain,
        dtb_m, rate_m, skip_m,
        stb, xn, hid_recv, side, bcw_send, bcw_recv, bc_sums, bc_made, br_send, br_recv,
        in_sem, send_sem, recv_sem, relay_sem, side_sem,
    ):
        me = lax.axis_index("tp")
        chip, core = me // 2, lax.rem(me, 2)
        row = lax.axis_index("dp")
        odd = lax.rem(row, 2)
        barrier = pltpu.get_barrier_semaphore()

        def device(step, which):
            return {"tp": lax.rem(chip + step, chips) * 2 + which}

        loads = {}

        def load(name, src, dst):
            loads[name] = pltpu.make_async_copy(src, dst, in_sem.at[len(loads)])
            loads[name].start()

        load("hid", hid, hid_recv.at[core])

        @pl.when(core == 0)
        def _():
            pl.semaphore_signal(barrier, inc=1, device_id=device(0, 1), device_id_type=MESH)

        @pl.when(core == 1)
        def _():
            for step in steps_far:
                pl.semaphore_signal(barrier, inc=1, device_id=device(step, 1), device_id_type=MESH)

            @pl.when(odd == 0)
            def _():
                for t in range(n_tp):
                    pl.semaphore_signal(barrier, inc=1, device_id={"tp": t, "dp": row + 1}, device_id_type=MESH)

            @pl.when(odd == 1)
            def _():
                for step in steps_far:
                    pl.semaphore_signal(barrier, inc=1, device_id=device(step, 0), device_id_type=MESH)

        load("slot", slot, slot_v)
        load("slot_m", slot, slot_m)
        load("act", act, act_v)
        load("bc_w", bc_w, bcw)
        load("in_gain", in_gain, gain)
        load("cbc_s", cbc_s, cbcs)
        load("cbc_w", cbc_w, cbcw)
        load("cbc_b", cbc_b, cbcb)
        load("dt_w", dt_w, dtw)
        load("cx_s", cx_s, cxs)
        load("cx_w", cx_w, cxw)
        load("cx_b", cx_b, cxb)
        load("norm_gain", norm_gain, ngain)
        load("dt_bias", dt_bias, dtb_m)
        load("log_rate", log_rate, rate_m)
        load("skip_gain", skip_gain, skip_m)
        load("state", state, st)
        load("x_w", x_w, xw)
        load("z_w", z_w, zw)
        load("out_w", out_w, ow)

        def first_send(step, which, dst_slot, phase=0):
            arrival = 5 if step == half else phase
            return pltpu.make_async_remote_copy(
                src_ref=hid_recv.at[core], dst_ref=hid_recv.at[dst_slot],
                send_sem=send_sem.at[phase], recv_sem=recv_sem.at[arrival],
                device_id=device(step, which), device_id_type=MESH,
            )

        def relay(first=1, count=n_tp - 1):
            return pltpu.make_async_remote_copy(
                src_ref=hid_recv.at[pl.ds(first, count)], dst_ref=hid_recv.at[pl.ds(first, count)],
                send_sem=relay_sem.at[0], recv_sem=recv_sem.at[0],
                device_id=device(0, 0), device_id_type=MESH,
            )

        @pl.when(core == 0)
        def _():
            loads["hid"].wait()
            pl.semaphore_wait(barrier, 1 + odd * (2 * chips - 1))
            first_send(0, 1, 0, 4).start()
            for step in steps_far:
                first_send(step, 1, 2 * (chips - step)).start()

        for name in ("slot", "slot_m", "act", "in_gain", "cbc_s", "cbc_w", "cbc_b"):
            loads[name].wait()
        slot_row = slot_v[...]
        by_slot = iota((seqs, seqs), 0) == jnp.broadcast_to(slot_row, (seqs, seqs))
        to_slot = one_hot(by_slot)
        eye16 = eye(seqs)
        diagonal = iota((seqs, seqs), 0) == iota((seqs, seqs), 1)
        to_seq = dot_nt(eye16, to_slot).astype(BF16)
        act_f = jnp.broadcast_to(act_v[...].astype(F32), (seqs, seqs))
        live_row = act_v[...] > 0
        act_col = jnp.sum(jnp.where(diagonal, act_f, 0.0), axis=1, keepdims=True) > 0
        live_slot = jnp.sum(jnp.where(by_slot, act_f, 0.0), axis=1, keepdims=True) > 0
        bc_rows = jnp.concatenate([cbcw[...].astype(F32), cbcb[...].astype(F32)], axis=0)
        row_at, col_at = iota((bc_dev, bc_dev), 0), iota((bc_dev, bc_dev), 1)
        mirror = one_hot(col_at == row_at // SUBS * SUBS + lax.rem(SUBS - lax.rem(row_at, SUBS), SUBS))
        bc_cols = dot_nt(mirror, bc_rows.astype(BF16))
        bc_old = [dot(dot_nt(mirror, cbcs[k]).astype(BF16), to_slot) for k in range(3)]
        bc_base = (bc_old[0] * bc_cols[:, 0:1] + bc_old[1] * bc_cols[:, 1:2]) + bc_old[2] * bc_cols[:, 2:3]
        pad = jnp.zeros((bc_dev, LANES - seqs), F32)
        side[core, 0] = jnp.concatenate([bc_base + bc_cols[:, 4:5], pad], axis=1)
        side[core, 1] = jnp.broadcast_to(bc_cols[:, 3:4], (bc_dev, LANES))
        def lend():
            return pltpu.make_async_remote_copy(
                src_ref=side.at[0], dst_ref=side.at[0], send_sem=side_sem.at[0], recv_sem=side_sem.at[1],
                device_id=device(0, 1), device_id_type=MESH,
            )

        @pl.when(core == 0)
        def _():
            lend().start()

        loads["bc_w"].wait()
        turned = dot(mirror, bcw[...]).astype(BF16)
        bcw[...] = turned
        for k in range(tiles):
            bcw_send[k] = turned[:, k * LANES : (k + 1) * LANES]

        def share_tile(of_chip):
            return (of_chip * 2 * feats) // LANES

        def share(of_chip, to_row):
            return pltpu.make_async_remote_copy(
                src_ref=bcw_send.at[pl.ds(share_tile(of_chip), 3)], dst_ref=bcw_recv.at[me],
                send_sem=send_sem.at[3], recv_sem=recv_sem.at[3],
                device_id={"tp": 2 * of_chip + 1, "dp": to_row}, device_id_type=MESH,
            )

        for name in ("cx_s", "cx_w", "cx_b", "norm_gain", "dt_bias", "log_rate", "skip_gain"):
            loads[name].wait()
        eye_ch = eye(chans)
        g0 = ngain[...].reshape(1, chans)
        g1 = g0.astype(BF16).astype(F32)
        g2 = (g0 - g1).astype(BF16).astype(F32)
        g3 = (g0 - g1) - g2
        rows = jnp.concatenate([cxw[...].astype(F32), cxb[...].astype(F32).reshape(1, chans), g1, g2, g3], axis=0)
        cols = dot_nt(eye_ch, rows.astype(BF16))
        gain_col = (cols[:, 5:6] + cols[:, 6:7]) + cols[:, 7:8]
        x_old = [dot(dot_nt(eye_ch, cxs[k]).astype(BF16), to_slot) for k in range(3)]
        x_base = (x_old[0] * cols[:, 0:1] + x_old[1] * cols[:, 1:2]) + x_old[2] * cols[:, 2:3]
        loads["state"].wait()

        def narrow(i, carry):
            stb[i] = st[slot_m[0, i]].astype(BF16)
            return carry

        lax.fori_loop(0, seqs, narrow, 0)
        loads["dt_w"].wait()

        @pl.when(core == 1)
        def _():
            loads["hid"].wait()
            pl.semaphore_wait(barrier, chips + odd * chips)
            pl.semaphore_signal(barrier, inc=1, device_id=device(0, 0), device_id_type=MESH)
            for step in steps_far:
                first_send(step, 1, 2 * (chips - step) + 1).start()

        @pl.when(odd == 1)
        def _():
            for step in steps_far:
                for to_row in (row - 1, row):
                    share(lax.rem(chip + step, chips), to_row).start()
            share(chip, row - 1).start()

            @pl.when(core == 0)
            def _():
                share(chip, row).start()

            @pl.when(core == 1)
            def _():
                bcw_recv[me] = bcw_send[pl.ds(share_tile(chip), 3)]


        def all_of(phase, dst_ref, count):
            return pltpu.make_async_remote_copy(
                src_ref=dst_ref.at[pl.ds(0, count)], dst_ref=dst_ref.at[pl.ds(0, count)],
                send_sem=send_sem.at[phase], recv_sem=recv_sem.at[phase],
                device_id=device(0, 1 - core), device_id_type=MESH,
            )

        lines = n_tp * bc_dev // SUBS
        own_lines = 2 * bc_dev // SUBS

        def packed(x):
            count = x.shape[0]
            spread = jnp.concatenate([x, jnp.zeros((count, LANES - seqs), F32)], axis=1)
            spread = pltpu.roll(spread.reshape(count // SUBS, SUBS, LANES), 0, 2, stride=seqs, stride_axis=1)
            return jnp.sum(spread, axis=1)

        def relay_made():
            return pltpu.make_async_remote_copy(
                src_ref=bc_made, dst_ref=bc_made, send_sem=relay_sem.at[1], recv_sem=recv_sem.at[1],
                device_id=device(0, 0), device_id_type=MESH,
            )

        @pl.when(core == 1)
        def _():
            @pl.when(odd == 0)
            def _():
                all_of(3, bcw_recv, n_tp).wait_recv()

            @pl.when(odd == 1)
            def _():
                all_of(3, bcw_recv, n_tp - 1).wait_recv()

            first = share_tile(chip)
            first_send(0, 1, 0, 4).wait_recv()
            pair = jnp.concatenate([hid_recv[0].astype(F32), hid_recv[1].astype(F32), jnp.zeros((seqs, 3 * LANES - 2 * feats), F32)], axis=1)
            pair = pltpu.roll(pair, lax.rem(chip * 2 * feats, LANES), 1)
            terms = 0.0
            for k in range(3):
                scaled_k = (pair[:, k * LANES : (k + 1) * LANES] * gain[pl.ds(first + k, 1), :]).astype(BF16)
                weights = jnp.concatenate([bcw_recv[t, k] for t in range(n_tp)], axis=0)
                terms = terms + dot_nt(weights, scaled_k)
            bc_sums[chip, 0:lines, :] = packed(terms)
            lend().wait_recv()
            for j in range(2):
                own = packed(jnp.concatenate([side[0, j], side[1, j]], axis=0)[:, :seqs])
                bc_sums[chip, lines + j * own_lines : lines + (j + 1) * own_lines, :] = own
            for step in steps_far:
                pltpu.make_async_remote_copy(
                    src_ref=bc_sums.at[chip], dst_ref=bc_sums.at[chip], send_sem=send_sem.at[1], recv_sem=recv_sem.at[1],
                    device_id=device(step, 1), device_id_type=MESH,
                ).start()

        @pl.when(core == 0)
        def _():
            all_of(0, hid_recv, n_tp - 1).wait_recv()

        @pl.when(core == 1)
        def _():
            all_of(0, hid_recv, n_tp - 4).wait_recv()
            relay(1, 2 * half - 1).start()
            relay(2 * half + 2, n_tp - 2 * half - 2).start()
            pltpu.make_async_remote_copy(
                src_ref=hid_recv.at[pl.ds(2 * half, 2)], dst_ref=hid_recv.at[pl.ds(2 * half, 2)],
                send_sem=send_sem.at[0], recv_sem=recv_sem.at[5],
                device_id=device(half, 1), device_id_type=MESH,
            ).wait_recv()
            relay(2 * half, 2).start()

        blocks = [
            hid_recv[2 * lax.rem(t // 2 - chip + chips, chips) + t % 2].astype(F32) for t in range(n_tp)
        ]
        whole = jnp.concatenate(blocks, axis=1)
        for k in range(tiles):
            at = slice(k * LANES, (k + 1) * LANES)
            xn[:, at] = (whole[:, at] * gain[k : k + 1, :]).astype(BF16)
        squares = whole[:, :LANES] * whole[:, :LANES]
        for k in range(1, tiles):
            part = whole[:, k * LANES : (k + 1) * LANES]
            squares = squares + part * part
        inv_col = lax.rsqrt(jnp.sum(squares, axis=1, keepdims=True) / width + EPS)
        inv = jnp.sum(jnp.where(diagonal, jnp.broadcast_to(inv_col, (seqs, seqs)), 0.0), axis=0, keepdims=True)

        of_seq = lax.rem(iota((seqs, LANES), 1), seqs) == iota((seqs, LANES), 0)
        inv_lanes = jnp.sum(jnp.where(of_seq, jnp.broadcast_to(inv_col, (seqs, LANES)), 0.0), axis=0, keepdims=True)

        dt_proj = (dot_nt(dtw[...], xn[...]) * inv).astype(BF16).astype(F32)
        loads["x_w"].wait()
        loads["z_w"].wait()
        x_proj = (dot_nt(xw[...], xn[...]) * inv).astype(BF16)
        z_proj = (dot_nt(zw[...], xn[...]) * inv).astype(BF16)
        @pl.when(core == 1)
        def _():
            all_of(1, bc_sums, chips - 1).wait_recv()
            sums = bc_sums[0, 0:lines, :]
            for c in range(1, chips):
                sums = sums + bc_sums[c, 0:lines, :]
            base, tap = [
                jnp.concatenate([bc_sums[c, at : at + own_lines, :] for c in range(chips)], axis=0)
                for at in (lines, lines + own_lines)
            ]
            made = silu(base + (sums * inv_lanes).astype(BF16).astype(F32) * tap)
            bc_made[...] = made.astype(BF16).astype(F32)
            relay_made().start()

        @pl.when(core == 0)
        def _():
            relay_made().wait_recv()

        bc_conv = bc_made[...]

        def unpacked(at):
            found = []
            for eight in range(NS // SUBS):
                line = bc_conv[at // SUBS + eight : at // SUBS + eight + 1, :]
                found.append(pltpu.roll(jnp.broadcast_to(line, (SUBS, LANES)), 0, 1, stride=seqs, stride_axis=0))
            return jnp.concatenate(found, axis=0)[:, :seqs]

        c_f, b_f = unpacked(NS), unpacked(0)
        lane = iota((NS, seqs), 1)
        c_big = jnp.concatenate([jnp.where(lane == b, c_f, 0.0).astype(BF16) for b in range(seqs)], axis=0)
        s_c = []
        for at in (0, chans // 2):
            s_big = jnp.concatenate([stb[b, at : at + chans // 2, :] for b in range(seqs)], axis=1)
            s_c.append(dot(s_big, c_big))
        s_c = jnp.concatenate(s_c, axis=0)
        x_conv = silu(x_base + x_proj.astype(F32) * cols[:, 3:4] + cols[:, 4:5]).astype(BF16)
        x_f = x_conv.astype(F32)
        z_gate = silu(z_proj.astype(F32))
        steps, decays = [], []
        for h in range(heads):
            raw = dt_proj[h : h + 1, :] + dtb_m[h]
            step = jnp.maximum(raw, 0.0) + jnp.log1p(jnp.exp(-jnp.abs(raw)))
            rate = jnp.exp(jnp.full((1, seqs), rate_m[h], F32))
            steps.append(jnp.where(live_row, step, 0.0))
            decays.append(jnp.where(live_row, jnp.exp(-step * rate), 1.0))

        def per_channel(values):
            return jnp.concatenate([jnp.broadcast_to(v, (HP, seqs)) for v in values], axis=0)

        dtx = per_channel(steps) * x_f
        decay = per_channel(decays)
        skipped = jnp.concatenate([jnp.full((HP, seqs), skip_m[h], F32) for h in range(heads)], axis=0) * x_f
        bc_dot = jnp.sum(b_f * c_f, axis=0, keepdims=True)
        y = (decay * s_c + dtx * bc_dot) + skipped
        gated = y * z_gate
        scaled = (gated * gain_col).astype(BF16)
        sq_row = jnp.broadcast_to(jnp.sum(gated * gated, axis=0, keepdims=True), (seqs, seqs))
        sq_col = jnp.sum(jnp.where(diagonal, sq_row, 0.0), axis=1, keepdims=True)
        sq_1 = sq_col.astype(BF16).astype(F32)
        sq_2 = (sq_col - sq_1).astype(BF16).astype(F32)
        sq_cols = [half_rows for term in (sq_1, sq_2, (sq_col - sq_1) - sq_2) for half_rows in (term[:SUBS], term[SUBS:])]
        loads["out_w"].wait()
        rows_seq = dot_nt(eye16, scaled).astype(BF16)
        lane_at = iota((SUBS, LANES), 1)
        spare = feats - LANES
        tails = {}
        for start in sorted({(t * feats) % LANES for t in range(n_tp)}):
            tail = jnp.zeros((SUBS, LANES), F32)
            for j, term in enumerate(sq_cols):
                tail = jnp.where(lane_at == (start + 2 * spare + j) % LANES, term, tail)
            tails[start] = tail

        def within(at):
            at = lax.rem(at, LANES)
            return (lane_at >= at) & (lane_at < at + spare)

        def folded(tile_0, tile_1, start, tail):
            main = jnp.where(iota((seqs, LANES), 1) >= start, tile_0, tile_1)
            rest = jnp.where(within(start + spare), pltpu.roll(tile_1[SUBS:], spare, 1), tail)
            rest = jnp.where(within(start), tile_1[:SUBS], rest)
            return jnp.concatenate([main, rest], axis=0).astype(BF16)

        def window_send(src, peer):
            pltpu.make_async_remote_copy(
                src_ref=src, dst_ref=br_recv.at[me], send_sem=send_sem.at[2], recv_sem=recv_sem.at[2],
                device_id={"tp": peer}, device_id_type=MESH,
            ).start()

        def windows(step):
            to = lax.rem(chip + step, chips)
            first, start = share_tile(to), lax.rem(to * 2 * feats, LANES)
            branch = [dot(rows_seq, ow[:, pl.ds(pl.multiple_of((first + k) * LANES, LANES), LANES)]) for k in range(3)]
            for j in range(2):
                begin = start + (j * feats) % LANES
                tail = jnp.zeros((SUBS, LANES), F32)
                for at, found in tails.items():
                    tail = jnp.where(begin == at, found, tail)
                br_send[2 * to + j] = folded(branch[j], branch[j + 1], begin, tail)

        for group in ([half], [half - 1, half + 1], [k for k in steps_far if abs(k - half) > 1] + [0]):
            for step in group:
                windows(step)
            for step in group:
                for which in (1, 0) if step else (1 - core,):
                    peer = lax.rem(chip + step, chips) * 2 + which
                    window_send(br_send.at[peer], peer)
        br_recv[me] = br_send[me]

        x_now = dot_nt(to_slot, x_proj)
        bc_proj = (dot_nt(bcw[...], xn[...]) * inv).astype(BF16)
        bc_now = dot(dot_nt(to_slot, bc_proj).astype(BF16), mirror)
        for out, old, now in ((out_cx, cxs, x_now), (out_cbc, cbcs, bc_now)):
            held = [old[k].astype(F32) for k in range(3)]
            for k, new in enumerate((held[1], held[2], now)):
                out[k] = jnp.where(live_slot, new, held[k]).astype(BF16)
        of_heads = jnp.concatenate(steps + decays + [jnp.zeros((-2 * heads % SUBS, seqs), F32)], axis=0)
        of_heads = exact_dot(of_heads, to_seq)
        steps_slot = [of_heads[h : h + 1, :] for h in range(heads)]
        decays_slot = [of_heads[heads + h : heads + h + 1, :] for h in range(heads)]
        dtx_slot = per_channel(steps_slot) * dot(x_conv, to_seq)
        decay_slot = per_channel(decays_slot)
        b_rows = dot_nt(to_slot, b_f.astype(BF16))
        for b in range(seqs):
            grown = dtx_slot[:, b : b + 1] * b_rows[b : b + 1, :]
            out_state[b] = decay_slot[:, b : b + 1] * st[b] + grown

        all_of(2, br_recv, others).wait_recv()
        total = br_recv[0].astype(F32)
        for t in range(1, n_tp):
            total = total + br_recv[t].astype(F32)
        shift = lax.rem(me * feats, LANES)
        sq_at = lane_at - lax.rem(shift + 2 * spare, LANES)
        sq_rows = [
            jnp.sum(jnp.where((sq_at == j) | (sq_at == j + 2) | (sq_at == j + 4), total[seqs:], 0.0), axis=1, keepdims=True)
            for j in range(2)
        ]
        inv_out = lax.rsqrt(jnp.concatenate(sq_rows, axis=0) / INNER + EPS)
        total = pltpu.roll(total, lax.rem(LANES - shift, LANES), 1)
        rest = total[seqs:]
        rest = jnp.concatenate([rest, pltpu.roll(rest, LANES - spare, 1)], axis=0)
        branch_sum = jnp.concatenate([total[:seqs], rest[:, :spare]], axis=1)
        kept = hid_recv[core].astype(F32)
        fresh = (kept + inv_out * branch_sum).astype(BF16).astype(F32)
        out_layer[...] = jnp.where(act_col, fresh, kept).astype(BF16)

        all_of(2, br_recv, others).wait_send()

        def hid_sent(count):
            return pltpu.make_async_remote_copy(
                src_ref=hid_recv.at[pl.ds(0, count)], dst_ref=hid_recv.at[pl.ds(0, count)],
                send_sem=send_sem.at[0], recv_sem=recv_sem.at[0],
                device_id=device(0, 1 - core), device_id_type=MESH,
            )

        @pl.when((odd == 1) & (core == 0))
        def _():
            all_of(3, bcw_recv, n_tp).wait_send()

        @pl.when((odd == 1) & (core == 1))
        def _():
            all_of(3, bcw_recv, n_tp - 1).wait_send()

        @pl.when(core == 0)
        def _():
            hid_sent(chips - 1).wait_send()
            first_send(0, 1, 0, 4).wait_send()
            lend().wait_send()

        @pl.when(core == 1)
        def _():
            hid_sent(chips - 1).wait_send()
            relay().wait_send()
            relay_made().wait_send()
            all_of(1, bc_sums, chips - 1).wait_send()

    return body


def shards(
    hidden, in_gain, z_weight, x_weight, bc_weight, dt_weight, conv_x_weight, conv_x_bias,
    conv_bc_weight, conv_bc_bias, conv_x_state, conv_bc_state, dt_bias, log_rate, skip_gain,
    ssm_state, norm_gain, out_weight, pool_slot, active,
):
    n_tp = lax.axis_size("tp")
    seqs, feats = hidden.shape
    heads = ssm_state.shape[1]
    chans = z_weight.shape[1]
    bc_dev = bc_weight.shape[1]
    width = in_gain.shape[0]
    tiles = width // LANES
    vmem = pl.BlockSpec(memory_space=pltpu.VMEM)
    hbm = pl.BlockSpec(memory_space=pl.ANY)
    shape = jax.ShapeDtypeStruct
    results = (
        ((seqs, feats), BF16),
        ((3, seqs, chans), BF16),
        ((3, seqs, bc_dev), BF16),
        ((seqs, chans, NS), F32),
    )
    made = pl.pallas_call(
        make_kernel(n_tp, seqs, feats, heads, chans, bc_dev),
        out_shape=tuple(pltpu.VMEM(dims, kind) for dims, kind in results),
        in_specs=[hbm] * 20,
        out_specs=(vmem,) * 4,
        scratch_shapes=[
            pltpu.VMEM((chans, width), BF16),
            pltpu.VMEM((chans, width), BF16),
            pltpu.VMEM((bc_dev, width), BF16),
            pltpu.VMEM((heads, width), BF16),
            pltpu.VMEM((3, seqs, chans), BF16),
            pltpu.VMEM((3, seqs, bc_dev), BF16),
            pltpu.VMEM((seqs, chans, NS), F32),
            pltpu.VMEM((chans, width), BF16),
            pltpu.VMEM((tiles, LANES), F32),
            pltpu.VMEM((1, seqs), jnp.int32),
            pltpu.SMEM((1, seqs), jnp.int32),
            pltpu.VMEM((1, seqs), jnp.int32),
            pltpu.VMEM((4, chans), BF16),
            pltpu.VMEM((chans,), BF16),
            pltpu.VMEM((4, bc_dev), BF16),
            pltpu.VMEM((1, bc_dev), BF16),
            pltpu.VMEM((chans,), F32),
            pltpu.SMEM((heads,), F32),
            pltpu.SMEM((heads,), F32),
            pltpu.SMEM((heads,), F32),
            pltpu.VMEM((seqs, chans, NS), BF16),
            pltpu.VMEM((seqs, width), BF16),
            pltpu.VMEM((n_tp, seqs, feats), BF16),
            pltpu.VMEM((2, 2, bc_dev, LANES), F32),
            pltpu.VMEM((tiles, bc_dev, LANES), BF16),
            pltpu.VMEM((n_tp, 3, bc_dev, LANES), BF16),
            pltpu.VMEM((n_tp // 2, (n_tp + 4) * bc_dev // SUBS, LANES), F32),
            pltpu.VMEM((n_tp * bc_dev // SUBS, LANES), F32),
            pltpu.VMEM((n_tp, seqs + SUBS, LANES), BF16),
            pltpu.VMEM((n_tp, seqs + SUBS, LANES), BF16),
            pltpu.SemaphoreType.DMA((20 + 1,)),
            pltpu.SemaphoreType.DMA((5,)),
            pltpu.SemaphoreType.DMA((6,)),
            pltpu.SemaphoreType.DMA((2,)),
            pltpu.SemaphoreType.DMA((2,)),
        ],
        compiler_params=pltpu.CompilerParams(
            collective_id=0, has_side_effects=True, vmem_limit_bytes=60 * 1024 * 1024
        ),
        name="step",
    )(
        hidden, pool_slot, active.reshape(1, seqs), in_gain.reshape(tiles, LANES),
        z_weight.T, x_weight.T, bc_weight.T, dt_weight.T,
        conv_x_weight, conv_x_bias, conv_bc_weight, conv_bc_bias.reshape(1, bc_dev),
        conv_x_state.transpose(1, 0, 2), conv_bc_state.transpose(1, 0, 2),
        dt_bias, log_rate, skip_gain, ssm_state.reshape(seqs, chans, NS),
        norm_gain, out_weight,
    )
    out_layer, out_cx, out_cbc, out_state = pl.pallas_call(
        put_out,
        out_shape=tuple(shape(dims, kind) for dims, kind in results),
        in_specs=[vmem] * 4,
        out_specs=(hbm,) * 4,
        scratch_shapes=[pltpu.SemaphoreType.DMA((7,))],
        name="put",
    )(*(pltpu.with_memory_space_constraint(x, pltpu.VMEM) for x in made))
    return (
        out_layer,
        out_cx.transpose(1, 0, 2),
        out_cbc.transpose(1, 0, 2),
        out_state.reshape(ssm_state.shape),
    )


def solution(mesh):
    rows = ("groups", "dp")
    placed = (
        P(rows, "tp"), P(), P(None, "tp"), P(None, "tp"), P(None, "tp"), P(None, "tp"), P(None, "tp"),
        P("tp"), P(None, "tp"), P("tp"), P(rows, None, "tp"), P(rows, None, "tp"), P("tp"), P("tp"),
        P("tp"), P(rows, "tp", None, None), P("tp"), P("tp", None), P(rows, None), P(rows),
    )
    return jax.shard_map(
        shards,
        mesh=mesh,
        in_specs=placed,
        out_specs=(P(rows, "tp"), P(rows, None, "tp"), P(rows, None, "tp"), P(rows, "tp", None, None)),
        check_vma=False,
    )
```
